32 devices in a mesh: il: 2 (over core), xl: 4 (over y, x), ta: 4 (over z).
Axes of the slice: x: 2, y: 2, z: 4, core: 2. Of those that a mesh axis runs over, the one named last changes fastest.
Arguments:
- traces: float32 [32, 832, 1024], P('il', 'xl', 'ta'), may hold values from -6 to 6
- bin_steps: int32 [2, 32, 832], P(None, 'il', 'xl'), may hold values from -1 to 1
Outputs:
- regridded: float32 [16, 416, 1536], P('il', 'xl', 'ta')
The draws below stay inside these ranges and needn't reach their ends.
Inputs may be any that keep to these rules, and one draw needn't show every extreme that they name: `bin_steps`: every entry is -1, 0 or 1.
All inputs are finite; a program needn't handle non-finite values.
Results may differ from the reference program's by a relative error of at most 0.0001.
Values sent between devices are 32-bit elements; how exact they have to be, the bound alone decides.
A program may use at most 128 MiB of HBM per device.

```python
import jax
import jax.numpy as jnp
from jax import lax

CT = 256
TAPS = 16
P_SIZE = 3
Q = 2
NI = 32
NX = 832
NT = 1024
BI = 16
BX = 416
N_TA = 4


def set_ends(entries, own_key, low, largest):
    longest = entries.shape.index(max(entries.shape))
    spots = []
    for shift in (0, 1):
        where = [jax.random.randint(jax.random.fold_in(own_key, axis), (), 0, length) for axis, length in enumerate(entries.shape)]
        where[longest] = (where[longest] + shift) % entries.shape[longest]
        spots.append(tuple(where))
    return entries.at[spots[0]].set(low).at[spots[1]].set(largest)


def block_scale(key, shape, cuts, smallest, high):
    loudness, own = 1.0, jax.random.fold_in(key, 6)
    for dim, blocks in cuts:
        draws = jnp.exp(jax.random.uniform(jax.random.fold_in(own, dim), (blocks,), jnp.float32, smallest / len(cuts), high / len(cuts)))
        loudness = loudness * jnp.repeat(draws, shape[dim] // blocks).reshape([-1 if axis == dim else 1 for axis in range(len(shape))])
    return loudness


def gaussian(key, dims, spread, most, split=(), kind=jnp.bfloat16):
    drawn = spread * jax.random.normal(key, dims, jnp.float32)
    if split:
        drawn = drawn * block_scale(key, dims, split, -0.22, 0.18)
    return jnp.clip(drawn, -most, most).astype(kind)


def setup_inputs(seed: int = 0) -> dict:
    streams_of = jax.random.split(jax.random.key(seed), 3)
    traces = gaussian(streams_of[0], (NI, NX, NT), 1.0, 6.0, ((0, 2), (1, 4), (2, 4)), jnp.float32)
    bin_steps = set_ends(jax.random.randint(streams_of[1], (2, NI, NX), -1, 2), jax.random.fold_in(streams_of[1], 1), -1, 1).astype(jnp.int32)
    return {"traces": traces, "bin_steps": bin_steps}


def lanczos_table(row_count, col_count, tap_reach, ratio_p, ratio_q):
    row_ids = lax.broadcasted_iota(jnp.int32, (row_count, col_count), 0)
    col_ids = lax.broadcasted_iota(jnp.int32, (row_count, col_count), 1)
    offset = (col_ids * ratio_q - (row_ids - tap_reach) * ratio_p).astype(jnp.float32) / jnp.float32(ratio_p)
    inside = jnp.abs(offset) < jnp.float32(tap_reach)
    weights = jnp.sinc(offset) * jnp.sinc(offset / jnp.float32(tap_reach))
    return jnp.where(inside, weights, jnp.zeros_like(weights))


def reference(traces, bin_steps):
    tap_reach = TAPS // 2
    bin_total = jnp.zeros((BI + 2, BX + 2, NT), jnp.float32)
    fold_count = jnp.zeros((BI + 2, BX + 2), jnp.float32)
    for row_phase in (0, 1):
        for col_phase in (0, 1):
            sub_traces = traces[row_phase::2, col_phase::2]
            step_il = bin_steps[0, row_phase::2, col_phase::2]
            step_xl = bin_steps[1, row_phase::2, col_phase::2]
            for shift_il in (-1, 0, 1):
                for shift_xl in (-1, 0, 1):
                    chosen = ((step_il == shift_il) & (step_xl == shift_xl)).astype(jnp.float32)
                    widths = ((1 + shift_il, 1 - shift_il), (1 + shift_xl, 1 - shift_xl))
                    bin_total = bin_total + jnp.pad(sub_traces * chosen[:, :, None], widths + ((0, 0),))
                    fold_count = fold_count + jnp.pad(chosen, widths)
    stacked = bin_total[1:-1, 1:-1] / jnp.maximum(fold_count[1:-1, 1:-1], 1.0)[:, :, None]
    padded = jnp.pad(stacked, ((0, 0), (0, 0), (tap_reach, tap_reach)))
    taps_table = lanczos_table(CT + 2 * tap_reach, CT * P_SIZE // Q, tap_reach, P_SIZE, Q)
    blocks = []
    for block_idx in range(N_TA):
        block_rows = padded[:, :, block_idx * CT: block_idx * CT + CT + 2 * tap_reach].reshape(BI * BX, CT + 2 * tap_reach)
        result = jnp.dot(block_rows, taps_table, precision=lax.Precision.HIGHEST, preferred_element_type=jnp.float32)
        blocks.append(result.reshape(BI, BX, CT * P_SIZE // Q))
    return jnp.concatenate(blocks, axis=2)
```

```python
import functools

import numpy as np
import jax
import jax.numpy as jnp
from jax import lax
from jax.experimental import pallas as pl
from jax.experimental.pallas import tpu as pltpu
from jax.sharding import PartitionSpec as P

TAPS = 16
P_SIZE = 3
Q = 2
REACH = TAPS // 2
LANES = 128
MESH = pl.DeviceIdType.MESH
F32, BF16 = jnp.float32, jnp.bfloat16


def lanczos_table(span):
    rows = np.arange(span + 2 * REACH)[:, None] - REACH
    cols = np.arange(span * P_SIZE // Q)[None, :]
    offset = (cols * Q - rows * P_SIZE).astype(np.float64) / P_SIZE
    weights = np.sinc(offset) * np.sinc(offset / REACH)
    return np.where(np.abs(offset) < REACH, weights, 0.0).astype(np.float32)


def split_table(table):
    high = table.astype(BF16)
    low = (table - high.astype(np.float32)).astype(BF16)
    return high, low


def halves(values):
    high = values.astype(BF16)
    low = (values - high.astype(F32)).astype(BF16)
    return high, low


def dot(a, b):
    return jnp.dot(a, b, preferred_element_type=F32)


def column_ranges(n_cols):
    own_cols, rest = n_cols // 2, n_cols - LANES
    if own_cols % 8 or rest % 16 or not LANES < 2 * rest <= 2 * LANES:
        raise ValueError("column count")
    height = (LANES // 2 + 1 + 7) // 8 * 8
    first = (LANES // 2 - 1) // 8 * 8
    return (0, LANES, 0, height), (LANES, n_cols, first, own_cols - first)


def binning(n_xl, n_ta, traces, steps_hbm, t_high_hbm, t_low_hbm, main, factor, halo_out, rim_out,
            x_left, x_right, edge_x, steps, t_high, t_low, keys, hot_a, hot_b, acc,
            rim_send, corner_send, rim_recv, corner_recv, il_recv, halo_send, halo_rim, halo_recv, halo_rim_recv,
            diag_recv, diag_corner, left_sem, right_sem, edge_sem, table_sem, send_sem, recv_sem):
    n_rows, n_cols, _ = x_left.shape
    span = LANES + x_right.shape[2]
    n_pairs, own_cols = n_rows // 2, n_cols // 2
    il, xl, ta = lax.axis_index("il"), lax.axis_index("xl"), lax.axis_index("ta")
    other = 1 - il
    has_xl, has_ta = (xl < n_xl - 1, xl > 0), (ta < n_ta - 1, ta > 0)
    xl_at, ta_at = (xl + 1, xl - 1), (ta + 1, ta - 1)
    ranges = column_ranges(n_cols)

    def when(condition, work):
        pl.when(condition)(work)

    step_load = pltpu.make_async_copy(steps_hbm, steps, table_sem.at[2])
    step_load.start()
    edge_loads = [pltpu.make_async_copy(traces.at[:, pl.ds(start, 8)], edge_x.at[d], edge_sem.at[d])
                  for d, start in enumerate((n_cols - 8, 0))]
    left_loads, right_loads = [], []
    for p in range(n_pairs):
        rows = pl.ds(2 * p, 2)
        left_loads.append(pltpu.make_async_copy(traces.at[rows, :, pl.ds(0, LANES)], x_left.at[rows], left_sem.at[p]))
        right_loads.append(pltpu.make_async_copy(traces.at[rows, :, pl.ds(LANES, span - LANES)], x_right.at[rows],
                                                 right_sem.at[p]))
    table_loads = [pltpu.make_async_copy(t_high_hbm, t_high, table_sem.at[0]),
                   pltpu.make_async_copy(t_low_hbm, t_low, table_sem.at[1])]
    for load in edge_loads:
        load.start()

    barrier = pltpu.get_barrier_semaphore()

    def greet(partner):
        pl.semaphore_signal(barrier, inc=1, device_id=partner, device_id_type=MESH)
        pl.semaphore_signal(barrier, inc=1, device_id={"il": other, **partner}, device_id_type=MESH)

    pl.semaphore_signal(barrier, inc=1, device_id={"il": other}, device_id_type=MESH)
    for d in range(2):
        when(has_ta[d], lambda d=d: greet({"ta": ta_at[d]}))
        when(has_xl[d], lambda d=d: greet({"xl": xl_at[d]}))
    for d in range(2):
        for e in range(2):
            when(has_xl[d] & has_ta[e], lambda d=d, e=e: greet({"xl": xl_at[d], "ta": ta_at[e]}))
    count_xl = sum(jnp.where(has, 1, 0) for has in has_xl)
    count_ta = sum(jnp.where(has, 1, 0) for has in has_ta)
    peers = 2 * (1 + count_xl) * (1 + count_ta) - 1
    for load in left_loads + right_loads + table_loads:
        load.start()

    for e in range(2):
        def no_ta(e=e):
            halo_recv[e] = jnp.zeros_like(halo_recv[e])
            halo_rim_recv[e] = jnp.zeros_like(halo_rim_recv[e])
        when(jnp.logical_not(has_ta[1 - e]), no_ta)
    for d in range(2):
        def no_xl(d=d):
            rim_recv[d] = jnp.zeros_like(rim_recv[d])
            corner_recv[d] = jnp.zeros_like(corner_recv[d])
        when(jnp.logical_not(has_xl[1 - d]), no_xl)
        for e in range(2):
            def no_diag(d=d, e=e):
                diag_recv[d, e] = jnp.zeros_like(diag_recv[d, e])
                diag_corner[d, e] = jnp.zeros_like(diag_corner[d, e])
            when(jnp.logical_not(has_xl[1 - d] & has_ta[1 - e]), no_diag)

    lane = lax.broadcasted_iota(jnp.int32, (1, LANES), 1)
    is_first, is_last = lane < REACH, lane >= LANES - REACH
    step_load.wait()
    col = lax.broadcasted_iota(jnp.int32, (n_rows, n_cols), 1)
    row = lax.broadcasted_iota(jnp.int32, (n_rows, n_cols), 0)
    bin_col = lax.shift_right_logical(col, 1) + steps[1]
    bin_row = steps[0] + 1
    own = (bin_col >= 0) & (bin_col < own_cols)
    code_a, code_b = [jnp.where(own, bin_row * height + bin_col - first, -1)[:, start:stop]
                      for start, stop, first, height in ranges]
    rest = n_cols - LANES
    keys[0] = code_a
    padded = jnp.concatenate([code_b, jnp.full((n_rows, LANES - rest), -1, jnp.int32)], axis=1)
    keys[1] = padded
    keys[2] = pltpu.roll(padded, rest, 1)

    def one_hot(key, height):
        rows = lax.broadcasted_iota(jnp.int32, (height, key.shape[1]), 0)
        return jnp.where(rows == key, 1.0, 0.0).astype(BF16)

    rim_bin = bin_row - 1 + lax.shift_right_logical(row, 1)
    outside = jnp.where(il == 0, n_pairs, -1)
    rim_code = jnp.where(rim_bin == outside, n_pairs, jnp.where((rim_bin < 0) | (rim_bin >= n_pairs), -1, rim_bin))
    for load in edge_loads:
        load.wait()
    for d, (start, column) in enumerate(((n_cols - 8, own_cols), (0, -1))):
        target = jnp.where(bin_col == column, rim_code, -1)
        key = jnp.concatenate([target[i: i + 1, start: start + 8] for i in range(n_rows)], axis=1)
        chosen = one_hot(key, n_pairs + 8)
        high, low = halves(edge_x[d].reshape(n_rows * 8, span))
        sums = dot(chosen, high) + dot(chosen, low)
        folds = dot(chosen, jnp.ones((n_rows * 8, LANES), BF16))
        ends = jnp.where(is_first, sums[:, :LANES], jnp.where(is_last, sums[:, span - LANES:], folds))
        rim_send[d, :, :span] = sums[:n_pairs]
        rim_send[d, :, span:] = ends[:n_pairs]
        corner_send[d, :, :span] = sums[n_pairs: n_pairs + 1]
        corner_send[d, :, span:] = ends[n_pairs: n_pairs + 1]

    for p in range(n_pairs):
        key = jnp.concatenate([keys[0, 2 * p: 2 * p + 1], keys[0, 2 * p + 1: 2 * p + 2]], axis=1)
        hot_a[p] = one_hot(key, 3 * ranges[0][3])
        second = keys[2, 2 * p + 1: 2 * p + 2]
        key = jnp.concatenate([jnp.where(lane < rest, keys[1, 2 * p: 2 * p + 1], second),
                               second[:, :2 * rest - LANES]], axis=1)
        hot_b[p] = one_hot(key, 3 * ranges[1][3])
    hots = (hot_a, hot_b)

    def merge(p, parts, lanes):
        (_, _, _, height), (_, _, first, rest_height) = ranges
        for r in range(3):
            a = parts[0][r * height: (r + 1) * height]
            b = parts[1][r * rest_height: (r + 1) * rest_height]
            both = a[first:] + b[: height - first]
            for at, part in ((0, a[:first]), (first, both), (height, b[height - first:])):
                where = (p + r, slice(at, at + part.shape[0]), lanes)
                acc[where] = part if p == 0 or r == 2 else acc[where] + part

    def bin_pair(p, x, lanes):
        parts, wide = [], x.shape[2]
        for hot, (start, stop, _, _) in zip(hots, ranges):
            high, low = halves(jnp.concatenate([x[2 * p, start:stop], x[2 * p + 1, start:stop]], axis=0))
            sums = dot(hot[p], jnp.concatenate([high, low], axis=1))
            parts.append(sums[:, :wide] + sums[:, wide:])
        merge(p, parts, lanes)

    def count_pair(p):
        parts = [dot(hot[p], jnp.ones((hot.shape[2], LANES), BF16)) for hot in hots]
        merge(p, parts, slice(span, span + LANES))

    def remote(src, dst, slot, partner):
        return pltpu.make_async_remote_copy(src_ref=src, dst_ref=dst, send_sem=send_sem.at[slot],
                                            recv_sem=recv_sem.at[slot], device_id=partner, device_id_type=MESH)

    rim_row = jnp.where(il == 0, n_pairs + 1, 0)
    own_row = jnp.where(il == 0, n_pairs - 1, 0)
    to_other = remote(acc.at[rim_row], il_recv, 0, {"il": other})
    rims, halos, diags = [], [], {}
    for d in range(2):
        rims.append((remote(rim_send.at[d], rim_recv.at[d], 1 + d, {"xl": xl_at[d]}),
                     remote(corner_send.at[d], corner_recv.at[d], 3 + d, {"il": other, "xl": xl_at[d]})))
        halos.append((remote(halo_send.at[d], halo_recv.at[d], 5 + d, {"ta": ta_at[d]}),
                      remote(halo_rim.at[d], halo_rim_recv.at[d], 7 + d, {"il": other, "ta": ta_at[d]})))
        for e in range(2):
            to, end = {"xl": xl_at[d], "ta": ta_at[e]}, pl.ds(span, LANES)
            diags[d, e] = (remote(rim_send.at[d, :, end], diag_recv.at[d, e], 9 + 2 * d + e, to),
                           remote(corner_send.at[d, :, end], diag_corner.at[d, e], 13 + 2 * d + e, {"il": other, **to}))

    def start_all(copies):
        for copy in copies:
            copy.start()

    def pack_halo(e):
        lanes = slice(0, LANES) if e else slice(span - LANES, span)
        rows = slice(0, REACH) if e else slice(LANES - REACH, LANES)
        for b in range(n_pairs):
            halo_send[e, b, :, :own_cols] = acc[b + 1, :, lanes].T[rows]
        halo_rim[e, :, :own_cols] = acc[rim_row, :, lanes].T[rows]

    pl.semaphore_wait(barrier, peers)
    for d in range(2):
        def go(d=d):
            start_all(rims[d])
            for e in range(2):
                when(has_ta[e], lambda e=e: start_all(diags[d, e]))
        when(has_xl[d], go)
    for load in left_loads:
        load.wait()
    for p in range(n_pairs):
        bin_pair(p, x_left, slice(0, LANES))
    pack_halo(1)
    when(has_ta[1], lambda: start_all(halos[1]))
    for load in right_loads:
        load.wait()
    for p in range(n_pairs):
        bin_pair(p, x_right, slice(LANES, span))
    pack_halo(0)
    when(has_ta[0], lambda: start_all(halos[0]))
    for p in range(n_pairs):
        count_pair(p)
    to_other.start()

    def resample(values):
        high, low = halves(values)
        return dot(high, t_high[...]) + (dot(low, t_high[...]) + dot(high, t_low[...]))

    for load in table_loads:
        load.wait()
    for i in range(n_pairs):
        b = jnp.where(il == 0, i, n_pairs - 1 - i)
        if i == n_pairs - 1:
            to_other.wait_recv()
            acc[b + 1] = acc[b + 1] + il_recv[...]
        main[b] = resample(acc[b + 1, :, :span])
    for d in range(2):
        def arrived(d=d):
            for copy in rims[d]:
                copy.wait_recv()
        when(has_xl[1 - d], arrived)
    sub = lax.broadcasted_iota(jnp.int32, (n_pairs, 1), 0)
    rim = jnp.concatenate([rim_recv[d] + jnp.where(sub == own_row, corner_recv[d], 0.0) for d in range(2)], axis=0)
    more = resample(rim[:, :span])
    more_fold = jnp.broadcast_to(rim[:, span + LANES // 2: span + LANES // 2 + 1], (2 * n_pairs, LANES))
    ends_row = lax.broadcasted_iota(jnp.int32, (8, 1), 0)
    tops = ((0, 0, 0), (own_cols - 8, 7, n_pairs))

    def add_rows(values, extra, b):
        top, bottom = [values[at: at + 8] + jnp.where(ends_row == where, extra[base + b: base + b + 1], 0.0)
                       for at, where, base in tops]
        return jnp.concatenate([top, values[8: own_cols - 8], bottom], axis=0)

    for b in range(n_pairs):
        scale = 1.0 / jnp.maximum(add_rows(acc[b + 1, :, span:], more_fold, b), 1.0)
        factor[b] = scale
        main[b] = add_rows(main[b], more, b) * jnp.concatenate([scale] * (main.shape[2] // LANES), axis=1)

    for d in range(2):
        for e in range(2):
            def diag_arrived(d=d, e=e):
                for copy in diags[d, e]:
                    copy.wait_recv()
            when(has_xl[1 - d] & has_ta[1 - e], diag_arrived)
    for d in range(2):
        first, last = [diag_recv[d, e] + jnp.where(sub == own_row, diag_corner[d, e], 0.0) for e in (1, 0)]
        rim_out[d * n_pairs: (d + 1) * n_pairs] = jnp.where(is_first, first, jnp.where(is_last, last, 0.0))
    for e in range(2):
        def halo_arrived(e=e):
            for copy in halos[e]:
                copy.wait_recv()
        when(has_ta[1 - e], halo_arrived)
        halo_out[e] = halo_recv[e]
        halo_out[e, own_row] = halo_recv[e, own_row] + halo_rim_recv[e]
    to_other.wait_send()
    for d in range(2):
        def sent(d=d):
            for copy in rims[d]:
                copy.wait_send()
            for e in range(2):
                def diag_sent(d=d, e=e):
                    for copy in diags[d, e]:
                        copy.wait_send()
                when(has_ta[e], diag_sent)
        when(has_xl[d], sent)

        def halo_sent(d=d):
            for copy in halos[d]:
                copy.wait_send()
        when(has_ta[d], halo_sent)


def finish(main, factor, halo, rim, t_edge, t_rim, out, staged, out_sem):
    n_pairs, own_cols, width = main.shape
    inner = pl.ds(LANES, width - 2 * LANES)
    writes = [pltpu.make_async_copy(main.at[:, :, inner], out.at[:, :, inner], out_sem.at[n_pairs, 0])]
    writes[0].start()
    high = rim[...].astype(BF16)
    low = (rim[...] - high.astype(F32)).astype(BF16)
    more = dot(jnp.concatenate([high, low, high], axis=1), t_rim[...])
    ends_row = lax.broadcasted_iota(jnp.int32, (8, 1), 0)
    tops = ((0, 0, 0), (own_cols - 8, 7, n_pairs))
    for b in range(n_pairs):
        edges = jnp.concatenate([halo[0, b], halo[1, b]], axis=0)
        high = edges.astype(BF16).astype(F32)
        terms = jnp.concatenate([high, edges - high, high], axis=0).T[:own_cols].astype(BF16)
        ends = dot(terms, t_edge[...])
        top, bottom = [ends[at: at + 8] + jnp.where(ends_row == where, more[base + b: base + b + 1], 0.0)
                       for at, where, base in tops]
        ends = jnp.concatenate([top, ends[8: own_cols - 8], bottom], axis=0)
        for d, start in enumerate((0, width - LANES)):
            staged[b, d] = main[b, :, start: start + LANES] + ends[:, d * LANES: (d + 1) * LANES] * factor[b]
            write = pltpu.make_async_copy(staged.at[b, d], out.at[b, :, pl.ds(start, LANES)], out_sem.at[b, d])
            write.start()
            writes.append(write)
    for write in writes:
        write.wait()


def shards(n_xl, n_ta, traces, bin_steps):
    n_rows, n_cols, span = traces.shape
    n_pairs, own_cols = n_rows // 2, n_cols // 2
    width = span + LANES
    out_span = span * P_SIZE // Q
    if n_pairs % 8 or span % LANES or out_span % LANES or out_span < 3 * LANES:
        raise ValueError("block shape")
    table = lanczos_table(span)
    t_high, t_low = split_table(table[REACH:-REACH])
    edge_cols = np.concatenate([table[:, :LANES], table[:, -LANES:]], axis=1)
    edge_high, edge_low = split_table(np.concatenate([edge_cols[:REACH], edge_cols[-REACH:]]))
    t_edge = np.concatenate([edge_high, edge_high, edge_low])
    rim_high, rim_low = split_table(np.concatenate(
        [edge_cols[-REACH:], np.zeros((LANES - 2 * REACH, 2 * LANES), np.float32), edge_cols[:REACH]]))
    t_rim = np.concatenate([rim_high, rim_high, rim_low])
    vmem = pl.BlockSpec(memory_space=pltpu.VMEM)
    hbm = pl.BlockSpec(memory_space=pltpu.HBM)
    (start_a, stop_a, _, height_a), (start_b, stop_b, _, height_b) = column_ranges(n_cols)
    main, factor, halo, rim = pl.pallas_call(
        functools.partial(binning, n_xl, n_ta),
        out_shape=(pltpu.VMEM((n_pairs, own_cols, out_span), F32), pltpu.VMEM((n_pairs, own_cols, LANES), F32),
                   pltpu.VMEM((2, n_pairs, REACH, LANES), F32), pltpu.VMEM((2 * n_pairs, LANES), F32)),
        in_specs=[hbm] * 4,
        out_specs=[vmem] * 4,
        scratch_shapes=[
            pltpu.VMEM((n_rows, n_cols, LANES), F32),
            pltpu.VMEM((n_rows, n_cols, span - LANES), F32),
            pltpu.VMEM((2, n_rows, 8, span), F32),
            pltpu.VMEM((2, n_rows, n_cols), jnp.int32),
            pltpu.VMEM(t_high.shape, BF16),
            pltpu.VMEM(t_low.shape, BF16),
            pltpu.VMEM((3, n_rows, LANES), jnp.int32),
            pltpu.VMEM((n_pairs, 3 * height_a, 2 * (stop_a - start_a)), BF16),
            pltpu.VMEM((n_pairs, 3 * height_b, 2 * (stop_b - start_b)), BF16),
            pltpu.VMEM((n_pairs + 2, own_cols, width), F32),
            pltpu.VMEM((2, n_pairs, width), F32),
            pltpu.VMEM((2, 1, width), F32),
            pltpu.VMEM((2, n_pairs, width), F32),
            pltpu.VMEM((2, 1, width), F32),
            pltpu.VMEM((own_cols, width), F32),
            pltpu.VMEM((2, n_pairs, REACH, LANES), F32),
            pltpu.VMEM((2, REACH, LANES), F32),
            pltpu.VMEM((2, n_pairs, REACH, LANES), F32),
            pltpu.VMEM((2, REACH, LANES), F32),
            pltpu.VMEM((2, 2, n_pairs, LANES), F32),
            pltpu.VMEM((2, 2, 1, LANES), F32),
            pltpu.SemaphoreType.DMA((n_pairs,)),
            pltpu.SemaphoreType.DMA((n_pairs,)),
            pltpu.SemaphoreType.DMA((2,)),
            pltpu.SemaphoreType.DMA((3,)),
            pltpu.SemaphoreType.DMA((17,)),
            pltpu.SemaphoreType.DMA((17,)),
        ],
        compiler_params=pltpu.CompilerParams(collective_id=0, has_side_effects=True, vmem_limit_bytes=24 * 2**20),
        name="binning",
    )(*[pltpu.with_memory_space_constraint(a, pltpu.HBM) for a in (traces, bin_steps, jnp.asarray(t_high), jnp.asarray(t_low))])
    return pl.pallas_call(
        finish,
        out_shape=jax.ShapeDtypeStruct((n_pairs, own_cols, out_span), F32),
        in_specs=[vmem] * 6,
        out_specs=hbm,
        scratch_shapes=[pltpu.VMEM((n_pairs, 2, own_cols, LANES), F32), pltpu.SemaphoreType.DMA((n_pairs + 1, 2))],
        compiler_params=pltpu.CompilerParams(vmem_limit_bytes=16 * 2**20),
        name="finish",
    )(main, factor, halo, rim, jnp.asarray(t_edge), jnp.asarray(t_rim))


def solution(mesh):
    if mesh.shape["il"] != 2:
        raise ValueError("il size")
    return jax.shard_map(
        functools.partial(shards, mesh.shape["xl"], mesh.shape["ta"]),
        mesh=mesh,
        in_specs=(P("il", "xl", "ta"), P(None, "il", "xl")),
        out_specs=P("il", "xl", "ta"),
        check_vma=False,
    )
```

```python
import functools

import numpy as np
import jax
import jax.numpy as jnp
from jax import lax
from jax.experimental import pallas as pl
from jax.experimental.pallas import tpu as pltpu
from jax.sharding import PartitionSpec as P

TAPS = 16
P_SIZE = 3
Q = 2
REACH = TAPS // 2
LANES = 128
EARLY = 2
MESH = pl.DeviceIdType.MESH
F32, BF16 = jnp.float32, jnp.bfloat16


def lanczos_table(span):
    rows = np.arange(span + 2 * REACH)[:, None] - REACH
    cols = np.arange(span * P_SIZE // Q)[None, :]
    offset = (cols * Q - rows * P_SIZE).astype(np.float64) / P_SIZE
    weights = np.sinc(offset) * np.sinc(offset / REACH)
    return np.where(np.abs(offset) < REACH, weights, 0.0).astype(np.float32)


def split_table(table):
    high = table.astype(BF16)
    low = (table - high.astype(np.float32)).astype(BF16)
    return high, low


def halves(values):
    high = values.astype(BF16)
    low = (values - high.astype(F32)).astype(BF16)
    return high, low


def dot(a, b):
    return jnp.dot(a, b, preferred_element_type=F32)


def column_ranges(n_cols):
    own_cols, rest = n_cols // 2, n_cols - LANES
    if own_cols % 8 or rest % 16 or not LANES < 2 * rest <= 2 * LANES:
        raise ValueError("column count")
    height = (LANES // 2 + 1 + 7) // 8 * 8
    first = (LANES // 2 - 1) // 8 * 8
    return (0, LANES, 0, height), (LANES, n_cols, first, own_cols - first)


def binning(n_xl, n_ta, traces, steps_hbm, tables_hbm, main, factor, halo_out, rim_out,
            x_left, x_right, edge_x, steps, tables, keys, hot_a, hot_b, acc,
            rim_send, corner_send, rim_recv, corner_recv, il_recv, halo_send, halo_rim, halo_recv, halo_rim_recv,
            diag_recv, diag_corner, load_sem, late_sem, send_sem, recv_sem):
    n_rows, n_cols, _ = x_left.shape
    span = LANES + x_right.shape[2]
    n_pairs, own_cols = n_rows // 2, n_cols // 2
    il, xl, ta = lax.axis_index("il"), lax.axis_index("xl"), lax.axis_index("ta")
    other = 1 - il
    has_xl, has_ta = (xl < n_xl - 1, xl > 0), (ta < n_ta - 1, ta > 0)
    xl_at, ta_at = (xl + 1, xl - 1), (ta + 1, ta - 1)
    ranges = column_ranges(n_cols)

    def when(condition, work):
        pl.when(condition)(work)

    step_load = pltpu.make_async_copy(steps_hbm, steps, load_sem.at[3])
    step_load.start()
    edge_loads = [pltpu.make_async_copy(traces.at[:, pl.ds(start, 8)], edge_x.at[d], load_sem.at[4 + d])
                  for d, start in enumerate((n_cols - 8, 0))]
    for load in edge_loads:
        load.start()

    def load_samples(x, start, rows, slot):
        samples = pl.ds(start, x.shape[2])
        return pltpu.make_async_copy(traces.at[rows, :, samples], x.at[rows], load_sem.at[slot])

    table_load = pltpu.make_async_copy(tables_hbm, tables, load_sem.at[2])

    barrier = pltpu.get_barrier_semaphore()

    def greet(has, partner, semaphore=barrier):
        def signal():
            pl.semaphore_signal(semaphore, inc=1, device_id=partner, device_id_type=MESH)
            pl.semaphore_signal(semaphore, inc=1, device_id={"il": other, **partner}, device_id_type=MESH)
        when(has, signal)

    pl.semaphore_signal(barrier, inc=1, device_id={"il": other}, device_id_type=MESH)
    for d in range(2):
        greet(has_xl[0] & has_ta[d], {"xl": xl + 1, "ta": ta_at[d]})
    for d in range(2):
        greet(has_xl[d], {"xl": xl_at[d]})
        greet(has_ta[d], {"ta": ta_at[d]})
    count_xl, count_ta = [sum(jnp.where(has, 1, 0) for has in pair) for pair in (has_xl, has_ta)]
    peers = 1 + 2 * (count_xl + count_ta + jnp.where(has_xl[1], count_ta, 0))
    for p in range(n_pairs):
        load_samples(x_left, 0, pl.ds(2 * p, 2), 0).start()

    for e in range(2):
        def no_ta(e=e):
            halo_recv[e] = jnp.zeros_like(halo_recv[e])
            halo_rim_recv[e] = jnp.zeros_like(halo_rim_recv[e])
        when(jnp.logical_not(has_ta[1 - e]), no_ta)
    for d in range(2):
        def no_xl(d=d):
            rim_recv[d] = jnp.zeros_like(rim_recv[d])
            corner_recv[d] = jnp.zeros_like(corner_recv[d])
        when(jnp.logical_not(has_xl[1 - d]), no_xl)
        for e in range(2):
            def no_diag(d=d, e=e):
                diag_recv[d, e] = jnp.zeros_like(diag_recv[d, e])
                diag_corner[d, e] = jnp.zeros_like(diag_corner[d, e])
            when(jnp.logical_not(has_xl[1 - d] & has_ta[1 - e]), no_diag)

    lane = lax.broadcasted_iota(jnp.int32, (1, LANES), 1)
    is_first, is_last = lane < REACH, lane >= LANES - REACH
    step_load.wait()
    col = lax.broadcasted_iota(jnp.int32, (n_rows, n_cols), 1)
    row = lax.broadcasted_iota(jnp.int32, (n_rows, n_cols), 0)
    bin_col = lax.shift_right_logical(col, 1) + steps[1]
    bin_row = steps[0] + 1
    own = (bin_col >= 0) & (bin_col < own_cols)
    code_a, code_b = [jnp.where(own, bin_row * height + bin_col - first, -1)[:, start:stop]
                      for start, stop, first, height in ranges]
    rest = n_cols - LANES
    keys[0] = code_a
    padded = jnp.concatenate([code_b, jnp.full((n_rows, LANES - rest), -1, jnp.int32)], axis=1)
    keys[1] = padded
    keys[2] = pltpu.roll(padded, rest, 1)

    def one_hot(key, height):
        rows = lax.broadcasted_iota(jnp.int32, (height, key.shape[1]), 0)
        return jnp.where(rows == key, 1.0, 0.0).astype(BF16)

    rim_bin = bin_row - 1 + lax.shift_right_logical(row, 1)
    outside = jnp.where(il == 0, n_pairs, -1)
    rim_code = jnp.where(rim_bin == outside, n_pairs, jnp.where((rim_bin < 0) | (rim_bin >= n_pairs), -1, rim_bin))
    for load in edge_loads:
        load.wait()
    for d, (start, column) in enumerate(((n_cols - 8, own_cols), (0, -1))):
        target = jnp.where(bin_col == column, rim_code, -1)
        key = jnp.concatenate([target[i: i + 1, start: start + 8] for i in range(n_rows)], axis=1)
        chosen = one_hot(key, n_pairs + 8)
        high, low = halves(edge_x[d].reshape(n_rows * 8, span))
        sums = dot(chosen, high) + dot(chosen, low)
        folds = dot(chosen, jnp.ones((n_rows * 8, LANES), BF16))
        ends = jnp.where(is_first, sums[:, :LANES], jnp.where(is_last, sums[:, span - LANES:], folds))
        rim_send[d, :, :span] = sums[:n_pairs]
        rim_send[d, :, span:] = ends[:n_pairs]
        corner_send[d, :, :span] = sums[n_pairs: n_pairs + 1]
        corner_send[d, :, span:] = ends[n_pairs: n_pairs + 1]

    for p in range(n_pairs):
        load_samples(x_right, LANES, pl.ds(2 * p, 2), 1).start()
    table_load.start()
    for p in range(n_pairs):
        key = jnp.concatenate([keys[0, 2 * p: 2 * p + 1], keys[0, 2 * p + 1: 2 * p + 2]], axis=1)
        hot_a[p] = one_hot(key, 3 * ranges[0][3])
        second = keys[2, 2 * p + 1: 2 * p + 2]
        key = jnp.concatenate([jnp.where(lane < rest, keys[1, 2 * p: 2 * p + 1], second),
                               second[:, :2 * rest - LANES]], axis=1)
        hot_b[p] = one_hot(key, 3 * ranges[1][3])
    hots = (hot_a, hot_b)

    def merge(p, parts, lanes):
        (_, _, _, height), (_, _, first, rest_height) = ranges
        for r in range(3):
            a = parts[0][r * height: (r + 1) * height]
            b = parts[1][r * rest_height: (r + 1) * rest_height]
            both = a[first:] + b[: height - first]
            for at, part in ((0, a[:first]), (first, both), (height, b[height - first:])):
                where = (p + r, slice(at, at + part.shape[0]), lanes)
                acc[where] = part if p == 0 or r == 2 else acc[where] + part

    def bin_pair(p, x, lanes):
        parts, wide = [], x.shape[2]
        for hot, (start, stop, _, _) in zip(hots, ranges):
            high, low = halves(jnp.concatenate([x[2 * p, start:stop], x[2 * p + 1, start:stop]], axis=0))
            sums = dot(hot[p], jnp.concatenate([high, low], axis=1))
            parts.append(sums[:, :wide] + sums[:, wide:])
        merge(p, parts, lanes)

    def count_pair(p):
        parts = [dot(hot[p], jnp.ones((hot.shape[2], LANES), BF16)) for hot in hots]
        merge(p, parts, slice(span, span + LANES))

    def remote(src, dst, slot, partner):
        return pltpu.make_async_remote_copy(src_ref=src, dst_ref=dst, send_sem=send_sem.at[slot],
                                            recv_sem=recv_sem.at[slot], device_id=partner, device_id_type=MESH)

    rim_row = jnp.where(il == 0, n_pairs + 1, 0)
    own_row = jnp.where(il == 0, n_pairs - 1, 0)
    to_other = remote(acc.at[rim_row], il_recv, 0, {"il": other})
    rims, halos, diags = [], [], {}
    for d in range(2):
        rims.append((remote(rim_send.at[d], rim_recv.at[d], 1 + d, {"xl": xl_at[d]}),
                     remote(corner_send.at[d], corner_recv.at[d], 3 + d, {"il": other, "xl": xl_at[d]})))
        halos.append((remote(halo_send.at[d], halo_recv.at[d], 5 + d, {"ta": ta_at[d]}),
                      remote(halo_rim.at[d], halo_rim_recv.at[d], 7 + d, {"il": other, "ta": ta_at[d]})))
        for e in range(2):
            to, end = {"xl": xl_at[d], "ta": ta_at[e]}, pl.ds(span, LANES)
            diags[d, e] = (remote(rim_send.at[d, :, end], diag_recv.at[d, e], 9 + 2 * d + e, to),
                           remote(corner_send.at[d, :, end], diag_corner.at[d, e], 13 + 2 * d + e, {"il": other, **to}))

    def start_all(copies):
        for copy in copies:
            copy.start()

    def pack_halo(e):
        lanes = slice(0, LANES) if e else slice(span - LANES, span)
        rows = slice(0, REACH) if e else slice(LANES - REACH, LANES)
        for b in range(n_pairs):
            halo_send[e, b, :, :own_cols] = acc[b + 1, :, lanes].T[rows]
        halo_rim[e, :, :own_cols] = acc[rim_row, :, lanes].T[rows]

    def send_diags(d):
        for e in (1, 0):
            when(has_ta[e], lambda e=e: start_all(diags[d, e]))

    def send_rims(d):
        send_diags(d)
        start_all(rims[d])

    every_row = pl.ds(0, n_rows)
    load_samples(x_left, 0, every_row, 0).wait()
    for p in range(EARLY):
        bin_pair(p, x_left, slice(0, LANES))
    pl.semaphore_wait(barrier, peers)
    for e in range(2):
        greet(has_ta[e], {"ta": ta_at[e]}, late_sem)
    when(has_xl[1], lambda: send_rims(1))
    when(has_xl[0], lambda: start_all(rims[0]))
    for p in range(EARLY, n_pairs):
        bin_pair(p, x_left, slice(0, LANES))
    pack_halo(1)
    when(has_ta[1], lambda: start_all(halos[1]))
    load_samples(x_right, LANES, every_row, 1).wait()
    for p in range(n_pairs // 2):
        bin_pair(p, x_right, slice(LANES, span))

    def late():
        pl.semaphore_wait(late_sem, 2 * count_ta)
        when(has_xl[0], lambda: send_diags(0))

    first = (xl == 0) & (ta == 0)
    when(jnp.logical_not(first), late)
    for p in range(n_pairs // 2, n_pairs):
        bin_pair(p, x_right, slice(LANES, span))
    pack_halo(0)
    when(has_ta[0], lambda: start_all(halos[0]))
    for p in range(n_pairs):
        count_pair(p)
    to_other.start()
    when(first, late)

    def resample(values):
        high, low = halves(values)
        return dot(high, tables[0]) + (dot(low, tables[0]) + dot(high, tables[1]))

    table_load.wait()
    for i in range(n_pairs):
        b = jnp.where(il == 0, i, n_pairs - 1 - i)
        if i == n_pairs - 1:
            to_other.wait_recv()
            acc[b + 1] = acc[b + 1] + il_recv[...]
        main[b] = resample(acc[b + 1, :, :span])
    for d in range(2):
        def arrived(d=d):
            for copy in rims[d]:
                copy.wait_recv()
        when(has_xl[1 - d], arrived)
    sub = lax.broadcasted_iota(jnp.int32, (n_pairs, 1), 0)
    rim = jnp.concatenate([rim_recv[d] + jnp.where(sub == own_row, corner_recv[d], 0.0) for d in range(2)], axis=0)
    more = resample(rim[:, :span])
    more_fold = jnp.broadcast_to(rim[:, span + LANES // 2: span + LANES // 2 + 1], (2 * n_pairs, LANES))
    ends_row = lax.broadcasted_iota(jnp.int32, (8, 1), 0)
    tops = ((0, 0, 0), (own_cols - 8, 7, n_pairs))

    def add_rows(values, extra, b):
        top, bottom = [values[at: at + 8] + jnp.where(ends_row == where, extra[base + b: base + b + 1], 0.0)
                       for at, where, base in tops]
        return jnp.concatenate([top, values[8: own_cols - 8], bottom], axis=0)

    for b in range(n_pairs):
        scale = 1.0 / jnp.maximum(add_rows(acc[b + 1, :, span:], more_fold, b), 1.0)
        factor[b] = scale
        main[b] = add_rows(main[b], more, b) * jnp.concatenate([scale] * (main.shape[2] // LANES), axis=1)

    for d in range(2):
        for e in range(2):
            def diag_arrived(d=d, e=e):
                for copy in diags[d, e]:
                    copy.wait_recv()
            when(has_xl[1 - d] & has_ta[1 - e], diag_arrived)
    for d in range(2):
        first, last = [diag_recv[d, e] + jnp.where(sub == own_row, diag_corner[d, e], 0.0) for e in (1, 0)]
        rim_out[d * n_pairs: (d + 1) * n_pairs] = jnp.where(is_first, first, jnp.where(is_last, last, 0.0))
    for e in range(2):
        def halo_arrived(e=e):
            for copy in halos[e]:
                copy.wait_recv()
        when(has_ta[1 - e], halo_arrived)
        halo_out[e] = halo_recv[e]
        halo_out[e, own_row] = halo_recv[e, own_row] + halo_rim_recv[e]
    to_other.wait_send()
    for d in range(2):
        def sent(d=d):
            for copy in rims[d]:
                copy.wait_send()
            for e in range(2):
                def diag_sent(d=d, e=e):
                    for copy in diags[d, e]:
                        copy.wait_send()
                when(has_ta[e], diag_sent)
        when(has_xl[d], sent)

        def halo_sent(d=d):
            for copy in halos[d]:
                copy.wait_send()
        when(has_ta[d], halo_sent)


def finish(main, factor, halo, rim, t_edge, t_rim, out, staged, out_sem):
    n_pairs, own_cols, width = main.shape
    inner = pl.ds(LANES, width - 2 * LANES)
    writes = [pltpu.make_async_copy(main.at[:, :, inner], out.at[:, :, inner], out_sem.at[0])]
    writes[0].start()
    high = rim[...].astype(BF16)
    low = (rim[...] - high.astype(F32)).astype(BF16)
    more = dot(jnp.concatenate([high, low, high], axis=1), t_rim[...])
    ends_row = lax.broadcasted_iota(jnp.int32, (8, 1), 0)
    tops = ((0, 0, 0), (own_cols - 8, 7, n_pairs))
    for b in range(n_pairs):
        edges = jnp.concatenate([halo[0, b], halo[1, b]], axis=0)
        high = edges.astype(BF16).astype(F32)
        terms = jnp.concatenate([high, edges - high, high], axis=0).T[:own_cols].astype(BF16)
        ends = dot(terms, t_edge[...])
        top, bottom = [ends[at: at + 8] + jnp.where(ends_row == where, more[base + b: base + b + 1], 0.0)
                       for at, where, base in tops]
        ends = jnp.concatenate([top, ends[8: own_cols - 8], bottom], axis=0)
        for d, start in enumerate((0, width - LANES)):
            staged[b, d] = main[b, :, start: start + LANES] + ends[:, d * LANES: (d + 1) * LANES] * factor[b]
            write = pltpu.make_async_copy(staged.at[b, d], out.at[b, :, pl.ds(start, LANES)], out_sem.at[1])
            write.start()
    writes[0].wait()
    for d, start in enumerate((0, width - LANES)):
        pltpu.make_async_copy(staged.at[:, d], out.at[:, :, pl.ds(start, LANES)], out_sem.at[1]).wait()


def shards(n_xl, n_ta, traces, bin_steps):
    n_rows, n_cols, span = traces.shape
    n_pairs, own_cols = n_rows // 2, n_cols // 2
    width = span + LANES
    out_span = span * P_SIZE // Q
    if n_pairs % 8 or span % LANES or out_span % LANES or out_span < 3 * LANES:
        raise ValueError("block shape")
    table = lanczos_table(span)
    tables = np.stack(split_table(table[REACH:-REACH]))
    edge_cols = np.concatenate([table[:, :LANES], table[:, -LANES:]], axis=1)
    edge_high, edge_low = split_table(np.concatenate([edge_cols[:REACH], edge_cols[-REACH:]]))
    t_edge = np.concatenate([edge_high, edge_high, edge_low])
    rim_high, rim_low = split_table(np.concatenate(
        [edge_cols[-REACH:], np.zeros((LANES - 2 * REACH, 2 * LANES), np.float32), edge_cols[:REACH]]))
    t_rim = np.concatenate([rim_high, rim_high, rim_low])
    vmem = pl.BlockSpec(memory_space=pltpu.VMEM)
    hbm = pl.BlockSpec(memory_space=pltpu.HBM)
    (start_a, stop_a, _, height_a), (start_b, stop_b, _, height_b) = column_ranges(n_cols)
    main, factor, halo, rim = pl.pallas_call(
        functools.partial(binning, n_xl, n_ta),
        out_shape=(pltpu.VMEM((n_pairs, own_cols, out_span), F32), pltpu.VMEM((n_pairs, own_cols, LANES), F32),
                   pltpu.VMEM((2, n_pairs, REACH, LANES), F32), pltpu.VMEM((2 * n_pairs, LANES), F32)),
        in_specs=[hbm] * 3,
        out_specs=[vmem] * 4,
        scratch_shapes=[
            pltpu.VMEM((n_rows, n_cols, LANES), F32),
            pltpu.VMEM((n_rows, n_cols, span - LANES), F32),
            pltpu.VMEM((2, n_rows, 8, span), F32),
            pltpu.VMEM((2, n_rows, n_cols), jnp.int32),
            pltpu.VMEM(tables.shape, BF16),
            pltpu.VMEM((3, n_rows, LANES), jnp.int32),
            pltpu.VMEM((n_pairs, 3 * height_a, 2 * (stop_a - start_a)), BF16),
            pltpu.VMEM((n_pairs, 3 * height_b, 2 * (stop_b - start_b)), BF16),
            pltpu.VMEM((n_pairs + 2, own_cols, width), F32),
            pltpu.VMEM((2, n_pairs, width), F32),
            pltpu.VMEM((2, 1, width), F32),
            pltpu.VMEM((2, n_pairs, width), F32),
            pltpu.VMEM((2, 1, width), F32),
            pltpu.VMEM((own_cols, width), F32),
            pltpu.VMEM((2, n_pairs, REACH, LANES), F32),
            pltpu.VMEM((2, REACH, LANES), F32),
            pltpu.VMEM((2, n_pairs, REACH, LANES), F32),
            pltpu.VMEM((2, REACH, LANES), F32),
            pltpu.VMEM((2, 2, n_pairs, LANES), F32),
            pltpu.VMEM((2, 2, 1, LANES), F32),
            pltpu.SemaphoreType.DMA((6,)),
            pltpu.SemaphoreType.REGULAR,
            pltpu.SemaphoreType.DMA((17,)),
            pltpu.SemaphoreType.DMA((17,)),
        ],
        compiler_params=pltpu.CompilerParams(collective_id=0, has_side_effects=True, vmem_limit_bytes=24 * 2**20),
        name="binning",
    )(*[pltpu.with_memory_space_constraint(a, pltpu.HBM) for a in (traces, bin_steps, jnp.asarray(tables))])
    return pl.pallas_call(
        finish,
        out_shape=jax.ShapeDtypeStruct((n_pairs, own_cols, out_span), F32),
        in_specs=[vmem] * 6,
        out_specs=hbm,
        scratch_shapes=[pltpu.VMEM((n_pairs, 2, own_cols, LANES), F32), pltpu.SemaphoreType.DMA((2,))],
        compiler_params=pltpu.CompilerParams(vmem_limit_bytes=16 * 2**20),
        name="finish",
    )(main, factor, halo, rim, jnp.asarray(t_edge), jnp.asarray(t_rim))


def solution(mesh):
    if mesh.shape["il"] != 2:
        raise ValueError("il size")
    return jax.shard_map(
        functools.partial(shards, mesh.shape["xl"], mesh.shape["ta"]),
        mesh=mesh,
        in_specs=(P("il", "xl", "ta"), P(None, "il", "xl")),
        out_specs=P("il", "xl", "ta"),
        check_vma=False,
    )
```

```python
import functools

import numpy as np
import jax
import jax.numpy as jnp
from jax import lax
from jax.experimental import pallas as pl
from jax.experimental.pallas import tpu as pltpu
from jax.sharding import PartitionSpec as P

TAPS = 16
P_SIZE = 3
Q = 2
REACH = TAPS // 2
LANES = 128
MESH = pl.DeviceIdType.MESH
F32, BF16 = jnp.float32, jnp.bfloat16


def lanczos_table(span):
    rows = np.arange(span + 2 * REACH)[:, None] - REACH
    cols = np.arange(span * P_SIZE // Q)[None, :]
    offset = (cols * Q - rows * P_SIZE).astype(np.float64) / P_SIZE
    weights = np.sinc(offset) * np.sinc(offset / REACH)
    return np.where(np.abs(offset) < REACH, weights, 0.0).astype(np.float32)


def split_table(table):
    high = table.astype(BF16)
    low = (table - high.astype(np.float32)).astype(BF16)
    return high, low


def halves(values):
    high = values.astype(BF16)
    low = (values - high.astype(F32)).astype(BF16)
    return high, low


def dot(a, b):
    return jnp.dot(a, b, preferred_element_type=F32)


def column_ranges(n_cols):
    own_cols, rest = n_cols // 2, n_cols - LANES
    if own_cols % 8 or rest % 16 or not LANES < 2 * rest <= 2 * LANES:
        raise ValueError("column count")
    height = (LANES // 2 + 1 + 7) // 8 * 8
    first = (LANES // 2 - 1) // 8 * 8
    return (0, LANES, 0, height), (LANES, n_cols, first, own_cols - first)


def binning(n_xl, n_ta, traces, steps_hbm, tables_hbm, main, factor, halo_out, rim_out,
            x_left, x_right, edge_x, steps, tables, keys, hot_a, hot_b, acc,
            rim_send, corner_send, rim_recv, corner_recv, il_recv, halo_send, halo_recv, wide_rows,
            diag_recv, diag_corner, load_sem, late_sem, send_sem, recv_sem):
    n_rows, n_cols, _ = x_left.shape
    span = LANES + x_right.shape[2]
    n_pairs, own_cols = n_rows // 2, n_cols // 2
    il, xl, ta = lax.axis_index("il"), lax.axis_index("xl"), lax.axis_index("ta")
    other = 1 - il
    has_xl, has_ta = (xl < n_xl - 1, xl > 0), (ta < n_ta - 1, ta > 0)
    xl_at, ta_at = (xl + 1, xl - 1), (ta + 1, ta - 1)
    ranges = column_ranges(n_cols)

    def when(condition, work):
        pl.when(condition)(work)

    step_load = pltpu.make_async_copy(steps_hbm, steps, load_sem.at[3])
    step_load.start()
    edge_loads = [pltpu.make_async_copy(traces.at[:, pl.ds(start, 8)], edge_x.at[d], load_sem.at[4 + d])
                  for d, start in enumerate((n_cols - 8, 0))]
    for load in edge_loads:
        load.start()

    def load_samples(x, start, rows, slot):
        samples = pl.ds(start, x.shape[2])
        return pltpu.make_async_copy(traces.at[rows, :, samples], x.at[rows], load_sem.at[slot])

    table_load = pltpu.make_async_copy(tables_hbm, tables, load_sem.at[2])

    barrier = pltpu.get_barrier_semaphore()

    def greet(has, partner):
        def signal():
            pl.semaphore_signal(barrier, inc=1, device_id=partner, device_id_type=MESH)
            pl.semaphore_signal(barrier, inc=1, device_id={"il": other, **partner}, device_id_type=MESH)
        when(has, signal)

    pl.semaphore_signal(barrier, inc=1, device_id={"il": other}, device_id_type=MESH)
    for d in range(2):
        greet(has_xl[0] & has_ta[d], {"xl": xl + 1, "ta": ta_at[d]})
    for d in range(2):
        greet(has_xl[d], {"xl": xl_at[d]})
        greet(has_ta[d], {"ta": ta_at[d]})
    count_xl, count_ta = [sum(jnp.where(has, 1, 0) for has in pair) for pair in (has_xl, has_ta)]
    peers = 1 + 2 * (count_xl + count_ta + jnp.where(has_xl[1], count_ta, 0))
    for p in range(n_pairs):
        load_samples(x_left, 0, pl.ds(2 * p, 2), 0).start()

    for e in range(2):
        def no_ta(e=e):
            halo_recv[e] = jnp.zeros_like(halo_recv[e])
        when(jnp.logical_not(has_ta[1 - e]), no_ta)
    for d in range(2):
        def no_xl(d=d):
            rim_recv[d] = jnp.zeros_like(rim_recv[d])
            corner_recv[d] = jnp.zeros_like(corner_recv[d])
        when(jnp.logical_not(has_xl[1 - d]), no_xl)
        for e in range(2):
            def no_diag(d=d, e=e):
                diag_recv[d, e] = jnp.zeros_like(diag_recv[d, e])
                diag_corner[d, e] = jnp.zeros_like(diag_corner[d, e])
            when(jnp.logical_not(has_xl[1 - d] & has_ta[1 - e]), no_diag)

    lane = lax.broadcasted_iota(jnp.int32, (1, LANES), 1)
    is_first, is_last = lane < REACH, lane >= LANES - REACH
    step_load.wait()
    col = lax.broadcasted_iota(jnp.int32, (n_rows, n_cols), 1)
    row = lax.broadcasted_iota(jnp.int32, (n_rows, n_cols), 0)
    bin_col = lax.shift_right_logical(col, 1) + steps[1]
    bin_row = steps[0] + 1
    own = (bin_col >= 0) & (bin_col < own_cols)
    code_a, code_b = [jnp.where(own, bin_row * height + bin_col - first, -1)[:, start:stop]
                      for start, stop, first, height in ranges]
    rest = n_cols - LANES
    keys[0] = code_a
    padded = jnp.concatenate([code_b, jnp.full((n_rows, LANES - rest), -1, jnp.int32)], axis=1)
    keys[1] = padded
    keys[2] = pltpu.roll(padded, rest, 1)

    def one_hot(key, height):
        rows = lax.broadcasted_iota(jnp.int32, (height, key.shape[1]), 0)
        return jnp.where(rows == key, 1.0, 0.0).astype(BF16)

    rim_bin = bin_row - 1 + lax.shift_right_logical(row, 1)
    outside = jnp.where(il == 0, n_pairs, -1)
    rim_code = jnp.where(rim_bin == outside, n_pairs, jnp.where((rim_bin < 0) | (rim_bin >= n_pairs), -1, rim_bin))
    for load in edge_loads:
        load.wait()
    for d, (start, column) in enumerate(((n_cols - 8, own_cols), (0, -1))):
        target = jnp.where(bin_col == column, rim_code, -1)
        key = jnp.concatenate([target[i: i + 1, start: start + 8] for i in range(n_rows)], axis=1)
        chosen = one_hot(key, n_pairs + 8)
        high, low = halves(edge_x[d].reshape(n_rows * 8, span))
        sums = dot(chosen, high) + dot(chosen, low)
        folds = dot(chosen, jnp.ones((n_rows * 8, LANES), BF16))
        ends = jnp.where(is_first, sums[:, :LANES], jnp.where(is_last, sums[:, span - LANES:], folds))
        rim_send[d, :, :span] = sums[:n_pairs]
        rim_send[d, :, span:] = ends[:n_pairs]
        corner_send[d, :, :span] = sums[n_pairs: n_pairs + 1]
        corner_send[d, :, span:] = ends[n_pairs: n_pairs + 1]

    for p in range(n_pairs):
        key = jnp.concatenate([keys[0, 2 * p: 2 * p + 1], keys[0, 2 * p + 1: 2 * p + 2]], axis=1)
        hot_a[p] = one_hot(key, 3 * ranges[0][3])
        second = keys[2, 2 * p + 1: 2 * p + 2]
        key = jnp.concatenate([jnp.where(lane < rest, keys[1, 2 * p: 2 * p + 1], second),
                               second[:, :2 * rest - LANES]], axis=1)
        hot_b[p] = one_hot(key, 3 * ranges[1][3])
    hots = (hot_a, hot_b)
    for p in range(n_pairs):
        load_samples(x_right, LANES, pl.ds(2 * p, 2), 1).start()
    table_load.start()

    def merge(p, r, parts, lanes):
        (_, _, _, height), (_, _, first, _) = ranges
        a, b = parts
        both = a[first:] + b[: height - first]
        for at, part in ((0, a[:first]), (first, both), (height, b[height - first:])):
            where = (p + r, slice(at, at + part.shape[0]), lanes)
            acc[where] = part if p == 0 or r == 2 else acc[where] + part

    def groups(parts, r):
        return [part[r * height: (r + 1) * height] for part, (_, _, _, height) in zip(parts, ranges)]

    def bin_pair(p, x, lanes):
        parts, wide = [], x.shape[2]
        for hot, (start, stop, _, _) in zip(hots, ranges):
            high, low = halves(jnp.concatenate([x[2 * p, start:stop], x[2 * p + 1, start:stop]], axis=0))
            sums = dot(hot[p], jnp.concatenate([high, low], axis=1))
            parts.append(sums[:, :wide] + sums[:, wide:])
        for r in range(3):
            merge(p, r, groups(parts, r), lanes)

    ends = (0, 0), (n_pairs - 1, 2)

    def count_pair(p):
        parts = [dot(hot[p], jnp.ones((hot.shape[2], LANES), BF16)) for hot in hots]
        for r in range(3):
            if (p, r) not in ends:
                merge(p, r, groups(parts, r), slice(span, span + LANES))

    def remote(src, dst, slot, partner):
        return pltpu.make_async_remote_copy(src_ref=src, dst_ref=dst, send_sem=send_sem.at[slot],
                                            recv_sem=recv_sem.at[slot], device_id=partner, device_id_type=MESH)

    rim_row = jnp.where(il == 0, n_pairs + 1, 0)
    own_row = jnp.where(il == 0, n_pairs - 1, 0)
    to_other = remote(acc.at[rim_row], il_recv, 0, {"il": other})

    rims, halos, diags = [], [], {}
    for d in range(2):
        to, rows = {"xl": xl_at[d]}, pl.ds(0, n_pairs)
        rims.append((remote(rim_send.at[d], rim_recv.at[d], 1 + d, to),
                     remote(corner_send.at[d], corner_recv.at[d], 1 + d, {"il": other, **to})))
        to = {"ta": ta_at[d]}
        halos.append((remote(halo_send.at[d, rows], halo_recv.at[d, rows], 3 + d, to),
                      remote(halo_send.at[d, n_pairs], halo_recv.at[d, n_pairs], 3 + d, {"il": other, **to})))
        for e in range(2):
            to, end, slot = {"xl": xl_at[d], "ta": ta_at[e]}, pl.ds(span, LANES), 5 + 2 * d + e
            diags[d, e] = (remote(rim_send.at[d, :, end], diag_recv.at[d, e], slot, to),
                           remote(corner_send.at[d, :, end], diag_corner.at[d, e], slot, {"il": other, **to}))

    def wait_all(semaphores, slot, rows):
        pltpu.make_async_copy(rows, rows, semaphores.at[slot]).wait()

    def wait_rims(semaphores, d):
        wait_all(semaphores, 1 + d, wide_rows)

    def wait_halos(semaphores, e):
        wait_all(semaphores, 3 + e, halo_recv.at[e])

    def wait_diags(semaphores, d, e):
        wait_all(semaphores, 5 + 2 * d + e, wide_rows.at[:, :, pl.ds(0, LANES)])

    def start_all(copies):
        for copy in copies:
            copy.start()

    def pack_halo(e):
        lanes = slice(0, LANES) if e else slice(span - LANES, span)
        rows = slice(0, REACH) if e else slice(LANES - REACH, LANES)
        for b in range(n_pairs):
            halo_send[e, b, :, :own_cols] = acc[b + 1, :, lanes].T[rows]
        halo_send[e, n_pairs, :, :own_cols] = acc[rim_row, :, lanes].T[rows]

    def send_diags(d):
        for e in (1, 0):
            when(has_ta[e], lambda e=e: start_all(diags[d, e]))

    def send_rims(d):
        send_diags(d)
        start_all(rims[d])

    def late(e):
        def go():
            pl.semaphore_wait(late_sem.at[e], 1)
            when(has_xl[0], lambda: start_all(diags[0, e]))
        when(has_ta[e], go)

    every_row = pl.ds(0, n_rows)
    pl.semaphore_wait(barrier, peers)
    for e in range(2):
        when(has_ta[e], lambda e=e: pl.semaphore_signal(late_sem.at[1 - e], inc=1, device_id={"ta": ta_at[e]},
                                                        device_id_type=MESH))
    when(has_xl[1], lambda: send_rims(1))
    when(has_xl[0], lambda: start_all(rims[0]))
    load_samples(x_left, 0, every_row, 0).wait()
    for p in range(n_pairs):
        bin_pair(p, x_left, slice(0, LANES))
    pack_halo(1)
    when(has_ta[1], lambda: start_all(halos[1]))
    late(1)
    load_samples(x_right, LANES, every_row, 1).wait()
    for p in range(n_pairs):
        bin_pair(p, x_right, slice(LANES, span))

    first = (xl == 0) & (ta == 0)
    when(jnp.logical_not(first), lambda: late(0))
    for p, r in ends:
        chosen = [hot[p, r * height: (r + 1) * height] for hot, (_, _, _, height) in zip(hots, ranges)]
        merge(p, r, [dot(part, jnp.ones((part.shape[1], LANES), BF16)) for part in chosen], slice(span, span + LANES))
    to_other.start()
    pack_halo(0)
    when(has_ta[0], lambda: start_all(halos[0]))
    for p in range(n_pairs):
        count_pair(p)
    when(first, lambda: late(0))

    def resample(values):
        high, low = halves(values)
        return dot(high, tables[0]) + (dot(low, tables[0]) + dot(high, tables[1]))

    table_load.wait()
    for i in range(n_pairs):
        b = jnp.where(il == 0, i, n_pairs - 1 - i)
        if i == n_pairs - 1:
            to_other.wait_recv()
            acc[b + 1] = acc[b + 1] + il_recv[...]
        main[b] = resample(acc[b + 1, :, :span])
    for d in range(2):
        when(has_xl[1 - d], lambda d=d: wait_rims(recv_sem, d))
    sub = lax.broadcasted_iota(jnp.int32, (n_pairs, 1), 0)
    rim = jnp.concatenate([rim_recv[d] + jnp.where(sub == own_row, corner_recv[d], 0.0) for d in range(2)], axis=0)
    more = resample(rim[:, :span])
    more_fold = jnp.broadcast_to(rim[:, span + LANES // 2: span + LANES // 2 + 1], (2 * n_pairs, LANES))
    ends_row = lax.broadcasted_iota(jnp.int32, (8, 1), 0)
    tops = ((0, 0, 0), (own_cols - 8, 7, n_pairs))

    def add_rows(values, extra, b):
        top, bottom = [values[at: at + 8] + jnp.where(ends_row == where, extra[base + b: base + b + 1], 0.0)
                       for at, where, base in tops]
        return jnp.concatenate([top, values[8: own_cols - 8], bottom], axis=0)

    for b in range(n_pairs):
        scale = 1.0 / jnp.maximum(add_rows(acc[b + 1, :, span:], more_fold, b), 1.0)
        factor[b] = scale
        main[b] = add_rows(main[b], more, b) * jnp.concatenate([scale] * (main.shape[2] // LANES), axis=1)

    for d in range(2):
        for e in range(2):
            when(has_xl[1 - d] & has_ta[1 - e], lambda d=d, e=e: wait_diags(recv_sem, d, e))
    for d in range(2):
        first, last = [diag_recv[d, e] + jnp.where(sub == own_row, diag_corner[d, e], 0.0) for e in (1, 0)]
        rim_out[d * n_pairs: (d + 1) * n_pairs] = jnp.where(is_first, first, jnp.where(is_last, last, 0.0))
    for e in range(2):
        when(has_ta[1 - e], lambda e=e: wait_halos(recv_sem, e))
        halo_out[e] = halo_recv[e, :n_pairs]
        halo_out[e, own_row] = halo_recv[e, own_row] + halo_recv[e, n_pairs]
    to_other.wait_send()
    for d in range(2):
        when(has_xl[d], lambda d=d: wait_rims(send_sem, d))
        when(has_ta[d], lambda d=d: wait_halos(send_sem, d))
        for e in range(2):
            when(has_xl[d] & has_ta[e], lambda d=d, e=e: wait_diags(send_sem, d, e))


def finish(main, factor, halo, rim, t_edge, t_rim, out, staged, out_sem):
    n_pairs, own_cols, width = main.shape
    inner = pl.ds(LANES, width - 2 * LANES)
    writes = [pltpu.make_async_copy(main.at[:, :, inner], out.at[:, :, inner], out_sem.at[0])]
    writes[0].start()
    high = rim[...].astype(BF16)
    low = (rim[...] - high.astype(F32)).astype(BF16)
    more = dot(jnp.concatenate([high, low, high], axis=1), t_rim[...])
    ends_row = lax.broadcasted_iota(jnp.int32, (8, 1), 0)
    tops = ((0, 0, 0), (own_cols - 8, 7, n_pairs))
    for b in range(n_pairs):
        edges = jnp.concatenate([halo[0, b], halo[1, b]], axis=0)
        high = edges.astype(BF16).astype(F32)
        terms = jnp.concatenate([high, edges - high, high], axis=0).T[:own_cols].astype(BF16)
        ends = dot(terms, t_edge[...])
        top, bottom = [ends[at: at + 8] + jnp.where(ends_row == where, more[base + b: base + b + 1], 0.0)
                       for at, where, base in tops]
        ends = jnp.concatenate([top, ends[8: own_cols - 8], bottom], axis=0)
        for d, start in enumerate((0, width - LANES)):
            staged[b, d] = main[b, :, start: start + LANES] + ends[:, d * LANES: (d + 1) * LANES] * factor[b]
            write = pltpu.make_async_copy(staged.at[b, d], out.at[b, :, pl.ds(start, LANES)], out_sem.at[1])
            write.start()
    writes[0].wait()
    for d, start in enumerate((0, width - LANES)):
        pltpu.make_async_copy(staged.at[:, d], out.at[:, :, pl.ds(start, LANES)], out_sem.at[1]).wait()


def shards(n_xl, n_ta, traces, bin_steps):
    n_rows, n_cols, span = traces.shape
    n_pairs, own_cols = n_rows // 2, n_cols // 2
    width = span + LANES
    out_span = span * P_SIZE // Q
    if n_pairs % 8 or span % LANES or out_span % LANES or out_span < 3 * LANES:
        raise ValueError("block shape")
    table = lanczos_table(span)
    tables = np.stack(split_table(table[REACH:-REACH]))
    edge_cols = np.concatenate([table[:, :LANES], table[:, -LANES:]], axis=1)
    edge_high, edge_low = split_table(np.concatenate([edge_cols[:REACH], edge_cols[-REACH:]]))
    t_edge = np.concatenate([edge_high, edge_high, edge_low])
    rim_high, rim_low = split_table(np.concatenate(
        [edge_cols[-REACH:], np.zeros((LANES - 2 * REACH, 2 * LANES), np.float32), edge_cols[:REACH]]))
    t_rim = np.concatenate([rim_high, rim_high, rim_low])
    vmem = pl.BlockSpec(memory_space=pltpu.VMEM)
    hbm = pl.BlockSpec(memory_space=pltpu.HBM)
    (start_a, stop_a, _, height_a), (start_b, stop_b, _, height_b) = column_ranges(n_cols)
    main, factor, halo, rim = pl.pallas_call(
        functools.partial(binning, n_xl, n_ta),
        out_shape=(pltpu.VMEM((n_pairs, own_cols, out_span), F32), pltpu.VMEM((n_pairs, own_cols, LANES), F32),
                   pltpu.VMEM((2, n_pairs, REACH, LANES), F32), pltpu.VMEM((2 * n_pairs, LANES), F32)),
        in_specs=[hbm] * 3,
        out_specs=[vmem] * 4,
        scratch_shapes=[
            pltpu.VMEM((n_rows, n_cols, LANES), F32),
            pltpu.VMEM((n_rows, n_cols, span - LANES), F32),
            pltpu.VMEM((2, n_rows, 8, span), F32),
            pltpu.VMEM((2, n_rows, n_cols), jnp.int32),
            pltpu.VMEM(tables.shape, BF16),
            pltpu.VMEM((3, n_rows, LANES), jnp.int32),
            pltpu.VMEM((n_pairs, 3 * height_a, 2 * (stop_a - start_a)), BF16),
            pltpu.VMEM((n_pairs, 3 * height_b, 2 * (stop_b - start_b)), BF16),
            pltpu.VMEM((n_pairs + 2, own_cols, width), F32),
            pltpu.VMEM((2, n_pairs, width), F32),
            pltpu.VMEM((2, 1, width), F32),
            pltpu.VMEM((2, n_pairs, width), F32),
            pltpu.VMEM((2, 1, width), F32),
            pltpu.VMEM((own_cols, width), F32),
            pltpu.VMEM((2, n_pairs + 1, REACH, LANES), F32),
            pltpu.VMEM((2, n_pairs + 1, REACH, LANES), F32),
            pltpu.VMEM((n_pairs + 1, 1, width), F32),
            pltpu.VMEM((2, 2, n_pairs, LANES), F32),
            pltpu.VMEM((2, 2, 1, LANES), F32),
            pltpu.SemaphoreType.DMA((6,)),
            pltpu.SemaphoreType.REGULAR((2,)),
            pltpu.SemaphoreType.DMA((9,)),
            pltpu.SemaphoreType.DMA((9,)),
        ],
        compiler_params=pltpu.CompilerParams(collective_id=0, has_side_effects=True, vmem_limit_bytes=24 * 2**20),
        name="binning",
    )(*[pltpu.with_memory_space_constraint(a, pltpu.HBM) for a in (traces, bin_steps, jnp.asarray(tables))])
    return pl.pallas_call(
        finish,
        out_shape=jax.ShapeDtypeStruct((n_pairs, own_cols, out_span), F32),
        in_specs=[vmem] * 6,
        out_specs=hbm,
        scratch_shapes=[pltpu.VMEM((n_pairs, 2, own_cols, LANES), F32), pltpu.SemaphoreType.DMA((2,))],
        compiler_params=pltpu.CompilerParams(vmem_limit_bytes=16 * 2**20),
        name="finish",
    )(main, factor, halo, rim, jnp.asarray(t_edge), jnp.asarray(t_rim))


def solution(mesh):
    if mesh.shape["il"] != 2:
        raise ValueError("il size")
    return jax.shard_map(
        functools.partial(shards, mesh.shape["xl"], mesh.shape["ta"]),
        mesh=mesh,
        in_specs=(P("il", "xl", "ta"), P(None, "il", "xl")),
        out_specs=P("il", "xl", "ta"),
        check_vma=False,
    )
```

```python
import functools

import numpy as np
import jax
import jax.numpy as jnp
from jax import lax
from jax.experimental import pallas as pl
from jax.experimental.pallas import tpu as pltpu
from jax.sharding import PartitionSpec as P

TAPS = 16
P_SIZE = 3
Q = 2
REACH = TAPS // 2
LANES = 128
MESH = pl.DeviceIdType.MESH
F32, BF16 = jnp.float32, jnp.bfloat16


def lanczos_table(span):
    rows = np.arange(span + 2 * REACH)[:, None] - REACH
    cols = np.arange(span * P_SIZE // Q)[None, :]
    offset = (cols * Q - rows * P_SIZE).astype(np.float64) / P_SIZE
    weights = np.sinc(offset) * np.sinc(offset / REACH)
    return np.where(np.abs(offset) < REACH, weights, 0.0).astype(np.float32)


def split_table(table):
    high = table.astype(BF16)
    low = (table - high.astype(np.float32)).astype(BF16)
    return high, low


def halves(values):
    high = values.astype(BF16)
    low = (values - high.astype(F32)).astype(BF16)
    return high, low


def dot(a, b):
    return jnp.dot(a, b, preferred_element_type=F32)


def column_ranges(n_cols):
    own_cols, rest = n_cols // 2, n_cols - LANES
    if own_cols % 8 or rest % 16 or not LANES < 2 * rest <= 2 * LANES:
        raise ValueError("column count")
    height = (LANES // 2 + 1 + 7) // 8 * 8
    first = (LANES // 2 - 1) // 8 * 8
    return (0, LANES, 0, height), (LANES, n_cols, first, own_cols - first)


def scoped(kernel, *semaphores):
    def run(*refs):
        pl.run_scoped(lambda *scratch: kernel(*refs, *scratch), *semaphores)
    return run


def binning(n_xl, n_ta, traces, steps_hbm, tables_hbm, main, factor, halo_out, rim_out,
            x_left, x_right, edge_x, steps, tables, keys, hot_a, hot_b, acc,
            rim_send, corner_send, rim_recv, corner_recv, il_recv, halo_send, halo_recv, wide_rows,
            diag_recv, diag_corner, load_sem, late_sem, recv_sem):
    n_rows, n_cols, _ = x_left.shape
    span = LANES + x_right.shape[2]
    n_pairs, own_cols = n_rows // 2, n_cols // 2
    il, xl, ta = lax.axis_index("il"), lax.axis_index("xl"), lax.axis_index("ta")
    other = 1 - il
    has_xl, has_ta = (xl < n_xl - 1, xl > 0), (ta < n_ta - 1, ta > 0)
    xl_at, ta_at = (xl + 1, xl - 1), (ta + 1, ta - 1)
    ranges = column_ranges(n_cols)

    def when(condition, work):
        pl.when(condition)(work)

    step_load = pltpu.make_async_copy(steps_hbm, steps, load_sem.at[3])
    step_load.start()
    edge_loads = [pltpu.make_async_copy(traces.at[:, pl.ds(start, 8)], edge_x.at[d], load_sem.at[4 + d])
                  for d, start in enumerate((n_cols - 8, 0))]
    for load in edge_loads:
        load.start()

    def load_samples(x, start, rows, slot):
        samples = pl.ds(start, x.shape[2])
        return pltpu.make_async_copy(traces.at[rows, :, samples], x.at[rows], load_sem.at[slot])

    table_load = pltpu.make_async_copy(tables_hbm, tables, load_sem.at[2])

    barrier = pltpu.get_barrier_semaphore()

    def greet(has, partner):
        def signal():
            pl.semaphore_signal(barrier, inc=1, device_id=partner, device_id_type=MESH)
            pl.semaphore_signal(barrier, inc=1, device_id={"il": other, **partner}, device_id_type=MESH)
        when(has, signal)

    pl.semaphore_signal(barrier, inc=1, device_id={"il": other}, device_id_type=MESH)
    for d in range(2):
        greet(has_xl[0] & has_ta[d], {"xl": xl + 1, "ta": ta_at[d]})
    for d in range(2):
        greet(has_xl[d], {"xl": xl_at[d]})
        greet(has_ta[d], {"ta": ta_at[d]})
    count_xl, count_ta = [sum(jnp.where(has, 1, 0) for has in pair) for pair in (has_xl, has_ta)]
    peers = 1 + 2 * (count_xl + count_ta + jnp.where(has_xl[1], count_ta, 0))
    for p in range(n_pairs):
        load_samples(x_left, 0, pl.ds(2 * p, 2), 0).start()

    for e in range(2):
        def no_ta(e=e):
            halo_recv[e] = jnp.zeros_like(halo_recv[e])
        when(jnp.logical_not(has_ta[1 - e]), no_ta)
    for d in range(2):
        def no_xl(d=d):
            rim_recv[d] = jnp.zeros_like(rim_recv[d])
            corner_recv[d] = jnp.zeros_like(corner_recv[d])
        when(jnp.logical_not(has_xl[1 - d]), no_xl)
        for e in range(2):
            def no_diag(d=d, e=e):
                diag_recv[d, e] = jnp.zeros_like(diag_recv[d, e])
                diag_corner[d, e] = jnp.zeros_like(diag_corner[d, e])
            when(jnp.logical_not(has_xl[1 - d] & has_ta[1 - e]), no_diag)

    lane = lax.broadcasted_iota(jnp.int32, (1, LANES), 1)
    is_first, is_last = lane < REACH, lane >= LANES - REACH
    step_load.wait()
    col = lax.broadcasted_iota(jnp.int32, (n_rows, n_cols), 1)
    row = lax.broadcasted_iota(jnp.int32, (n_rows, n_cols), 0)
    bin_col = lax.shift_right_logical(col, 1) + steps[1]
    bin_row = steps[0] + 1
    own = (bin_col >= 0) & (bin_col < own_cols)
    code_a, code_b = [jnp.where(own, bin_row * height + bin_col - first, -1)[:, start:stop]
                      for start, stop, first, height in ranges]
    rest = n_cols - LANES
    keys[0] = code_a
    padded = jnp.concatenate([code_b, jnp.full((n_rows, LANES - rest), -1, jnp.int32)], axis=1)
    keys[1] = padded
    keys[2] = pltpu.roll(padded, rest, 1)

    def one_hot(key, height):
        rows = lax.broadcasted_iota(jnp.int32, (height, key.shape[1]), 0)
        return jnp.where(rows == key, 1.0, 0.0).astype(BF16)

    for p in range(n_pairs):
        key = jnp.concatenate([keys[0, 2 * p: 2 * p + 1], keys[0, 2 * p + 1: 2 * p + 2]], axis=1)
        hot_a[p] = one_hot(key, 3 * ranges[0][3])
        second = keys[2, 2 * p + 1: 2 * p + 2]
        key = jnp.concatenate([jnp.where(lane < rest, keys[1, 2 * p: 2 * p + 1], second),
                               second[:, :2 * rest - LANES]], axis=1)
        hot_b[p] = one_hot(key, 3 * ranges[1][3])
    rim_bin = bin_row - 1 + lax.shift_right_logical(row, 1)
    outside = jnp.where(il == 0, n_pairs, -1)
    rim_code = jnp.where(rim_bin == outside, n_pairs, jnp.where((rim_bin < 0) | (rim_bin >= n_pairs), -1, rim_bin))
    for load in edge_loads:
        load.wait()
    for d, (start, column) in enumerate(((n_cols - 8, own_cols), (0, -1))):
        target = jnp.where(bin_col == column, rim_code, -1)
        key = jnp.concatenate([target[i: i + 1, start: start + 8] for i in range(n_rows)], axis=1)
        chosen = one_hot(key, n_pairs + 8)
        high, low = halves(edge_x[d].reshape(n_rows * 8, span))
        sums = dot(chosen, high) + dot(chosen, low)
        folds = dot(chosen, jnp.ones((n_rows * 8, LANES), BF16))
        ends = jnp.where(is_first, sums[:, :LANES], jnp.where(is_last, sums[:, span - LANES:], folds))
        rim_send[d, :, :span] = sums[:n_pairs]
        rim_send[d, :, span:] = ends[:n_pairs]
        corner_send[d, :, :span] = sums[n_pairs: n_pairs + 1]
        corner_send[d, :, span:] = ends[n_pairs: n_pairs + 1]

    hots = (hot_a, hot_b)
    for p in range(n_pairs):
        load_samples(x_right, LANES, pl.ds(2 * p, 2), 1).start()
    table_load.start()

    def merge(p, r, parts, lanes):
        (_, _, _, height), (_, _, first, _) = ranges
        a, b = parts
        both = a[first:] + b[: height - first]
        for at, part in ((0, a[:first]), (first, both), (height, b[height - first:])):
            where = (p + r, slice(at, at + part.shape[0]), lanes)
            acc[where] = part if p == 0 or r == 2 else acc[where] + part

    def groups(parts, r):
        return [part[r * height: (r + 1) * height] for part, (_, _, _, height) in zip(parts, ranges)]

    def bin_pair(p, x, lanes):
        parts, wide = [], x.shape[2]
        for hot, (start, stop, _, _) in zip(hots, ranges):
            high, low = halves(jnp.concatenate([x[2 * p, start:stop], x[2 * p + 1, start:stop]], axis=0))
            sums = dot(hot[p], jnp.concatenate([high, low], axis=1))
            parts.append(sums[:, :wide] + sums[:, wide:])
        for r in range(3):
            merge(p, r, groups(parts, r), lanes)

    ends = (0, 0), (n_pairs - 1, 2)

    def count_pair(p):
        parts = [dot(hot[p], jnp.ones((hot.shape[2], LANES), BF16)) for hot in hots]
        for r in range(3):
            if (p, r) not in ends:
                merge(p, r, groups(parts, r), slice(span, span + LANES))

    def send_sem(slot):
        return load_sem.at[(6, 7, 3, 8, 0, 1, 9, 4, 5)[slot]]

    def remote(src, dst, slot, partner):
        return pltpu.make_async_remote_copy(src_ref=src, dst_ref=dst, send_sem=send_sem(slot), recv_sem=recv_sem.at[slot],
                                            device_id=partner, device_id_type=MESH)

    rim_row = jnp.where(il == 0, n_pairs + 1, 0)
    own_row = jnp.where(il == 0, n_pairs - 1, 0)
    to_other = remote(acc.at[rim_row], il_recv, 0, {"il": other})

    rims, halos, diags = [], [], {}
    for d in range(2):
        to, rows = {"xl": xl_at[d]}, pl.ds(0, n_pairs)
        rims.append((remote(rim_send.at[d], rim_recv.at[d], 1 + d, to),
                     remote(corner_send.at[d], corner_recv.at[d], 1 + d, {"il": other, **to})))
        to = {"ta": ta_at[d]}
        halos.append((remote(halo_send.at[d, rows], halo_recv.at[d, rows], 3 + d, to),
                      remote(halo_send.at[d, n_pairs], halo_recv.at[d, n_pairs], 3 + d, {"il": other, **to})))
        for e in range(2):
            to, end, slot = {"xl": xl_at[d], "ta": ta_at[e]}, pl.ds(span, LANES), 5 + 2 * d + e
            diags[d, e] = (remote(rim_send.at[d, :, end], diag_recv.at[d, e], slot, to),
                           remote(corner_send.at[d, :, end], diag_corner.at[d, e], slot, {"il": other, **to}))

    def received(slot):
        return recv_sem.at[slot]

    def wait_all(semaphores, slot, rows):
        pltpu.make_async_copy(rows, rows, semaphores(slot)).wait()

    def wait_rims(semaphores, d):
        wait_all(semaphores, 1 + d, wide_rows)

    def wait_halos(semaphores, e):
        wait_all(semaphores, 3 + e, halo_recv.at[e])

    def wait_diags(semaphores, d, e):
        wait_all(semaphores, 5 + 2 * d + e, wide_rows.at[:, :, pl.ds(0, LANES)])

    def start_all(copies):
        for copy in copies:
            copy.start()

    def pack_halo(e):
        lanes = slice(0, LANES) if e else slice(span - LANES, span)
        rows = slice(0, REACH) if e else slice(LANES - REACH, LANES)
        for b in range(n_pairs):
            halo_send[e, b, :, :own_cols] = acc[b + 1, :, lanes].T[rows]
        halo_send[e, n_pairs, :, :own_cols] = acc[rim_row, :, lanes].T[rows]

    def send_diags(d):
        for e in (1, 0):
            when(has_ta[e], lambda e=e: start_all(diags[d, e]))

    def send_rims(d):
        send_diags(d)
        start_all(rims[d])

    def late(e):
        def go():
            pl.semaphore_wait(late_sem.at[e], 1)
            when(has_xl[0], lambda: start_all(diags[0, e]))
        when(has_ta[e], go)

    every_row = pl.ds(0, n_rows)
    pl.semaphore_wait(barrier, peers)
    for e in range(2):
        when(has_ta[e], lambda e=e: pl.semaphore_signal(late_sem.at[1 - e], inc=1, device_id={"ta": ta_at[e]},
                                                        device_id_type=MESH))
    when(has_xl[1], lambda: send_rims(1))
    when(has_xl[0], lambda: start_all(rims[0]))
    load_samples(x_left, 0, every_row, 0).wait()
    for p in range(n_pairs):
        bin_pair(p, x_left, slice(0, LANES))
    pack_halo(1)
    when(has_ta[1], lambda: start_all(halos[1]))
    late(1)
    load_samples(x_right, LANES, every_row, 1).wait()
    for p in range(n_pairs):
        bin_pair(p, x_right, slice(LANES, span))

    first = (xl == 0) & (ta == 0)
    when(jnp.logical_not(first), lambda: late(0))
    for p, r in ends:
        chosen = [hot[p, r * height: (r + 1) * height] for hot, (_, _, _, height) in zip(hots, ranges)]
        merge(p, r, [dot(part, jnp.ones((part.shape[1], LANES), BF16)) for part in chosen], slice(span, span + LANES))
    to_other.start()
    pack_halo(0)
    when(has_ta[0], lambda: start_all(halos[0]))
    for p in range(n_pairs):
        count_pair(p)
    when(first, lambda: late(0))

    def resample(values):
        high, low = halves(values)
        return dot(high, tables[0]) + (dot(low, tables[0]) + dot(high, tables[1]))

    table_load.wait()
    for i in range(n_pairs):
        b = jnp.where(il == 0, i, n_pairs - 1 - i)
        if i == n_pairs - 1:
            to_other.wait_recv()
            acc[b + 1] = acc[b + 1] + il_recv[...]
        main[b] = resample(acc[b + 1, :, :span])
    for d in range(2):
        when(has_xl[1 - d], lambda d=d: wait_rims(received, d))
    sub = lax.broadcasted_iota(jnp.int32, (n_pairs, 1), 0)
    rim = jnp.concatenate([rim_recv[d] + jnp.where(sub == own_row, corner_recv[d], 0.0) for d in range(2)], axis=0)
    more = resample(rim[:, :span])
    more_fold = jnp.broadcast_to(rim[:, span + LANES // 2: span + LANES // 2 + 1], (2 * n_pairs, LANES))
    ends_row = lax.broadcasted_iota(jnp.int32, (8, 1), 0)
    tops = ((0, 0, 0), (own_cols - 8, 7, n_pairs))

    def add_rows(values, extra, b):
        top, bottom = [values[at: at + 8] + jnp.where(ends_row == where, extra[base + b: base + b + 1], 0.0)
                       for at, where, base in tops]
        return jnp.concatenate([top, values[8: own_cols - 8], bottom], axis=0)

    for b in range(n_pairs):
        scale = 1.0 / jnp.maximum(add_rows(acc[b + 1, :, span:], more_fold, b), 1.0)
        factor[b] = scale
        main[b] = add_rows(main[b], more, b) * jnp.concatenate([scale] * (main.shape[2] // LANES), axis=1)

    for d in range(2):
        for e in range(2):
            when(has_xl[1 - d] & has_ta[1 - e], lambda d=d, e=e: wait_diags(received, d, e))
    for d in range(2):
        first, last = [diag_recv[d, e] + jnp.where(sub == own_row, diag_corner[d, e], 0.0) for e in (1, 0)]
        rim_out[d * n_pairs: (d + 1) * n_pairs] = jnp.where(is_first, first, jnp.where(is_last, last, 0.0))
    for e in range(2):
        when(has_ta[1 - e], lambda e=e: wait_halos(received, e))
        halo_out[e] = halo_recv[e, :n_pairs]
        halo_out[e, own_row] = halo_recv[e, own_row] + halo_recv[e, n_pairs]
    to_other.wait_send()
    for d in range(2):
        when(has_xl[d], lambda d=d: wait_rims(send_sem, d))
        when(has_ta[d], lambda d=d: wait_halos(send_sem, d))
        for e in range(2):
            when(has_xl[d] & has_ta[e], lambda d=d, e=e: wait_diags(send_sem, d, e))


def finish(main, factor, halo, rim, t_edge, t_rim, out, staged, out_sem):
    n_pairs, own_cols, width = main.shape
    inner = pl.ds(LANES, width - 2 * LANES)
    writes = [pltpu.make_async_copy(main.at[:, :, inner], out.at[:, :, inner], out_sem.at[0])]
    writes[0].start()
    high = rim[...].astype(BF16)
    low = (rim[...] - high.astype(F32)).astype(BF16)
    more = dot(jnp.concatenate([high, low, high], axis=1), t_rim[...])
    ends_row = lax.broadcasted_iota(jnp.int32, (8, 1), 0)
    tops = ((0, 0, 0), (own_cols - 8, 7, n_pairs))
    for b in range(n_pairs):
        edges = jnp.concatenate([halo[0, b], halo[1, b]], axis=0)
        high = edges.astype(BF16).astype(F32)
        terms = jnp.concatenate([high, edges - high, high], axis=0).T[:own_cols].astype(BF16)
        ends = dot(terms, t_edge[...])
        top, bottom = [ends[at: at + 8] + jnp.where(ends_row == where, more[base + b: base + b + 1], 0.0)
                       for at, where, base in tops]
        ends = jnp.concatenate([top, ends[8: own_cols - 8], bottom], axis=0)
        for d, start in enumerate((0, width - LANES)):
            staged[b, d] = main[b, :, start: start + LANES] + ends[:, d * LANES: (d + 1) * LANES] * factor[b]
            write = pltpu.make_async_copy(staged.at[b, d], out.at[b, :, pl.ds(start, LANES)], out_sem.at[1])
            write.start()
    writes[0].wait()
    for d, start in enumerate((0, width - LANES)):
        pltpu.make_async_copy(staged.at[:, d], out.at[:, :, pl.ds(start, LANES)], out_sem.at[1]).wait()


def shards(n_xl, n_ta, traces, bin_steps):
    n_rows, n_cols, span = traces.shape
    n_pairs, own_cols = n_rows // 2, n_cols // 2
    width = span + LANES
    out_span = span * P_SIZE // Q
    if n_pairs % 8 or span % LANES or out_span % LANES or out_span < 3 * LANES:
        raise ValueError("block shape")
    table = lanczos_table(span)
    tables = np.stack(split_table(table[REACH:-REACH]))
    edge_cols = np.concatenate([table[:, :LANES], table[:, -LANES:]], axis=1)
    edge_high, edge_low = split_table(np.concatenate([edge_cols[:REACH], edge_cols[-REACH:]]))
    t_edge = np.concatenate([edge_high, edge_high, edge_low])
    rim_high, rim_low = split_table(np.concatenate(
        [edge_cols[-REACH:], np.zeros((LANES - 2 * REACH, 2 * LANES), np.float32), edge_cols[:REACH]]))
    t_rim = np.concatenate([rim_high, rim_high, rim_low])
    vmem = pl.BlockSpec(memory_space=pltpu.VMEM)
    hbm = pl.BlockSpec(memory_space=pltpu.HBM)
    (start_a, stop_a, _, height_a), (start_b, stop_b, _, height_b) = column_ranges(n_cols)
    main, factor, halo, rim = pl.pallas_call(
        scoped(functools.partial(binning, n_xl, n_ta), pltpu.SemaphoreType.DMA((10,)), pltpu.SemaphoreType.REGULAR((2,)),
               pltpu.SemaphoreType.DMA((9,))),
        out_shape=(pltpu.VMEM((n_pairs, own_cols, out_span), F32), pltpu.VMEM((n_pairs, own_cols, LANES), F32),
                   pltpu.VMEM((2, n_pairs, REACH, LANES), F32), pltpu.VMEM((2 * n_pairs, LANES), F32)),
        in_specs=[hbm] * 3,
        out_specs=[vmem] * 4,
        scratch_shapes=[
            pltpu.VMEM((n_rows, n_cols, LANES), F32),
            pltpu.VMEM((n_rows, n_cols, span - LANES), F32),
            pltpu.VMEM((2, n_rows, 8, span), F32),
            pltpu.VMEM((2, n_rows, n_cols), jnp.int32),
            pltpu.VMEM(tables.shape, BF16),
            pltpu.VMEM((3, n_rows, LANES), jnp.int32),
            pltpu.VMEM((n_pairs, 3 * height_a, 2 * (stop_a - start_a)), BF16),
            pltpu.VMEM((n_pairs, 3 * height_b, 2 * (stop_b - start_b)), BF16),
            pltpu.VMEM((n_pairs + 2, own_cols, width), F32),
            pltpu.VMEM((2, n_pairs, width), F32),
            pltpu.VMEM((2, 1, width), F32),
            pltpu.VMEM((2, n_pairs, width), F32),
            pltpu.VMEM((2, 1, width), F32),
            pltpu.VMEM((own_cols, width), F32),
            pltpu.VMEM((2, n_pairs + 1, REACH, LANES), F32),
            pltpu.VMEM((2, n_pairs + 1, REACH, LANES), F32),
            pltpu.VMEM((n_pairs + 1, 1, width), F32),
            pltpu.VMEM((2, 2, n_pairs, LANES), F32),
            pltpu.VMEM((2, 2, 1, LANES), F32),
        ],
        compiler_params=pltpu.CompilerParams(collective_id=0, has_side_effects=True, vmem_limit_bytes=24 * 2**20),
        name="binning",
    )(*[pltpu.with_memory_space_constraint(a, pltpu.HBM) for a in (traces, bin_steps, jnp.asarray(tables))])
    return pl.pallas_call(
        scoped(finish, pltpu.SemaphoreType.DMA((2,))),
        out_shape=jax.ShapeDtypeStruct((n_pairs, own_cols, out_span), F32),
        in_specs=[vmem] * 6,
        out_specs=hbm,
        scratch_shapes=[pltpu.VMEM((n_pairs, 2, own_cols, LANES), F32)],
        compiler_params=pltpu.CompilerParams(vmem_limit_bytes=16 * 2**20),
        name="finish",
    )(main, factor, halo, rim, jnp.asarray(t_edge), jnp.asarray(t_rim))


def solution(mesh):
    if mesh.shape["il"] != 2:
        raise ValueError("il size")
    return jax.shard_map(
        functools.partial(shards, mesh.shape["xl"], mesh.shape["ta"]),
        mesh=mesh,
        in_specs=(P("il", "xl", "ta"), P(None, "il", "xl")),
        out_specs=P("il", "xl", "ta"),
        check_vma=False,
    )
```

```python
import functools

import numpy as np
import jax
import jax.numpy as jnp
from jax import lax
from jax.experimental import pallas as pl
from jax.experimental.pallas import tpu as pltpu
from jax.sharding import PartitionSpec as P

TAPS = 16
P_SIZE = 3
Q = 2
REACH = TAPS // 2
LANES = 128
MESH = pl.DeviceIdType.MESH
F32, BF16 = jnp.float32, jnp.bfloat16


def lanczos_table(span):
    rows = np.arange(span + 2 * REACH)[:, None] - REACH
    cols = np.arange(span * P_SIZE // Q)[None, :]
    offset = (cols * Q - rows * P_SIZE).astype(np.float64) / P_SIZE
    weights = np.sinc(offset) * np.sinc(offset / REACH)
    return np.where(np.abs(offset) < REACH, weights, 0.0).astype(np.float32)


def split_table(table):
    high = table.astype(BF16)
    low = (table - high.astype(np.float32)).astype(BF16)
    return high, low


def halves(values):
    high = values.astype(BF16)
    low = (values - high.astype(F32)).astype(BF16)
    return high, low


def dot(a, b):
    return jnp.dot(a, b, preferred_element_type=F32)


def column_ranges(n_cols):
    own_cols, rest = n_cols // 2, n_cols - LANES
    if own_cols % 8 or rest % 16 or not LANES < 2 * rest <= 2 * LANES:
        raise ValueError("column count")
    height = (LANES // 2 + 1 + 7) // 8 * 8
    first = (LANES // 2 - 1) // 8 * 8
    return (0, LANES, 0, height), (LANES, n_cols, first, own_cols - first)


def scoped(kernel, *semaphores):
    def run(*refs):
        pl.run_scoped(lambda *scratch: kernel(*refs, *scratch), *semaphores)
    return run


def binning(n_xl, n_ta, traces, steps_hbm, tables_hbm, main, factor, halo_out, rim_out,
            x_left, x_right, edge_x, steps, tables, keys, hot_a, hot_b, acc,
            rim_send, corner_send, rim_recv, corner_recv, il_recv, halo_send, halo_recv, wide_rows,
            diag_recv, diag_corner, load_sem, late_sem, recv_sem):
    n_rows, n_cols, _ = x_left.shape
    span = LANES + x_right.shape[2]
    n_pairs, own_cols = n_rows // 2, n_cols // 2
    il, xl, ta = lax.axis_index("il"), lax.axis_index("xl"), lax.axis_index("ta")
    other = 1 - il
    has_xl, has_ta = (xl < n_xl - 1, xl > 0), (ta < n_ta - 1, ta > 0)
    xl_at, ta_at = (xl + 1, xl - 1), (ta + 1, ta - 1)
    ranges = column_ranges(n_cols)

    def when(condition, work):
        pl.when(condition)(work)

    step_load = pltpu.make_async_copy(steps_hbm, steps, load_sem.at[3])
    step_load.start()
    edge_loads = [pltpu.make_async_copy(traces.at[:, pl.ds(start, 8)], edge_x.at[d], load_sem.at[4 + d])
                  for d, start in enumerate((n_cols - 8, 0))]
    for load in edge_loads:
        load.start()

    def load_samples(x, start, rows, slot):
        samples = pl.ds(start, x.shape[2])
        return pltpu.make_async_copy(traces.at[rows, :, samples], x.at[rows], load_sem.at[slot])

    table_load = pltpu.make_async_copy(tables_hbm, tables, load_sem.at[2])

    barrier = pltpu.get_barrier_semaphore()

    def greet(has, partner):
        def signal():
            pl.semaphore_signal(barrier, inc=1, device_id=partner, device_id_type=MESH)
            pl.semaphore_signal(barrier, inc=1, device_id={"il": other, **partner}, device_id_type=MESH)
        when(has, signal)

    for d in (1, 0):
        greet(has_xl[d], {"xl": xl_at[d]})
    for d in (1, 0):
        greet(has_xl[0] & has_ta[d], {"xl": xl + 1, "ta": ta_at[d]})
    for d in (1, 0):
        greet(has_ta[d], {"ta": ta_at[d]})
    pl.semaphore_signal(barrier, inc=1, device_id={"il": other}, device_id_type=MESH)
    count_xl, count_ta = [sum(jnp.where(has, 1, 0) for has in pair) for pair in (has_xl, has_ta)]
    peers = 1 + 2 * (count_xl + count_ta + jnp.where(has_xl[1], count_ta, 0))
    for p in range(n_pairs):
        load_samples(x_left, 0, pl.ds(2 * p, 2), 0).start()

    for e in range(2):
        def no_ta(e=e):
            halo_recv[e] = jnp.zeros_like(halo_recv[e])
        when(jnp.logical_not(has_ta[1 - e]), no_ta)
    for d in range(2):
        def no_xl(d=d):
            rim_recv[d] = jnp.zeros_like(rim_recv[d])
            corner_recv[d] = jnp.zeros_like(corner_recv[d])
        when(jnp.logical_not(has_xl[1 - d]), no_xl)
        for e in range(2):
            def no_diag(d=d, e=e):
                diag_recv[d, e] = jnp.zeros_like(diag_recv[d, e])
                diag_corner[d, e] = jnp.zeros_like(diag_corner[d, e])
            when(jnp.logical_not(has_xl[1 - d] & has_ta[1 - e]), no_diag)

    lane = lax.broadcasted_iota(jnp.int32, (1, LANES), 1)
    is_first, is_last = lane < REACH, lane >= LANES - REACH
    step_load.wait()
    col = lax.broadcasted_iota(jnp.int32, (n_rows, n_cols), 1)
    row = lax.broadcasted_iota(jnp.int32, (n_rows, n_cols), 0)
    bin_col = lax.shift_right_logical(col, 1) + steps[1]
    bin_row = steps[0] + 1
    own = (bin_col >= 0) & (bin_col < own_cols)
    code_a, code_b = [jnp.where(own, bin_row * height + bin_col - first, -1)[:, start:stop]
                      for start, stop, first, height in ranges]
    rest = n_cols - LANES
    keys[0] = code_a
    padded = jnp.concatenate([code_b, jnp.full((n_rows, LANES - rest), -1, jnp.int32)], axis=1)
    keys[1] = padded
    keys[2] = pltpu.roll(padded, rest, 1)

    def one_hot(key, height):
        rows = lax.broadcasted_iota(jnp.int32, (height, key.shape[1]), 0)
        return jnp.where(rows == key, 1.0, 0.0).astype(BF16)

    for p in range(n_pairs):
        key = jnp.concatenate([keys[0, 2 * p: 2 * p + 1], keys[0, 2 * p + 1: 2 * p + 2]], axis=1)
        hot_a[p] = one_hot(key, 3 * ranges[0][3])
        second = keys[2, 2 * p + 1: 2 * p + 2]
        key = jnp.concatenate([jnp.where(lane < rest, keys[1, 2 * p: 2 * p + 1], second),
                               second[:, :2 * rest - LANES]], axis=1)
        hot_b[p] = one_hot(key, 3 * ranges[1][3])
    rim_bin = bin_row - 1 + lax.shift_right_logical(row, 1)
    outside = jnp.where(il == 0, n_pairs, -1)
    rim_code = jnp.where(rim_bin == outside, n_pairs, jnp.where((rim_bin < 0) | (rim_bin >= n_pairs), -1, rim_bin))
    for load in edge_loads:
        load.wait()
    for d, (start, column) in enumerate(((n_cols - 8, own_cols), (0, -1))):
        target = jnp.where(bin_col == column, rim_code, -1)
        key = jnp.concatenate([target[i: i + 1, start: start + 8] for i in range(n_rows)], axis=1)
        chosen = one_hot(key, n_pairs + 8)
        high, low = halves(edge_x[d].reshape(n_rows * 8, span))
        sums = dot(chosen, high) + dot(chosen, low)
        folds = dot(chosen, jnp.ones((n_rows * 8, LANES), BF16))
        ends = jnp.where(is_first, sums[:, :LANES], jnp.where(is_last, sums[:, span - LANES:], folds))
        rim_send[d, :, :span] = sums[:n_pairs]
        rim_send[d, :, span:] = ends[:n_pairs]
        corner_send[d, :, :span] = sums[n_pairs: n_pairs + 1]
        corner_send[d, :, span:] = ends[n_pairs: n_pairs + 1]

    hots = (hot_a, hot_b)
    for p in range(n_pairs):
        load_samples(x_right, LANES, pl.ds(2 * p, 2), 1).start()
    table_load.start()

    def merge(p, r, parts, lanes):
        (_, _, _, height), (_, _, first, _) = ranges
        a, b = parts
        both = a[first:] + b[: height - first]
        for at, part in ((0, a[:first]), (first, both), (height, b[height - first:])):
            where = (p + r, slice(at, at + part.shape[0]), lanes)
            acc[where] = part if p == 0 or r == 2 else acc[where] + part

    def groups(parts, r):
        return [part[r * height: (r + 1) * height] for part, (_, _, _, height) in zip(parts, ranges)]

    def bin_pair(p, x, lanes):
        parts, wide = [], x.shape[2]
        for hot, (start, stop, _, _) in zip(hots, ranges):
            high, low = halves(jnp.concatenate([x[2 * p, start:stop], x[2 * p + 1, start:stop]], axis=0))
            sums = dot(hot[p], jnp.concatenate([high, low], axis=1))
            parts.append(sums[:, :wide] + sums[:, wide:])
        for r in range(3):
            merge(p, r, groups(parts, r), lanes)

    ends = (0, 0), (n_pairs - 1, 2)

    def count_pair(p):
        parts = [dot(hot[p], jnp.ones((hot.shape[2], LANES), BF16)) for hot in hots]
        for r in range(3):
            if (p, r) not in ends:
                merge(p, r, groups(parts, r), slice(span, span + LANES))

    def send_sem(slot):
        return load_sem.at[(6, 7, 3, 8, 0, 1, 9, 4, 5)[slot]]

    def remote(src, dst, slot, partner):
        return pltpu.make_async_remote_copy(src_ref=src, dst_ref=dst, send_sem=send_sem(slot), recv_sem=recv_sem.at[slot],
                                            device_id=partner, device_id_type=MESH)

    rim_row = jnp.where(il == 0, n_pairs + 1, 0)
    own_row = jnp.where(il == 0, n_pairs - 1, 0)
    to_other = remote(acc.at[rim_row], il_recv, 0, {"il": other})

    rims, halos, diags = [], [], {}
    for d in range(2):
        to, rows = {"xl": xl_at[d]}, pl.ds(0, n_pairs)
        rims.append((remote(rim_send.at[d], rim_recv.at[d], 1 + d, to),
                     remote(corner_send.at[d], corner_recv.at[d], 1 + d, {"il": other, **to})))
        to = {"ta": ta_at[d]}
        halos.append((remote(halo_send.at[d, rows], halo_recv.at[d, rows], 3 + d, to),
                      remote(halo_send.at[d, n_pairs], halo_recv.at[d, n_pairs], 3 + d, {"il": other, **to})))
        for e in range(2):
            to, end, slot = {"xl": xl_at[d], "ta": ta_at[e]}, pl.ds(span, LANES), 5 + 2 * d + e
            diags[d, e] = (remote(rim_send.at[d, :, end], diag_recv.at[d, e], slot, to),
                           remote(corner_send.at[d, :, end], diag_corner.at[d, e], slot, {"il": other, **to}))

    def received(slot):
        return recv_sem.at[slot]

    def wait_all(semaphores, slot, rows):
        pltpu.make_async_copy(rows, rows, semaphores(slot)).wait()

    def wait_rims(semaphores, d):
        wait_all(semaphores, 1 + d, wide_rows)

    def wait_halos(semaphores, e):
        wait_all(semaphores, 3 + e, halo_recv.at[e])

    def wait_diags(semaphores, d, e):
        wait_all(semaphores, 5 + 2 * d + e, wide_rows.at[:, :, pl.ds(0, LANES)])

    def start_all(copies):
        for copy in copies:
            copy.start()

    def pack_halo(e):
        lanes = slice(0, LANES) if e else slice(span - LANES, span)
        rows = slice(0, REACH) if e else slice(LANES - REACH, LANES)
        for b in range(n_pairs):
            halo_send[e, b, :, :own_cols] = acc[b + 1, :, lanes].T[rows]
        halo_send[e, n_pairs, :, :own_cols] = acc[rim_row, :, lanes].T[rows]

    def send_diags(d):
        for e in (1, 0):
            when(has_ta[e], lambda e=e: start_all(diags[d, e]))

    def send_rims(d):
        send_diags(d)
        start_all(rims[d])

    def late(e):
        def go():
            pl.semaphore_wait(late_sem.at[e], 1)
            when(has_xl[0], lambda: start_all(diags[0, e]))
        when(has_ta[e], go)

    every_row = pl.ds(0, n_rows)
    pl.semaphore_wait(barrier, peers)
    for e in range(2):
        when(has_ta[e], lambda e=e: pl.semaphore_signal(late_sem.at[1 - e], inc=1, device_id={"ta": ta_at[e]},
                                                        device_id_type=MESH))
    when(has_xl[1], lambda: send_rims(1))
    when(has_xl[0], lambda: start_all(rims[0]))
    load_samples(x_left, 0, every_row, 0).wait()
    for p in range(n_pairs):
        bin_pair(p, x_left, slice(0, LANES))
    pack_halo(1)
    when(has_ta[1] & (il == 0), lambda: start_all(halos[1]))
    late(1)
    load_samples(x_right, LANES, every_row, 1).wait()
    when(has_ta[1] & (il == 1), lambda: start_all(halos[1]))
    for p in range(n_pairs):
        bin_pair(p, x_right, slice(LANES, span))

    first = (xl == 0) & (ta == 0)
    when(jnp.logical_not(first), lambda: late(0))
    for p, r in ends:
        chosen = [hot[p, r * height: (r + 1) * height] for hot, (_, _, _, height) in zip(hots, ranges)]
        merge(p, r, [dot(part, jnp.ones((part.shape[1], LANES), BF16)) for part in chosen], slice(span, span + LANES))
    to_other.start()
    pack_halo(0)
    when(has_ta[0], lambda: start_all(halos[0]))
    for p in range(n_pairs):
        count_pair(p)
    when(first, lambda: late(0))

    def resample(values):
        high, low = halves(values)
        return dot(high, tables[0]) + (dot(low, tables[0]) + dot(high, tables[1]))

    table_load.wait()
    for i in range(n_pairs):
        b = jnp.where(il == 0, i, n_pairs - 1 - i)
        if i == n_pairs - 1:
            to_other.wait_recv()
            acc[b + 1] = acc[b + 1] + il_recv[...]
        main[b] = resample(acc[b + 1, :, :span])
    for d in range(2):
        when(has_xl[1 - d], lambda d=d: wait_rims(received, d))
    sub = lax.broadcasted_iota(jnp.int32, (n_pairs, 1), 0)
    rim = jnp.concatenate([rim_recv[d] + jnp.where(sub == own_row, corner_recv[d], 0.0) for d in range(2)], axis=0)
    more = resample(rim[:, :span])
    more_fold = jnp.broadcast_to(rim[:, span + LANES // 2: span + LANES // 2 + 1], (2 * n_pairs, LANES))
    ends_row = lax.broadcasted_iota(jnp.int32, (8, 1), 0)
    tops = ((0, 0, 0), (own_cols - 8, 7, n_pairs))

    def add_rows(values, extra, b):
        top, bottom = [values[at: at + 8] + jnp.where(ends_row == where, extra[base + b: base + b + 1], 0.0)
                       for at, where, base in tops]
        return jnp.concatenate([top, values[8: own_cols - 8], bottom], axis=0)

    for b in range(n_pairs):
        scale = 1.0 / jnp.maximum(add_rows(acc[b + 1, :, span:], more_fold, b), 1.0)
        factor[b] = scale
        main[b] = add_rows(main[b], more, b) * jnp.concatenate([scale] * (main.shape[2] // LANES), axis=1)

    for d in range(2):
        for e in range(2):
            when(has_xl[1 - d] & has_ta[1 - e], lambda d=d, e=e: wait_diags(received, d, e))
    for d in range(2):
        first, last = [diag_recv[d, e] + jnp.where(sub == own_row, diag_corner[d, e], 0.0) for e in (1, 0)]
        rim_out[d * n_pairs: (d + 1) * n_pairs] = jnp.where(is_first, first, jnp.where(is_last, last, 0.0))
    for e in range(2):
        when(has_ta[1 - e], lambda e=e: wait_halos(received, e))
        halo_out[e] = halo_recv[e, :n_pairs]
        halo_out[e, own_row] = halo_recv[e, own_row] + halo_recv[e, n_pairs]
    to_other.wait_send()
    for d in range(2):
        when(has_xl[d], lambda d=d: wait_rims(send_sem, d))
        when(has_ta[d], lambda d=d: wait_halos(send_sem, d))
        for e in range(2):
            when(has_xl[d] & has_ta[e], lambda d=d, e=e: wait_diags(send_sem, d, e))


def finish(main, factor, halo, rim, t_edge, t_rim, out, staged, out_sem):
    n_pairs, own_cols, width = main.shape
    starts = (0, width - LANES)
    has_before = lax.axis_index("ta") > 0

    def write_tiles(source, start, size, slot):
        return pltpu.make_async_copy(source, out.at[:, :, pl.ds(start, size)], out_sem.at[slot])

    def from_main(start, size, slot):
        return write_tiles(main.at[:, :, pl.ds(start, size)], start, size, slot)

    from_main(LANES, width - 2 * LANES, 2).start()
    pl.when(jnp.logical_not(has_before))(from_main(0, LANES, 0).start)
    ends_row = lax.broadcasted_iota(jnp.int32, (8, 1), 0)
    tops = ((0, 0, 0), (own_cols - 8, 7, n_pairs))

    def add_halo(tiles, table):
        high = rim[...].astype(BF16)
        low = (rim[...] - high.astype(F32)).astype(BF16)
        more = dot(jnp.concatenate([high, low, high], axis=1), t_rim[...])
        for pair in zip(tiles[::2], tiles[1::2]):
            terms = []
            for d, b in pair:
                high = halo[d, b].astype(BF16).astype(F32)
                terms += [high, halo[d, b] - high, high]
            both = dot(jnp.concatenate(terms, axis=0).T[:own_cols].astype(BF16), t_edge[table])
            for i, (d, b) in enumerate(pair):
                ends, lanes = both[:, i * LANES: (i + 1) * LANES], slice(d * LANES, (d + 1) * LANES)
                top, bottom = [ends[at: at + 8] + jnp.where(ends_row == where, more[base + b: base + b + 1, lanes], 0.0)
                               for at, where, base in tops]
                ends = jnp.concatenate([top, ends[8: own_cols - 8], bottom], axis=0)
                staged[d, b] = main[b, :, starts[d]: starts[d] + LANES] + ends * factor[b]
                pltpu.make_async_copy(staged.at[d, b], out.at[b, :, pl.ds(starts[d], LANES)], out_sem.at[d]).start()

    rows = range(n_pairs)
    pl.when(has_before)(lambda: add_halo([(d, b) for b in rows for d in range(2)], 0))
    pl.when(jnp.logical_not(has_before))(lambda: add_halo([(1, b) for b in rows], 1))
    from_main(LANES, width - 2 * LANES, 2).wait()
    for d in range(2):
        write_tiles(staged.at[d], starts[d], LANES, d).wait()


def shards(n_xl, n_ta, traces, bin_steps):
    n_rows, n_cols, span = traces.shape
    n_pairs, own_cols = n_rows // 2, n_cols // 2
    width = span + LANES
    out_span = span * P_SIZE // Q
    if n_pairs % 8 or span % LANES or out_span % LANES or out_span < 3 * LANES:
        raise ValueError("block shape")
    table = lanczos_table(span)
    tables = np.stack(split_table(table[REACH:-REACH]))
    edge_cols = np.concatenate([table[:, :LANES], table[:, -LANES:]], axis=1)
    edge_high, edge_low = split_table(np.stack([edge_cols[:REACH, :LANES], edge_cols[-REACH:, LANES:]]))
    before, after = np.concatenate([edge_high, edge_high, edge_low], axis=1)
    none = np.zeros_like(before)
    t_edge = np.stack([np.block([[first, none], [none, after]]) for first in (before, after)])
    rim_high, rim_low = split_table(np.concatenate(
        [edge_cols[-REACH:], np.zeros((LANES - 2 * REACH, 2 * LANES), np.float32), edge_cols[:REACH]]))
    t_rim = np.concatenate([rim_high, rim_high, rim_low])
    vmem = pl.BlockSpec(memory_space=pltpu.VMEM)
    hbm = pl.BlockSpec(memory_space=pltpu.HBM)
    (start_a, stop_a, _, height_a), (start_b, stop_b, _, height_b) = column_ranges(n_cols)
    main, factor, halo, rim = pl.pallas_call(
        scoped(functools.partial(binning, n_xl, n_ta), pltpu.SemaphoreType.DMA((10,)), pltpu.SemaphoreType.REGULAR((2,)),
               pltpu.SemaphoreType.DMA((9,))),
        out_shape=(pltpu.VMEM((n_pairs, own_cols, out_span), F32), pltpu.VMEM((n_pairs, own_cols, LANES), F32),
                   pltpu.VMEM((2, n_pairs, REACH, LANES), F32), pltpu.VMEM((2 * n_pairs, LANES), F32)),
        in_specs=[hbm] * 3,
        out_specs=[vmem] * 4,
        scratch_shapes=[
            pltpu.VMEM((n_rows, n_cols, LANES), F32),
            pltpu.VMEM((n_rows, n_cols, span - LANES), F32),
            pltpu.VMEM((2, n_rows, 8, span), F32),
            pltpu.VMEM((2, n_rows, n_cols), jnp.int32),
            pltpu.VMEM(tables.shape, BF16),
            pltpu.VMEM((3, n_rows, LANES), jnp.int32),
            pltpu.VMEM((n_pairs, 3 * height_a, 2 * (stop_a - start_a)), BF16),
            pltpu.VMEM((n_pairs, 3 * height_b, 2 * (stop_b - start_b)), BF16),
            pltpu.VMEM((n_pairs + 2, own_cols, width), F32),
            pltpu.VMEM((2, n_pairs, width), F32),
            pltpu.VMEM((2, 1, width), F32),
            pltpu.VMEM((2, n_pairs, width), F32),
            pltpu.VMEM((2, 1, width), F32),
            pltpu.VMEM((own_cols, width), F32),
            pltpu.VMEM((2, n_pairs + 1, REACH, LANES), F32),
            pltpu.VMEM((2, n_pairs + 1, REACH, LANES), F32),
            pltpu.VMEM((n_pairs + 1, 1, width), F32),
            pltpu.VMEM((2, 2, n_pairs, LANES), F32),
            pltpu.VMEM((2, 2, 1, LANES), F32),
        ],
        compiler_params=pltpu.CompilerParams(collective_id=0, has_side_effects=True, vmem_limit_bytes=24 * 2**20),
        name="binning",
    )(*[pltpu.with_memory_space_constraint(a, pltpu.HBM) for a in (traces, bin_steps, jnp.asarray(tables))])
    return pl.pallas_call(
        scoped(finish, pltpu.SemaphoreType.DMA((3,))),
        out_shape=jax.ShapeDtypeStruct((n_pairs, own_cols, out_span), F32),
        in_specs=[vmem] * 6,
        out_specs=hbm,
        scratch_shapes=[pltpu.VMEM((2, n_pairs, own_cols, LANES), F32)],
        compiler_params=pltpu.CompilerParams(vmem_limit_bytes=16 * 2**20),
        name="finish",
    )(main, factor, halo, rim, jnp.asarray(t_edge), jnp.asarray(t_rim))


def solution(mesh):
    if mesh.shape["il"] != 2:
        raise ValueError("il size")
    return jax.shard_map(
        functools.partial(shards, mesh.shape["xl"], mesh.shape["ta"]),
        mesh=mesh,
        in_specs=(P("il", "xl", "ta"), P(None, "il", "xl")),
        out_specs=P("il", "xl", "ta"),
        check_vma=False,
    )
```

```python
import functools

import numpy as np
import jax
import jax.numpy as jnp
from jax import lax
from jax.experimental import pallas as pl
from jax.experimental.pallas import tpu as pltpu
from jax.sharding import PartitionSpec as P

TAPS = 16
P_SIZE = 3
Q = 2
REACH = TAPS // 2
LANES = 128
LOADS = 4
MESH = pl.DeviceIdType.MESH
F32, BF16 = jnp.float32, jnp.bfloat16


def lanczos_table(span):
    rows = np.arange(span + 2 * REACH)[:, None] - REACH
    cols = np.arange(span * P_SIZE // Q)[None, :]
    offset = (cols * Q - rows * P_SIZE).astype(np.float64) / P_SIZE
    weights = np.sinc(offset) * np.sinc(offset / REACH)
    return np.where(np.abs(offset) < REACH, weights, 0.0).astype(np.float32)


def split_table(table):
    high = table.astype(BF16)
    low = (table - high.astype(np.float32)).astype(BF16)
    return high, low


def halves(values):
    high = values.astype(BF16)
    low = (values - high.astype(F32)).astype(BF16)
    return high, low


def dot(a, b):
    return jnp.dot(a, b, preferred_element_type=F32)


def column_ranges(n_cols):
    own_cols, rest = n_cols // 2, n_cols - LANES
    if own_cols % 8 or rest % 16 or not LANES < 2 * rest <= 2 * LANES:
        raise ValueError("column count")
    height = (LANES // 2 + 1 + 7) // 8 * 8
    first = (LANES // 2 - 1) // 8 * 8
    return (0, LANES, 0, height), (LANES, n_cols, first, own_cols - first)


def scoped(kernel, *semaphores):
    def run(*refs):
        pl.run_scoped(lambda *scratch: kernel(*refs, *scratch), *semaphores)
    return run


def binning(n_xl, n_ta, traces, steps_hbm, tables_hbm, main, factor, halo_out, rim_out,
            x_left, x_right, edge_x, steps, tables, keys, hot_a, hot_b, acc,
            rim_send, corner_send, rim_recv, corner_recv, il_recv, halo_send, halo_recv, wide_rows,
            diag_recv, diag_corner, load_sem, late_sem, recv_sem):
    n_rows, n_cols, _ = x_left.shape
    span = LANES + x_right.shape[2]
    n_pairs, own_cols = n_rows // 2, n_cols // 2
    il, xl, ta = lax.axis_index("il"), lax.axis_index("xl"), lax.axis_index("ta")
    other = 1 - il
    has_xl, has_ta = (xl < n_xl - 1, xl > 0), (ta < n_ta - 1, ta > 0)
    xl_at, ta_at = (xl + 1, xl - 1), (ta + 1, ta - 1)
    ranges = column_ranges(n_cols)

    def when(condition, work):
        pl.when(condition)(work)

    step_load = pltpu.make_async_copy(steps_hbm, steps, load_sem.at[3])
    step_load.start()
    edge_loads = [pltpu.make_async_copy(traces.at[:, pl.ds(start, 8)], edge_x.at[d], load_sem.at[4 + d])
                  for d, start in enumerate((n_cols - 8, 0))]
    for load in edge_loads:
        load.start()

    def load_samples(x, start, rows, slot):
        samples = pl.ds(start, x.shape[2])
        return pltpu.make_async_copy(traces.at[rows, :, samples], x.at[rows], load_sem.at[slot])

    table_load = pltpu.make_async_copy(tables_hbm, tables, load_sem.at[2])

    barrier = pltpu.get_barrier_semaphore()

    def greet(has, partner):
        def signal():
            pl.semaphore_signal(barrier, inc=1, device_id=partner, device_id_type=MESH)
            pl.semaphore_signal(barrier, inc=1, device_id={"il": other, **partner}, device_id_type=MESH)
        when(has, signal)

    for d in (1, 0):
        greet(has_xl[d], {"xl": xl_at[d]})
    for d in (1, 0):
        greet(has_xl[0] & has_ta[d], {"xl": xl + 1, "ta": ta_at[d]})
    for d in (1, 0):
        greet(has_ta[d], {"ta": ta_at[d]})
    pl.semaphore_signal(barrier, inc=1, device_id={"il": other}, device_id_type=MESH)
    count_xl, count_ta = [sum(jnp.where(has, 1, 0) for has in pair) for pair in (has_xl, has_ta)]
    peers = 1 + 2 * (count_xl + count_ta + jnp.where(has_xl[1], count_ta, 0))
    quarter = n_rows // LOADS
    for p in range(LOADS):
        load_samples(x_left, 0, pl.ds(quarter * p, quarter), 0).start()

    for e in range(2):
        def no_ta(e=e):
            halo_recv[e] = jnp.zeros_like(halo_recv[e])
        when(jnp.logical_not(has_ta[1 - e]), no_ta)
    for d in range(2):
        def no_xl(d=d):
            rim_recv[d] = jnp.zeros_like(rim_recv[d])
            corner_recv[d] = jnp.zeros_like(corner_recv[d])
        when(jnp.logical_not(has_xl[1 - d]), no_xl)
        for e in range(2):
            def no_diag(d=d, e=e):
                diag_recv[d, e] = jnp.zeros_like(diag_recv[d, e])
                diag_corner[d, e] = jnp.zeros_like(diag_corner[d, e])
            when(jnp.logical_not(has_xl[1 - d] & has_ta[1 - e]), no_diag)

    lane = lax.broadcasted_iota(jnp.int32, (1, LANES), 1)
    is_first, is_last = lane < REACH, lane >= LANES - REACH
    step_load.wait()
    col = lax.broadcasted_iota(jnp.int32, (n_rows, n_cols), 1)
    row = lax.broadcasted_iota(jnp.int32, (n_rows, n_cols), 0)
    bin_col = lax.shift_right_logical(col, 1) + steps[1]
    bin_row = steps[0] + 1
    own = (bin_col >= 0) & (bin_col < own_cols)
    code_a, code_b = [jnp.where(own, bin_row * height + bin_col - first, -1)[:, start:stop]
                      for start, stop, first, height in ranges]
    rest = n_cols - LANES
    keys[0] = code_a
    padded = jnp.concatenate([code_b, jnp.full((n_rows, LANES - rest), -1, jnp.int32)], axis=1)
    keys[1] = padded
    keys[2] = pltpu.roll(padded, rest, 1)

    def one_hot(key, height):
        rows = lax.broadcasted_iota(jnp.int32, (height, key.shape[1]), 0)
        return jnp.where(rows == key, 1.0, 0.0).astype(BF16)

    for p in range(n_pairs):
        key = jnp.concatenate([keys[0, 2 * p: 2 * p + 1], keys[0, 2 * p + 1: 2 * p + 2]], axis=1)
        hot_a[p] = one_hot(key, 3 * ranges[0][3])
        second = keys[2, 2 * p + 1: 2 * p + 2]
        key = jnp.concatenate([jnp.where(lane < rest, keys[1, 2 * p: 2 * p + 1], second),
                               second[:, :2 * rest - LANES]], axis=1)
        hot_b[p] = one_hot(key, 3 * ranges[1][3])
    rim_bin = bin_row - 1 + lax.shift_right_logical(row, 1)
    outside = jnp.where(il == 0, n_pairs, -1)
    rim_code = jnp.where(rim_bin == outside, n_pairs, jnp.where((rim_bin < 0) | (rim_bin >= n_pairs), -1, rim_bin))
    for load in edge_loads:
        load.wait()
    for d, (start, column) in enumerate(((n_cols - 8, own_cols), (0, -1))):
        target = jnp.where(bin_col == column, rim_code, -1)
        key = jnp.concatenate([target[i: i + 1, start: start + 8] for i in range(n_rows)], axis=1)
        chosen = one_hot(key, n_pairs + 8)
        high, low = halves(edge_x[d].reshape(n_rows * 8, span))
        sums = dot(chosen, high) + dot(chosen, low)
        folds = dot(chosen, jnp.ones((n_rows * 8, LANES), BF16))
        ends = jnp.where(is_first, sums[:, :LANES], jnp.where(is_last, sums[:, span - LANES:], folds))
        rim_send[d, :, :span] = sums[:n_pairs]
        rim_send[d, :, span:] = ends[:n_pairs]
        corner_send[d, :, :span] = sums[n_pairs: n_pairs + 1]
        corner_send[d, :, span:] = ends[n_pairs: n_pairs + 1]

    hots = (hot_a, hot_b)
    for p in range(LOADS):
        load_samples(x_right, LANES, pl.ds(quarter * p, quarter), 1).start()
    table_load.start()

    def merge(p, r, parts, lanes):
        (_, _, _, height), (_, _, first, _) = ranges
        a, b = parts
        both = a[first:] + b[: height - first]
        for at, part in ((0, a[:first]), (first, both), (height, b[height - first:])):
            where = (p + r, slice(at, at + part.shape[0]), lanes)
            acc[where] = part if p == 0 or r == 2 else acc[where] + part

    def groups(parts, r):
        return [part[r * height: (r + 1) * height] for part, (_, _, _, height) in zip(parts, ranges)]

    def bin_pair(p, x, lanes):
        parts, wide = [], x.shape[2]
        for hot, (start, stop, _, _) in zip(hots, ranges):
            high, low = halves(jnp.concatenate([x[2 * p, start:stop], x[2 * p + 1, start:stop]], axis=0))
            sums = dot(hot[p], jnp.concatenate([high, low], axis=1))
            parts.append(sums[:, :wide] + sums[:, wide:])
        for r in range(3):
            merge(p, r, groups(parts, r), lanes)

    ends = (0, 0), (n_pairs - 1, 2)

    def count_pair(p):
        parts = [dot(hot[p], jnp.ones((hot.shape[2], LANES), BF16)) for hot in hots]
        for r in range(3):
            if (p, r) not in ends:
                merge(p, r, groups(parts, r), slice(span, span + LANES))

    def send_sem(slot):
        return load_sem.at[(6, 7, 3, 8, 0, 1, 9, 4, 5)[slot]]

    def remote(src, dst, slot, partner):
        return pltpu.make_async_remote_copy(src_ref=src, dst_ref=dst, send_sem=send_sem(slot), recv_sem=recv_sem.at[slot],
                                            device_id=partner, device_id_type=MESH)

    rim_row = jnp.where(il == 0, n_pairs + 1, 0)
    own_row = jnp.where(il == 0, n_pairs - 1, 0)
    to_other = remote(acc.at[rim_row], il_recv, 0, {"il": other})

    rims, halos, diags = [], [], {}
    for d in range(2):
        to, rows = {"xl": xl_at[d]}, pl.ds(0, n_pairs)
        rims.append((remote(rim_send.at[d], rim_recv.at[d], 1 + d, to),
                     remote(corner_send.at[d], corner_recv.at[d], 1 + d, {"il": other, **to})))
        to = {"ta": ta_at[d]}
        halos.append((remote(halo_send.at[d, rows], halo_recv.at[d, rows], 3 + d, to),
                      remote(halo_send.at[d, n_pairs], halo_recv.at[d, n_pairs], 3 + d, {"il": other, **to})))
        for e in range(2):
            to, end, slot = {"xl": xl_at[d], "ta": ta_at[e]}, pl.ds(span, LANES), 5 + 2 * d + e
            diags[d, e] = (remote(rim_send.at[d, :, end], diag_recv.at[d, e], slot, to),
                           remote(corner_send.at[d, :, end], diag_corner.at[d, e], slot, {"il": other, **to}))

    def received(slot):
        return recv_sem.at[slot]

    def wait_all(semaphores, slot, rows):
        pltpu.make_async_copy(rows, rows, semaphores(slot)).wait()

    def wait_rims(semaphores, d):
        wait_all(semaphores, 1 + d, wide_rows)

    def wait_halos(semaphores, e):
        wait_all(semaphores, 3 + e, halo_recv.at[e])

    def wait_diags(semaphores, d, e):
        wait_all(semaphores, 5 + 2 * d + e, wide_rows.at[:, :, pl.ds(0, LANES)])

    def start_all(copies):
        for copy in copies:
            copy.start()

    def pack_halo(e):
        lanes = slice(0, LANES) if e else slice(span - LANES, span)
        rows = slice(0, REACH) if e else slice(LANES - REACH, LANES)
        for b in range(n_pairs):
            halo_send[e, b, :, :own_cols] = acc[b + 1, :, lanes].T[rows]
        halo_send[e, n_pairs, :, :own_cols] = acc[rim_row, :, lanes].T[rows]

    def send_diags(d):
        for e in (1, 0):
            when(has_ta[e], lambda e=e: start_all(diags[d, e]))

    def send_rims(d):
        send_diags(d)
        start_all(rims[d])

    def late(e):
        def go():
            pl.semaphore_wait(late_sem.at[e], 1)
            when(has_xl[0], lambda: start_all(diags[0, e]))
        when(has_ta[e], go)

    every_row = pl.ds(0, n_rows)
    pl.semaphore_wait(barrier, peers)
    when(has_xl[1], lambda: send_rims(1))
    for e in range(2):
        when(has_ta[e], lambda e=e: pl.semaphore_signal(late_sem.at[1 - e], inc=1, device_id={"ta": ta_at[e]},
                                                        device_id_type=MESH))
    when(has_xl[0], lambda: start_all(rims[0]))
    load_samples(x_left, 0, every_row, 0).wait()
    for p in range(n_pairs):
        bin_pair(p, x_left, slice(0, LANES))
    pack_halo(1)
    when(has_ta[1] & (il == 0), lambda: start_all(halos[1]))
    late(1)
    load_samples(x_right, LANES, every_row, 1).wait()
    when(has_ta[1] & (il == 1), lambda: start_all(halos[1]))
    for p in range(n_pairs):
        bin_pair(p, x_right, slice(LANES, span))

    first = (xl == 0) & (ta == 0)
    when(jnp.logical_not(first), lambda: late(0))
    for p, r in ends:
        chosen = [hot[p, r * height: (r + 1) * height] for hot, (_, _, _, height) in zip(hots, ranges)]
        merge(p, r, [dot(part, jnp.ones((part.shape[1], LANES), BF16)) for part in chosen], slice(span, span + LANES))
    to_other.start()
    pack_halo(0)
    when(has_ta[0], lambda: start_all(halos[0]))
    for p in range(n_pairs):
        count_pair(p)
    when(first, lambda: late(0))

    def resample(values):
        high, low = halves(values)
        return dot(high, tables[0]) + (dot(low, tables[0]) + dot(high, tables[1]))

    table_load.wait()
    for i in range(n_pairs):
        b = jnp.where(il == 0, i, n_pairs - 1 - i)
        if i == n_pairs - 1:
            to_other.wait_recv()
            acc[b + 1] = acc[b + 1] + il_recv[...]
        main[b] = resample(acc[b + 1, :, :span])
    for d in range(2):
        when(has_xl[1 - d], lambda d=d: wait_rims(received, d))
    sub = lax.broadcasted_iota(jnp.int32, (n_pairs, 1), 0)
    rim = jnp.concatenate([rim_recv[d] + jnp.where(sub == own_row, corner_recv[d], 0.0) for d in range(2)], axis=0)
    more = resample(rim[:, :span])
    more_fold = jnp.broadcast_to(rim[:, span + LANES // 2: span + LANES // 2 + 1], (2 * n_pairs, LANES))
    ends_row = lax.broadcasted_iota(jnp.int32, (8, 1), 0)
    tops = ((0, 0, 0), (own_cols - 8, 7, n_pairs))

    def add_rows(values, extra, b):
        top, bottom = [values[at: at + 8] + jnp.where(ends_row == where, extra[base + b: base + b + 1], 0.0)
                       for at, where, base in tops]
        return jnp.concatenate([top, values[8: own_cols - 8], bottom], axis=0)

    for b in range(n_pairs):
        scale = 1.0 / jnp.maximum(add_rows(acc[b + 1, :, span:], more_fold, b), 1.0)
        factor[b] = scale
        main[b] = add_rows(main[b], more, b) * jnp.concatenate([scale] * (main.shape[2] // LANES), axis=1)

    to_other.wait_send()
    for d in range(2):
        when(has_xl[d], lambda d=d: wait_rims(send_sem, d))
        when(has_ta[d], lambda d=d: wait_halos(send_sem, d))
        for e in range(2):
            when(has_xl[d] & has_ta[e], lambda d=d, e=e: wait_diags(send_sem, d, e))

    for d in range(2):
        for e in range(2):
            when(has_xl[1 - d] & has_ta[1 - e], lambda d=d, e=e: wait_diags(received, d, e))
    for d in range(2):
        first, last = [diag_recv[d, e] + jnp.where(sub == own_row, diag_corner[d, e], 0.0) for e in (1, 0)]
        rim_out[d * n_pairs: (d + 1) * n_pairs] = jnp.where(is_first, first, jnp.where(is_last, last, 0.0))
    for e in range(2):
        when(has_ta[1 - e], lambda e=e: wait_halos(received, e))
        halo_out[e] = halo_recv[e, :n_pairs]
        halo_out[e, own_row] = halo_recv[e, own_row] + halo_recv[e, n_pairs]


def finish(main, factor, halo, rim, t_edge, t_rim, out, staged, out_sem):
    n_pairs, own_cols, width = main.shape
    starts = (0, width - LANES)
    has_before = lax.axis_index("ta") > 0

    def write_tiles(source, start, size, slot):
        return pltpu.make_async_copy(source, out.at[:, :, pl.ds(start, size)], out_sem.at[slot])

    def from_main(start, size, slot):
        return write_tiles(main.at[:, :, pl.ds(start, size)], start, size, slot)

    from_main(LANES, width - 2 * LANES, 2).start()
    pl.when(jnp.logical_not(has_before))(from_main(0, LANES, 0).start)
    ends_row = lax.broadcasted_iota(jnp.int32, (8, 1), 0)
    tops = ((0, 0, 0), (own_cols - 8, 7, n_pairs))

    def add_halo(tiles, table):
        high = rim[...].astype(BF16)
        low = (rim[...] - high.astype(F32)).astype(BF16)
        more = dot(jnp.concatenate([high, low, high], axis=1), t_rim[...])
        for pair in zip(tiles[::2], tiles[1::2]):
            terms = []
            for d, b in pair:
                high = halo[d, b].astype(BF16).astype(F32)
                terms += [high, halo[d, b] - high, high]
            both = dot(jnp.concatenate(terms, axis=0).T[:own_cols].astype(BF16), t_edge[table])
            for i, (d, b) in enumerate(pair):
                ends, lanes = both[:, i * LANES: (i + 1) * LANES], slice(d * LANES, (d + 1) * LANES)
                top, bottom = [ends[at: at + 8] + jnp.where(ends_row == where, more[base + b: base + b + 1, lanes], 0.0)
                               for at, where, base in tops]
                ends = jnp.concatenate([top, ends[8: own_cols - 8], bottom], axis=0)
                staged[d, b] = main[b, :, starts[d]: starts[d] + LANES] + ends * factor[b]
                pltpu.make_async_copy(staged.at[d, b], out.at[b, :, pl.ds(starts[d], LANES)], out_sem.at[d]).start()

    rows = range(n_pairs)
    pl.when(has_before)(lambda: add_halo([(d, b) for b in rows for d in range(2)], 0))
    pl.when(jnp.logical_not(has_before))(lambda: add_halo([(1, b) for b in rows], 1))
    from_main(LANES, width - 2 * LANES, 2).wait()
    for d in range(2):
        write_tiles(staged.at[d], starts[d], LANES, d).wait()


def shards(n_xl, n_ta, traces, bin_steps):
    n_rows, n_cols, span = traces.shape
    n_pairs, own_cols = n_rows // 2, n_cols // 2
    width = span + LANES
    out_span = span * P_SIZE // Q
    if n_pairs % 8 or span % LANES or out_span % LANES or out_span < 3 * LANES:
        raise ValueError("block shape")
    table = lanczos_table(span)
    tables = np.stack(split_table(table[REACH:-REACH]))
    edge_cols = np.concatenate([table[:, :LANES], table[:, -LANES:]], axis=1)
    edge_high, edge_low = split_table(np.stack([edge_cols[:REACH, :LANES], edge_cols[-REACH:, LANES:]]))
    before, after = np.concatenate([edge_high, edge_high, edge_low], axis=1)
    none = np.zeros_like(before)
    t_edge = np.stack([np.block([[first, none], [none, after]]) for first in (before, after)])
    rim_high, rim_low = split_table(np.concatenate(
        [edge_cols[-REACH:], np.zeros((LANES - 2 * REACH, 2 * LANES), np.float32), edge_cols[:REACH]]))
    t_rim = np.concatenate([rim_high, rim_high, rim_low])
    vmem = pl.BlockSpec(memory_space=pltpu.VMEM)
    hbm = pl.BlockSpec(memory_space=pltpu.HBM)
    (start_a, stop_a, _, height_a), (start_b, stop_b, _, height_b) = column_ranges(n_cols)
    main, factor, halo, rim = pl.pallas_call(
        scoped(functools.partial(binning, n_xl, n_ta), pltpu.SemaphoreType.DMA((10,)), pltpu.SemaphoreType.REGULAR((2,)),
               pltpu.SemaphoreType.DMA((9,))),
        out_shape=(pltpu.VMEM((n_pairs, own_cols, out_span), F32), pltpu.VMEM((n_pairs, own_cols, LANES), F32),
                   pltpu.VMEM((2, n_pairs, REACH, LANES), F32), pltpu.VMEM((2 * n_pairs, LANES), F32)),
        in_specs=[hbm] * 3,
        out_specs=[vmem] * 4,
        scratch_shapes=[
            pltpu.VMEM((n_rows, n_cols, LANES), F32),
            pltpu.VMEM((n_rows, n_cols, span - LANES), F32),
            pltpu.VMEM((2, n_rows, 8, span), F32),
            pltpu.VMEM((2, n_rows, n_cols), jnp.int32),
            pltpu.VMEM(tables.shape, BF16),
            pltpu.VMEM((3, n_rows, LANES), jnp.int32),
            pltpu.VMEM((n_pairs, 3 * height_a, 2 * (stop_a - start_a)), BF16),
            pltpu.VMEM((n_pairs, 3 * height_b, 2 * (stop_b - start_b)), BF16),
            pltpu.VMEM((n_pairs + 2, own_cols, width), F32),
            pltpu.VMEM((2, n_pairs, width), F32),
            pltpu.VMEM((2, 1, width), F32),
            pltpu.VMEM((2, n_pairs, width), F32),
            pltpu.VMEM((2, 1, width), F32),
            pltpu.VMEM((own_cols, width), F32),
            pltpu.VMEM((2, n_pairs + 1, REACH, LANES), F32),
            pltpu.VMEM((2, n_pairs + 1, REACH, LANES), F32),
            pltpu.VMEM((n_pairs + 1, 1, width), F32),
            pltpu.VMEM((2, 2, n_pairs, LANES), F32),
            pltpu.VMEM((2, 2, 1, LANES), F32),
        ],
        compiler_params=pltpu.CompilerParams(collective_id=0, has_side_effects=True, vmem_limit_bytes=24 * 2**20),
        name="binning",
    )(*[pltpu.with_memory_space_constraint(a, pltpu.HBM) for a in (traces, bin_steps, jnp.asarray(tables))])
    return pl.pallas_call(
        scoped(finish, pltpu.SemaphoreType.DMA((3,))),
        out_shape=jax.ShapeDtypeStruct((n_pairs, own_cols, out_span), F32),
        in_specs=[vmem] * 6,
        out_specs=hbm,
        scratch_shapes=[pltpu.VMEM((2, n_pairs, own_cols, LANES), F32)],
        compiler_params=pltpu.CompilerParams(vmem_limit_bytes=16 * 2**20),
        name="finish",
    )(main, factor, halo, rim, jnp.asarray(t_edge), jnp.asarray(t_rim))


def solution(mesh):
    if mesh.shape["il"] != 2:
        raise ValueError("il size")
    return jax.shard_map(
        functools.partial(shards, mesh.shape["xl"], mesh.shape["ta"]),
        mesh=mesh,
        in_specs=(P("il", "xl", "ta"), P(None, "il", "xl")),
        out_specs=P("il", "xl", "ta"),
        check_vma=False,
    )
```

```python
import functools

import numpy as np
import jax
import jax.numpy as jnp
from jax import lax
from jax.experimental import pallas as pl
from jax.experimental.pallas import tpu as pltpu
from jax.sharding import PartitionSpec as P

TAPS = 16
P_SIZE = 3
Q = 2
REACH = TAPS // 2
LANES = 128
LOADS = 4
MESH = pl.DeviceIdType.MESH
F32, BF16 = jnp.float32, jnp.bfloat16


def lanczos_table(span):
    rows = np.arange(span + 2 * REACH)[:, None] - REACH
    cols = np.arange(span * P_SIZE // Q)[None, :]
    offset = (cols * Q - rows * P_SIZE).astype(np.float64) / P_SIZE
    weights = np.sinc(offset) * np.sinc(offset / REACH)
    return np.where(np.abs(offset) < REACH, weights, 0.0).astype(np.float32)


def split_table(table):
    high = table.astype(BF16)
    low = (table - high.astype(np.float32)).astype(BF16)
    return high, low


def halves(values):
    high = values.astype(BF16)
    low = (values - high.astype(F32)).astype(BF16)
    return high, low


def dot(a, b):
    return jnp.dot(a, b, preferred_element_type=F32)


def column_ranges(n_cols):
    own_cols, rest = n_cols // 2, n_cols - LANES
    if own_cols % 8 or rest % 16 or not LANES < 2 * rest <= 2 * LANES:
        raise ValueError("column count")
    height = (LANES // 2 + 1 + 7) // 8 * 8
    first = (LANES // 2 - 1) // 8 * 8
    return (0, LANES, 0, height), (LANES, n_cols, first, own_cols - first)


def scoped(kernel, *semaphores):
    def run(*refs):
        pl.run_scoped(lambda *scratch: kernel(*refs, *scratch), *semaphores)
    return run


def binning(n_xl, n_ta, traces, steps_hbm, tables_hbm, main, factor, halo_out, rim_out,
            x_left, x_right, edge_x, steps, tables, keys, hot_a, hot_b, acc,
            rim_send, corner_send, rim_recv, corner_recv, il_recv, halo_send, halo_recv, wide_rows,
            diag_recv, diag_corner, load_sem, late_sem, recv_sem):
    n_rows, n_cols, _ = x_left.shape
    span = LANES + x_right.shape[2]
    n_pairs, own_cols = n_rows // 2, n_cols // 2
    il, xl, ta = lax.axis_index("il"), lax.axis_index("xl"), lax.axis_index("ta")
    other = 1 - il
    has_xl, has_ta = (xl < n_xl - 1, xl > 0), (ta < n_ta - 1, ta > 0)
    xl_at, ta_at = (xl + 1, xl - 1), (ta + 1, ta - 1)
    ranges = column_ranges(n_cols)

    def when(condition, work):
        pl.when(condition)(work)

    barrier = pltpu.get_barrier_semaphore()

    def greet(has, partner):
        def signal():
            pl.semaphore_signal(barrier, inc=1, device_id=partner, device_id_type=MESH)
            pl.semaphore_signal(barrier, inc=1, device_id={"il": other, **partner}, device_id_type=MESH)
        when(has, signal)

    greet(has_ta[1], {"ta": ta - 1})
    greet(has_xl[1], {"xl": xl - 1})
    greet(has_xl[0] & has_ta[1], {"xl": xl + 1, "ta": ta - 1})

    step_load = pltpu.make_async_copy(steps_hbm, steps, load_sem.at[3])
    step_load.start()
    edge_loads = [pltpu.make_async_copy(traces.at[:, pl.ds(start, 8)], edge_x.at[d], load_sem.at[4 + d])
                  for d, start in enumerate((n_cols - 8, 0))]
    for load in edge_loads:
        load.start()

    def load_samples(x, start, rows, slot):
        samples = pl.ds(start, x.shape[2])
        return pltpu.make_async_copy(traces.at[rows, :, samples], x.at[rows], load_sem.at[slot])

    table_load = pltpu.make_async_copy(tables_hbm, tables, load_sem.at[2])

    quarter = n_rows // LOADS
    for p in range(LOADS):
        load_samples(x_left, 0, pl.ds(quarter * p, quarter), 0).start()

    greet(has_xl[0] & has_ta[0], {"xl": xl + 1, "ta": ta + 1})
    greet(has_xl[0], {"xl": xl + 1})
    greet(has_ta[0], {"ta": ta + 1})
    pl.semaphore_signal(barrier, inc=1, device_id={"il": other}, device_id_type=MESH)
    count_xl, count_ta = [sum(jnp.where(has, 1, 0) for has in pair) for pair in (has_xl, has_ta)]
    peers = 1 + 2 * (count_xl + count_ta + jnp.where(has_xl[1], count_ta, 0))

    for e in range(2):
        def no_ta(e=e):
            halo_recv[e] = jnp.zeros_like(halo_recv[e])
        when(jnp.logical_not(has_ta[1 - e]), no_ta)
    for d in range(2):
        def no_xl(d=d):
            rim_recv[d] = jnp.zeros_like(rim_recv[d])
            corner_recv[d] = jnp.zeros_like(corner_recv[d])
        when(jnp.logical_not(has_xl[1 - d]), no_xl)
        for e in range(2):
            def no_diag(d=d, e=e):
                diag_recv[d, e] = jnp.zeros_like(diag_recv[d, e])
                diag_corner[d, e] = jnp.zeros_like(diag_corner[d, e])
            when(jnp.logical_not(has_xl[1 - d] & has_ta[1 - e]), no_diag)

    lane = lax.broadcasted_iota(jnp.int32, (1, LANES), 1)
    is_first, is_last = lane < REACH, lane >= LANES - REACH
    step_load.wait()
    col = lax.broadcasted_iota(jnp.int32, (n_rows, n_cols), 1)
    row = lax.broadcasted_iota(jnp.int32, (n_rows, n_cols), 0)
    bin_col = lax.shift_right_logical(col, 1) + steps[1]
    bin_row = steps[0] + 1
    own = (bin_col >= 0) & (bin_col < own_cols)
    code_a, code_b = [jnp.where(own, bin_row * height + bin_col - first, -1)[:, start:stop]
                      for start, stop, first, height in ranges]
    rest = n_cols - LANES
    keys[0] = code_a
    padded = jnp.concatenate([code_b, jnp.full((n_rows, LANES - rest), -1, jnp.int32)], axis=1)
    keys[1] = padded
    keys[2] = pltpu.roll(padded, rest, 1)

    def one_hot(key, height):
        rows = lax.broadcasted_iota(jnp.int32, (height, key.shape[1]), 0)
        return jnp.where(rows == key, 1.0, 0.0).astype(BF16)

    for p in range(n_pairs):
        key = jnp.concatenate([keys[0, 2 * p: 2 * p + 1], keys[0, 2 * p + 1: 2 * p + 2]], axis=1)
        hot_a[p] = one_hot(key, 3 * ranges[0][3])
        second = keys[2, 2 * p + 1: 2 * p + 2]
        key = jnp.concatenate([jnp.where(lane < rest, keys[1, 2 * p: 2 * p + 1], second),
                               second[:, :2 * rest - LANES]], axis=1)
        hot_b[p] = one_hot(key, 3 * ranges[1][3])
    rim_bin = bin_row - 1 + lax.shift_right_logical(row, 1)
    outside = jnp.where(il == 0, n_pairs, -1)
    rim_code = jnp.where(rim_bin == outside, n_pairs, jnp.where((rim_bin < 0) | (rim_bin >= n_pairs), -1, rim_bin))
    for load in edge_loads:
        load.wait()
    for d, (start, column) in enumerate(((n_cols - 8, own_cols), (0, -1))):
        target = jnp.where(bin_col == column, rim_code, -1)
        key = jnp.concatenate([target[i: i + 1, start: start + 8] for i in range(n_rows)], axis=1)
        chosen = one_hot(key, n_pairs + 8)
        high, low = halves(edge_x[d].reshape(n_rows * 8, span))
        sums = dot(chosen, high) + dot(chosen, low)
        folds = dot(chosen, jnp.ones((n_rows * 8, LANES), BF16))
        ends = jnp.where(is_first, sums[:, :LANES], jnp.where(is_last, sums[:, span - LANES:], folds))
        rim_send[d, :, :span] = sums[:n_pairs]
        rim_send[d, :, span:] = ends[:n_pairs]
        corner_send[d, :, :span] = sums[n_pairs: n_pairs + 1]
        corner_send[d, :, span:] = ends[n_pairs: n_pairs + 1]

    hots = (hot_a, hot_b)
    for p in range(LOADS):
        load_samples(x_right, LANES, pl.ds(quarter * p, quarter), 1).start()
    table_load.start()

    def merge(p, r, parts, lanes):
        (_, _, _, height), (_, _, first, _) = ranges
        a, b = parts
        both = a[first:] + b[: height - first]
        for at, part in ((0, a[:first]), (first, both), (height, b[height - first:])):
            where = (p + r, slice(at, at + part.shape[0]), lanes)
            acc[where] = part if p == 0 or r == 2 else acc[where] + part

    def groups(parts, r):
        return [part[r * height: (r + 1) * height] for part, (_, _, _, height) in zip(parts, ranges)]

    def bin_pair(p, x, lanes):
        parts, wide = [], x.shape[2]
        for hot, (start, stop, _, _) in zip(hots, ranges):
            high, low = halves(jnp.concatenate([x[2 * p, start:stop], x[2 * p + 1, start:stop]], axis=0))
            sums = dot(hot[p], jnp.concatenate([high, low], axis=1))
            parts.append(sums[:, :wide] + sums[:, wide:])
        for r in range(3):
            merge(p, r, groups(parts, r), lanes)

    ends = (0, 0), (n_pairs - 1, 2)

    def count_pair(p):
        parts = [dot(hot[p], jnp.ones((hot.shape[2], LANES), BF16)) for hot in hots]
        for r in range(3):
            if (p, r) not in ends:
                merge(p, r, groups(parts, r), slice(span, span + LANES))

    def send_sem(slot):
        return load_sem.at[(6, 7, 3, 8, 0, 1, 9, 4, 5)[slot]]

    def remote(src, dst, slot, partner):
        return pltpu.make_async_remote_copy(src_ref=src, dst_ref=dst, send_sem=send_sem(slot), recv_sem=recv_sem.at[slot],
                                            device_id=partner, device_id_type=MESH)

    rim_row = jnp.where(il == 0, n_pairs + 1, 0)
    own_row = jnp.where(il == 0, n_pairs - 1, 0)
    to_other = remote(acc.at[rim_row], il_recv, 0, {"il": other})

    rims, halos, diags = [], [], {}
    for d in range(2):
        to, rows = {"xl": xl_at[d]}, pl.ds(0, n_pairs)
        rims.append((remote(rim_send.at[d], rim_recv.at[d], 1 + d, to),
                     remote(corner_send.at[d], corner_recv.at[d], 1 + d, {"il": other, **to})))
        to = {"ta": ta_at[d]}
        halos.append((remote(halo_send.at[d, rows], halo_recv.at[d, rows], 3 + d, to),
                      remote(halo_send.at[d, n_pairs], halo_recv.at[d, n_pairs], 3 + d, {"il": other, **to})))
        for e in range(2):
            to, end, slot = {"xl": xl_at[d], "ta": ta_at[e]}, pl.ds(span, LANES), 5 + 2 * d + e
            diags[d, e] = (remote(rim_send.at[d, :, end], diag_recv.at[d, e], slot, to),
                           remote(corner_send.at[d, :, end], diag_corner.at[d, e], slot, {"il": other, **to}))

    def received(slot):
        return recv_sem.at[slot]

    def wait_all(semaphores, slot, rows):
        pltpu.make_async_copy(rows, rows, semaphores(slot)).wait()

    def wait_rims(semaphores, d):
        wait_all(semaphores, 1 + d, wide_rows)

    def wait_halos(semaphores, e):
        wait_all(semaphores, 3 + e, halo_recv.at[e])

    def wait_diags(semaphores, d, e):
        wait_all(semaphores, 5 + 2 * d + e, wide_rows.at[:, :, pl.ds(0, LANES)])

    def start_all(copies):
        for copy in copies:
            copy.start()

    def pack_halo(e):
        lanes = slice(0, LANES) if e else slice(span - LANES, span)
        rows = slice(0, REACH) if e else slice(LANES - REACH, LANES)
        for b in range(n_pairs):
            halo_send[e, b, :, :own_cols] = acc[b + 1, :, lanes].T[rows]
        halo_send[e, n_pairs, :, :own_cols] = acc[rim_row, :, lanes].T[rows]

    def send_diags(d):
        for e in (1, 0):
            when(has_ta[e], lambda e=e: start_all(diags[d, e]))

    def send_rims(d):
        send_diags(d)
        start_all(rims[d])

    def late(e):
        def go():
            pl.semaphore_wait(late_sem.at[e], 1)
            when(has_xl[0], lambda: start_all(diags[0, e]))
        when(has_ta[e], go)

    every_row = pl.ds(0, n_rows)
    def bin_left():
        load_samples(x_left, 0, every_row, 0).wait()
        for p in range(n_pairs):
            bin_pair(p, x_left, slice(0, LANES))
        pack_halo(1)

    first = (xl == 0) & (ta == 0)
    opens_late = first | (xl >= 2)
    when(opens_late, bin_left)
    pl.semaphore_wait(barrier, peers)
    when(has_xl[1], lambda: send_rims(1))
    for e in range(2):
        when(has_ta[e], lambda e=e: pl.semaphore_signal(late_sem.at[1 - e], inc=1, device_id={"ta": ta_at[e]},
                                                        device_id_type=MESH))
    when(has_xl[0], lambda: start_all(rims[0]))
    when(jnp.logical_not(opens_late), bin_left)
    when(has_ta[1], halos[1][1].start)
    when(has_ta[1], halos[1][0].start)
    late(1)
    load_samples(x_right, LANES, every_row, 1).wait()
    for p in range(n_pairs):
        bin_pair(p, x_right, slice(LANES, span))

    when(jnp.logical_not(opens_late), lambda: late(0))
    pack_halo(0)
    when(has_ta[0], lambda: start_all(halos[0]))
    when(xl >= 2, lambda: late(0))
    for p, r in ends:
        chosen = [hot[p, r * height: (r + 1) * height] for hot, (_, _, _, height) in zip(hots, ranges)]
        merge(p, r, [dot(part, jnp.ones((part.shape[1], LANES), BF16)) for part in chosen], slice(span, span + LANES))
    to_other.start()
    for p in range(n_pairs):
        count_pair(p)
    when(first, lambda: late(0))

    def resample(values):
        high, low = halves(values)
        return dot(high, tables[0]) + (dot(low, tables[0]) + dot(high, tables[1]))

    table_load.wait()
    for i in range(n_pairs):
        b = jnp.where(il == 0, i, n_pairs - 1 - i)
        if i == n_pairs - 1:
            to_other.wait_recv()
            acc[b + 1] = acc[b + 1] + il_recv[...]
        main[b] = resample(acc[b + 1, :, :span])
    for d in range(2):
        when(has_xl[1 - d], lambda d=d: wait_rims(received, d))
    sub = lax.broadcasted_iota(jnp.int32, (n_pairs, 1), 0)
    rim = jnp.concatenate([rim_recv[d] + jnp.where(sub == own_row, corner_recv[d], 0.0) for d in range(2)], axis=0)
    more = resample(rim[:, :span])
    more_fold = jnp.broadcast_to(rim[:, span + LANES // 2: span + LANES // 2 + 1], (2 * n_pairs, LANES))
    ends_row = lax.broadcasted_iota(jnp.int32, (8, 1), 0)
    tops = ((0, 0, 0), (own_cols - 8, 7, n_pairs))

    def add_rows(values, extra, b):
        top, bottom = [values[at: at + 8] + jnp.where(ends_row == where, extra[base + b: base + b + 1], 0.0)
                       for at, where, base in tops]
        return jnp.concatenate([top, values[8: own_cols - 8], bottom], axis=0)

    for b in range(n_pairs):
        scale = 1.0 / jnp.maximum(add_rows(acc[b + 1, :, span:], more_fold, b), 1.0)
        factor[b] = scale
        main[b] = add_rows(main[b], more, b) * jnp.concatenate([scale] * (main.shape[2] // LANES), axis=1)

    to_other.wait_send()
    for d in range(2):
        when(has_xl[d], lambda d=d: wait_rims(send_sem, d))
        when(has_ta[d], lambda d=d: wait_halos(send_sem, d))
        for e in range(2):
            when(has_xl[d] & has_ta[e], lambda d=d, e=e: wait_diags(send_sem, d, e))

    for d in range(2):
        for e in range(2):
            when(has_xl[1 - d] & has_ta[1 - e], lambda d=d, e=e: wait_diags(received, d, e))
    for d in range(2):
        first, last = [diag_recv[d, e] + jnp.where(sub == own_row, diag_corner[d, e], 0.0) for e in (1, 0)]
        rim_out[d * n_pairs: (d + 1) * n_pairs] = jnp.where(is_first, first, jnp.where(is_last, last, 0.0))
    for e in range(2):
        when(has_ta[1 - e], lambda e=e: wait_halos(received, e))
        halo_out[e] = halo_recv[e, :n_pairs]
        halo_out[e, own_row] = halo_recv[e, own_row] + halo_recv[e, n_pairs]


def finish(main, factor, halo, rim, t_edge, t_rim, out, staged, out_sem):
    n_pairs, own_cols, width = main.shape
    starts = (0, width - LANES)
    has_before = lax.axis_index("ta") > 0

    def write_tiles(source, start, size, slot):
        return pltpu.make_async_copy(source, out.at[:, :, pl.ds(start, size)], out_sem.at[slot])

    def from_main(start, size, slot):
        return write_tiles(main.at[:, :, pl.ds(start, size)], start, size, slot)

    from_main(LANES, width - 2 * LANES, 2).start()
    pl.when(jnp.logical_not(has_before))(from_main(0, LANES, 0).start)
    ends_row = lax.broadcasted_iota(jnp.int32, (8, 1), 0)
    tops = ((0, 0, 0), (own_cols - 8, 7, n_pairs))

    def add_halo(tiles, table):
        high = rim[...].astype(BF16)
        low = (rim[...] - high.astype(F32)).astype(BF16)
        more = dot(jnp.concatenate([high, low, high], axis=1), t_rim[...])
        for pair in zip(tiles[::2], tiles[1::2]):
            terms = []
            for d, b in pair:
                high = halo[d, b].astype(BF16).astype(F32)
                terms += [high, halo[d, b] - high, high]
            both = dot(jnp.concatenate(terms, axis=0).T[:own_cols].astype(BF16), t_edge[table])
            for i, (d, b) in enumerate(pair):
                ends, lanes = both[:, i * LANES: (i + 1) * LANES], slice(d * LANES, (d + 1) * LANES)
                top, bottom = [ends[at: at + 8] + jnp.where(ends_row == where, more[base + b: base + b + 1, lanes], 0.0)
                               for at, where, base in tops]
                ends = jnp.concatenate([top, ends[8: own_cols - 8], bottom], axis=0)
                staged[d, b] = main[b, :, starts[d]: starts[d] + LANES] + ends * factor[b]
                pltpu.make_async_copy(staged.at[d, b], out.at[b, :, pl.ds(starts[d], LANES)], out_sem.at[d]).start()

    rows = range(n_pairs)
    pl.when(has_before)(lambda: add_halo([(d, b) for b in rows for d in range(2)], 0))
    pl.when(jnp.logical_not(has_before))(lambda: add_halo([(1, b) for b in rows], 1))
    from_main(LANES, width - 2 * LANES, 2).wait()
    for d in range(2):
        write_tiles(staged.at[d], starts[d], LANES, d).wait()


def shards(n_xl, n_ta, traces, bin_steps):
    n_rows, n_cols, span = traces.shape
    n_pairs, own_cols = n_rows // 2, n_cols // 2
    width = span + LANES
    out_span = span * P_SIZE // Q
    if n_pairs % 8 or span % LANES or out_span % LANES or out_span < 3 * LANES:
        raise ValueError("block shape")
    table = lanczos_table(span)
    tables = np.stack(split_table(table[REACH:-REACH]))
    edge_cols = np.concatenate([table[:, :LANES], table[:, -LANES:]], axis=1)
    edge_high, edge_low = split_table(np.stack([edge_cols[:REACH, :LANES], edge_cols[-REACH:, LANES:]]))
    before, after = np.concatenate([edge_high, edge_high, edge_low], axis=1)
    none = np.zeros_like(before)
    t_edge = np.stack([np.block([[first, none], [none, after]]) for first in (before, after)])
    rim_high, rim_low = split_table(np.concatenate(
        [edge_cols[-REACH:], np.zeros((LANES - 2 * REACH, 2 * LANES), np.float32), edge_cols[:REACH]]))
    t_rim = np.concatenate([rim_high, rim_high, rim_low])
    vmem = pl.BlockSpec(memory_space=pltpu.VMEM)
    hbm = pl.BlockSpec(memory_space=pltpu.HBM)
    (start_a, stop_a, _, height_a), (start_b, stop_b, _, height_b) = column_ranges(n_cols)
    main, factor, halo, rim = pl.pallas_call(
        scoped(functools.partial(binning, n_xl, n_ta), pltpu.SemaphoreType.DMA((10,)), pltpu.SemaphoreType.REGULAR((2,)),
               pltpu.SemaphoreType.DMA((9,))),
        out_shape=(pltpu.VMEM((n_pairs, own_cols, out_span), F32), pltpu.VMEM((n_pairs, own_cols, LANES), F32),
                   pltpu.VMEM((2, n_pairs, REACH, LANES), F32), pltpu.VMEM((2 * n_pairs, LANES), F32)),
        in_specs=[hbm] * 3,
        out_specs=[vmem] * 4,
        scratch_shapes=[
            pltpu.VMEM((n_rows, n_cols, LANES), F32),
            pltpu.VMEM((n_rows, n_cols, span - LANES), F32),
            pltpu.VMEM((2, n_rows, 8, span), F32),
            pltpu.VMEM((2, n_rows, n_cols), jnp.int32),
            pltpu.VMEM(tables.shape, BF16),
            pltpu.VMEM((3, n_rows, LANES), jnp.int32),
            pltpu.VMEM((n_pairs, 3 * height_a, 2 * (stop_a - start_a)), BF16),
            pltpu.VMEM((n_pairs, 3 * height_b, 2 * (stop_b - start_b)), BF16),
            pltpu.VMEM((n_pairs + 2, own_cols, width), F32),
            pltpu.VMEM((2, n_pairs, width), F32),
            pltpu.VMEM((2, 1, width), F32),
            pltpu.VMEM((2, n_pairs, width), F32),
            pltpu.VMEM((2, 1, width), F32),
            pltpu.VMEM((own_cols, width), F32),
            pltpu.VMEM((2, n_pairs + 1, REACH, LANES), F32),
            pltpu.VMEM((2, n_pairs + 1, REACH, LANES), F32),
            pltpu.VMEM((n_pairs + 1, 1, width), F32),
            pltpu.VMEM((2, 2, n_pairs, LANES), F32),
            pltpu.VMEM((2, 2, 1, LANES), F32),
        ],
        compiler_params=pltpu.CompilerParams(collective_id=0, has_side_effects=True, vmem_limit_bytes=24 * 2**20),
        name="binning",
    )(*[pltpu.with_memory_space_constraint(a, pltpu.HBM) for a in (traces, bin_steps, jnp.asarray(tables))])
    return pl.pallas_call(
        scoped(finish, pltpu.SemaphoreType.DMA((3,))),
        out_shape=jax.ShapeDtypeStruct((n_pairs, own_cols, out_span), F32),
        in_specs=[vmem] * 6,
        out_specs=hbm,
        scratch_shapes=[pltpu.VMEM((2, n_pairs, own_cols, LANES), F32)],
        compiler_params=pltpu.CompilerParams(vmem_limit_bytes=16 * 2**20),
        name="finish",
    )(main, factor, halo, rim, jnp.asarray(t_edge), jnp.asarray(t_rim))


def solution(mesh):
    if mesh.shape["il"] != 2:
        raise ValueError("il size")
    return jax.shard_map(
        functools.partial(shards, mesh.shape["xl"], mesh.shape["ta"]),
        mesh=mesh,
        in_specs=(P("il", "xl", "ta"), P(None, "il", "xl")),
        out_specs=P("il", "xl", "ta"),
        check_vma=False,
    )
```

```python
import functools

import numpy as np
import jax
import jax.numpy as jnp
from jax import lax
from jax.experimental import pallas as pl
from jax.experimental.pallas import tpu as pltpu
from jax.sharding import PartitionSpec as P

TAPS = 16
P_SIZE = 3
Q = 2
REACH = TAPS // 2
LANES = 128
LOADS = 4
MESH = pl.DeviceIdType.MESH
F32, BF16 = jnp.float32, jnp.bfloat16


def lanczos_table(span):
    rows = np.arange(span + 2 * REACH)[:, None] - REACH
    cols = np.arange(span * P_SIZE // Q)[None, :]
    offset = (cols * Q - rows * P_SIZE).astype(np.float64) / P_SIZE
    weights = np.sinc(offset) * np.sinc(offset / REACH)
    return np.where(np.abs(offset) < REACH, weights, 0.0).astype(np.float32)


def split_table(table):
    high = table.astype(BF16)
    low = (table - high.astype(np.float32)).astype(BF16)
    return high, low


def halves(values):
    high = values.astype(BF16)
    low = (values - high.astype(F32)).astype(BF16)
    return high, low


def dot(a, b):
    return jnp.dot(a, b, preferred_element_type=F32)


def column_ranges(n_cols):
    own_cols, rest = n_cols // 2, n_cols - LANES
    if own_cols % 8 or rest % 16 or not LANES < 2 * rest <= 2 * LANES:
        raise ValueError("column count")
    height = (LANES // 2 + 1 + 7) // 8 * 8
    first = (LANES // 2 - 1) // 8 * 8
    return (0, LANES, 0, height), (LANES, n_cols, first, own_cols - first)


def scoped(kernel, *semaphores):
    def run(*refs):
        pl.run_scoped(lambda *scratch: kernel(*refs, *scratch), *semaphores)
    return run


def binning(n_xl, n_ta, traces, steps_hbm, tables_hbm, main, factor, halo_out, rim_out,
            x_left, x_right, edge_x, steps, tables, keys, hot_a, hot_b, acc,
            rim_send, corner_send, rim_recv, corner_recv, il_recv, halo_send, halo_recv, wide_rows,
            diag_recv, diag_corner, load_sem, late_sem, recv_sem):
    n_rows, n_cols, _ = x_left.shape
    span = LANES + x_right.shape[2]
    n_pairs, own_cols = n_rows // 2, n_cols // 2
    il, xl, ta = lax.axis_index("il"), lax.axis_index("xl"), lax.axis_index("ta")
    other = 1 - il
    has_xl, has_ta = (xl < n_xl - 1, xl > 0), (ta < n_ta - 1, ta > 0)
    xl_at, ta_at = (xl + 1, xl - 1), (ta + 1, ta - 1)
    ranges = column_ranges(n_cols)

    def when(condition, work):
        pl.when(condition)(work)

    barrier = pltpu.get_barrier_semaphore()

    def greet(has, partner):
        def signal():
            pl.semaphore_signal(barrier, inc=1, device_id=partner, device_id_type=MESH)
            pl.semaphore_signal(barrier, inc=1, device_id={"il": other, **partner}, device_id_type=MESH)
        when(has, signal)

    greet(has_ta[1], {"ta": ta - 1})
    greet(has_xl[1], {"xl": xl - 1})
    greet(has_xl[0] & has_ta[1], {"xl": xl + 1, "ta": ta - 1})

    step_load = pltpu.make_async_copy(steps_hbm, steps, load_sem.at[3])
    step_load.start()
    edge_loads = [pltpu.make_async_copy(traces.at[:, pl.ds(start, 8)], edge_x.at[d], load_sem.at[4 + d])
                  for d, start in enumerate((n_cols - 8, 0))]
    for load in edge_loads:
        load.start()

    def load_samples(x, start, rows, slot):
        samples = pl.ds(start, x.shape[2])
        return pltpu.make_async_copy(traces.at[rows, :, samples], x.at[rows], load_sem.at[slot])

    table_load = pltpu.make_async_copy(tables_hbm, tables, load_sem.at[2])

    quarter = n_rows // LOADS
    for p in range(LOADS):
        load_samples(x_left, 0, pl.ds(quarter * p, quarter), 0).start()

    greet(has_xl[0] & has_ta[0], {"xl": xl + 1, "ta": ta + 1})
    greet(has_xl[0], {"xl": xl + 1})
    greet(has_ta[0], {"ta": ta + 1})
    pl.semaphore_signal(barrier, inc=1, device_id={"il": other}, device_id_type=MESH)
    count_xl, count_ta = [sum(jnp.where(has, 1, 0) for has in pair) for pair in (has_xl, has_ta)]
    peers = 1 + 2 * (count_xl + count_ta + jnp.where(has_xl[1], count_ta, 0))

    for e in range(2):
        def no_ta(e=e):
            halo_recv[e] = jnp.zeros_like(halo_recv[e])
        when(jnp.logical_not(has_ta[1 - e]), no_ta)
    for d in range(2):
        def no_xl(d=d):
            rim_recv[d] = jnp.zeros_like(rim_recv[d])
            corner_recv[d] = jnp.zeros_like(corner_recv[d])
        when(jnp.logical_not(has_xl[1 - d]), no_xl)
        for e in range(2):
            def no_diag(d=d, e=e):
                diag_recv[d, e] = jnp.zeros_like(diag_recv[d, e])
                diag_corner[d, e] = jnp.zeros_like(diag_corner[d, e])
            when(jnp.logical_not(has_xl[1 - d] & has_ta[1 - e]), no_diag)

    lane = lax.broadcasted_iota(jnp.int32, (1, LANES), 1)
    is_first, is_last = lane < REACH, lane >= LANES - REACH
    step_load.wait()
    col = lax.broadcasted_iota(jnp.int32, (n_rows, n_cols), 1)
    row = lax.broadcasted_iota(jnp.int32, (n_rows, n_cols), 0)
    bin_col = lax.shift_right_logical(col, 1) + steps[1]
    bin_row = steps[0] + 1
    own = (bin_col >= 0) & (bin_col < own_cols)
    code_a, code_b = [jnp.where(own, bin_row * height + bin_col - first, -1)[:, start:stop]
                      for start, stop, first, height in ranges]
    rest = n_cols - LANES
    keys[0] = code_a
    padded = jnp.concatenate([code_b, jnp.full((n_rows, LANES - rest), -1, jnp.int32)], axis=1)
    keys[1] = padded
    keys[2] = pltpu.roll(padded, rest, 1)

    def one_hot(key, height):
        rows = lax.broadcasted_iota(jnp.int32, (height, key.shape[1]), 0)
        return jnp.where(rows == key, 1.0, 0.0).astype(BF16)

    for p in range(n_pairs):
        key = jnp.concatenate([keys[0, 2 * p: 2 * p + 1], keys[0, 2 * p + 1: 2 * p + 2]], axis=1)
        hot_a[p] = one_hot(key, 3 * ranges[0][3])
        second = keys[2, 2 * p + 1: 2 * p + 2]
        key = jnp.concatenate([jnp.where(lane < rest, keys[1, 2 * p: 2 * p + 1], second),
                               second[:, :2 * rest - LANES]], axis=1)
        hot_b[p] = one_hot(key, 3 * ranges[1][3])
    rim_bin = bin_row - 1 + lax.shift_right_logical(row, 1)
    outside = jnp.where(il == 0, n_pairs, -1)
    rim_code = jnp.where(rim_bin == outside, n_pairs, jnp.where((rim_bin < 0) | (rim_bin >= n_pairs), -1, rim_bin))
    for load in edge_loads:
        load.wait()
    for d, (start, column) in enumerate(((n_cols - 8, own_cols), (0, -1))):
        target = jnp.where(bin_col == column, rim_code, -1)
        key = jnp.concatenate([target[i: i + 1, start: start + 8] for i in range(n_rows)], axis=1)
        chosen = one_hot(key, n_pairs + 8)
        high, low = halves(edge_x[d].reshape(n_rows * 8, span))
        sums = dot(chosen, high) + dot(chosen, low)
        folds = dot(chosen, jnp.ones((n_rows * 8, LANES), BF16))
        ends = jnp.where(is_first, sums[:, :LANES], jnp.where(is_last, sums[:, span - LANES:], folds))
        rim_send[d, :, :span] = sums[:n_pairs]
        rim_send[d, :, span:] = ends[:n_pairs]
        corner_send[d, :, :span] = sums[n_pairs: n_pairs + 1]
        corner_send[d, :, span:] = ends[n_pairs: n_pairs + 1]

    hots = (hot_a, hot_b)
    for p in range(LOADS):
        load_samples(x_right, LANES, pl.ds(quarter * p, quarter), 1).start()
    table_load.start()

    def merge(p, r, parts, lanes):
        (_, _, _, height), (_, _, first, _) = ranges
        a, b = parts
        both = a[first:] + b[: height - first]
        for at, part in ((0, a[:first]), (first, both), (height, b[height - first:])):
            where = (p + r, slice(at, at + part.shape[0]), lanes)
            acc[where] = part if p == 0 or r == 2 else acc[where] + part

    def groups(parts, r):
        return [part[r * height: (r + 1) * height] for part, (_, _, _, height) in zip(parts, ranges)]

    def bin_pair(p, x, lanes):
        parts, wide = [], x.shape[2]
        for hot, (start, stop, _, _) in zip(hots, ranges):
            high, low = halves(jnp.concatenate([x[2 * p, start:stop], x[2 * p + 1, start:stop]], axis=0))
            sums = dot(hot[p], jnp.concatenate([high, low], axis=1))
            parts.append(sums[:, :wide] + sums[:, wide:])
        for r in range(3):
            merge(p, r, groups(parts, r), lanes)

    ends = (0, 0), (n_pairs - 1, 2)

    def count_pair(p):
        parts = [dot(hot[p], jnp.ones((hot.shape[2], LANES), BF16)) for hot in hots]
        for r in range(3):
            if (p, r) not in ends:
                merge(p, r, groups(parts, r), slice(span, span + LANES))

    def send_sem(slot):
        return load_sem.at[(6, 7, 3, 8, 0, 1, 9, 4, 5)[slot]]

    def remote(src, dst, slot, partner):
        return pltpu.make_async_remote_copy(src_ref=src, dst_ref=dst, send_sem=send_sem(slot), recv_sem=recv_sem.at[slot],
                                            device_id=partner, device_id_type=MESH)

    rim_row = jnp.where(il == 0, n_pairs + 1, 0)
    own_row = jnp.where(il == 0, n_pairs - 1, 0)
    to_other = remote(acc.at[rim_row], il_recv, 0, {"il": other})

    rims, halos, diags = [], [], {}
    for d in range(2):
        to, rows = {"xl": xl_at[d]}, pl.ds(0, n_pairs)
        rims.append((remote(rim_send.at[d], rim_recv.at[d], 1 + d, to),
                     remote(corner_send.at[d], corner_recv.at[d], 1 + d, {"il": other, **to})))
        to = {"ta": ta_at[d]}
        halos.append((remote(halo_send.at[d, rows], halo_recv.at[d, rows], 3 + d, to),
                      remote(halo_send.at[d, n_pairs], halo_recv.at[d, n_pairs], 3 + d, {"il": other, **to})))
        for e in range(2):
            to, end, slot = {"xl": xl_at[d], "ta": ta_at[e]}, pl.ds(span, LANES), 5 + 2 * d + e
            diags[d, e] = (remote(rim_send.at[d, :, end], diag_recv.at[d, e], slot, to),
                           remote(corner_send.at[d, :, end], diag_corner.at[d, e], slot, {"il": other, **to}))

    def received(slot):
        return recv_sem.at[slot]

    def wait_all(semaphores, slot, rows):
        pltpu.make_async_copy(rows, rows, semaphores(slot)).wait()

    def wait_rims(semaphores, d):
        wait_all(semaphores, 1 + d, wide_rows)

    def wait_halos(semaphores, e):
        wait_all(semaphores, 3 + e, halo_recv.at[e])

    def wait_diags(semaphores, d, e):
        wait_all(semaphores, 5 + 2 * d + e, wide_rows.at[:, :, pl.ds(0, LANES)])

    def start_all(copies):
        for copy in copies:
            copy.start()

    def pack_halo(e):
        lanes = slice(0, LANES) if e else slice(span - LANES, span)
        rows = slice(0, REACH) if e else slice(LANES - REACH, LANES)
        for b in range(n_pairs):
            halo_send[e, b, :, :own_cols] = acc[b + 1, :, lanes].T[rows]
        halo_send[e, n_pairs, :, :own_cols] = acc[rim_row, :, lanes].T[rows]

    def send_diags(d):
        for e in (1, 0):
            when(has_ta[e], lambda e=e: start_all(diags[d, e]))

    def send_rims(d):
        send_diags(d)
        start_all(rims[d])

    def late(e):
        def go():
            pl.semaphore_wait(late_sem.at[e], 1)
            when(has_xl[0], lambda: start_all(diags[0, e]))
        when(has_ta[e], go)

    every_row = pl.ds(0, n_rows)
    def bin_left():
        load_samples(x_left, 0, every_row, 0).wait()
        for p in range(n_pairs):
            bin_pair(p, x_left, slice(0, LANES))
        pack_halo(1)

    first = (xl == 0) & (ta == 0)
    opens_late = first | (xl >= 2)
    when(opens_late, bin_left)
    pl.semaphore_wait(barrier, peers)
    when(has_xl[1], lambda: send_rims(1))
    for e in range(2):
        when(has_ta[e], lambda e=e: pl.semaphore_signal(late_sem.at[1 - e], inc=1, device_id={"ta": ta_at[e]},
                                                        device_id_type=MESH))
    when(has_xl[0], lambda: start_all(rims[0]))
    when(jnp.logical_not(opens_late), bin_left)
    when(has_ta[1], lambda: start_all(halos[1]))
    late(1)
    load_samples(x_right, LANES, every_row, 1).wait()
    for p in range(n_pairs):
        bin_pair(p, x_right, slice(LANES, span))

    when(jnp.logical_not(opens_late), lambda: late(0))
    pack_halo(0)
    when(has_ta[0], lambda: start_all(halos[0]))
    when(xl >= 2, lambda: late(0))
    for p, r in ends:
        chosen = [hot[p, r * height: (r + 1) * height] for hot, (_, _, _, height) in zip(hots, ranges)]
        merge(p, r, [dot(part, jnp.ones((part.shape[1], LANES), BF16)) for part in chosen], slice(span, span + LANES))
    to_other.start()
    for p in range(n_pairs):
        count_pair(p)
    when(first, lambda: late(0))

    def resample(values):
        high, low = halves(values)
        return dot(high, tables[0]) + (dot(low, tables[0]) + dot(high, tables[1]))

    table_load.wait()
    for i in range(n_pairs):
        b = jnp.where(il == 0, i, n_pairs - 1 - i)
        if i == n_pairs - 1:
            to_other.wait_recv()
            acc[b + 1] = acc[b + 1] + il_recv[...]
        main[b] = resample(acc[b + 1, :, :span])
    for d in range(2):
        when(has_xl[1 - d], lambda d=d: wait_rims(received, d))
    sub = lax.broadcasted_iota(jnp.int32, (n_pairs, 1), 0)
    rim = jnp.concatenate([rim_recv[d] + jnp.where(sub == own_row, corner_recv[d], 0.0) for d in range(2)], axis=0)
    more = resample(rim[:, :span])
    more_fold = jnp.broadcast_to(rim[:, span + LANES // 2: span + LANES // 2 + 1], (2 * n_pairs, LANES))
    ends_row = lax.broadcasted_iota(jnp.int32, (8, 1), 0)
    tops = ((0, 0, 0), (own_cols - 8, 7, n_pairs))

    def add_rows(values, extra, b):
        top, bottom = [values[at: at + 8] + jnp.where(ends_row == where, extra[base + b: base + b + 1], 0.0)
                       for at, where, base in tops]
        return jnp.concatenate([top, values[8: own_cols - 8], bottom], axis=0)

    for b in range(n_pairs):
        scale = 1.0 / jnp.maximum(add_rows(acc[b + 1, :, span:], more_fold, b), 1.0)
        factor[b] = scale
        main[b] = add_rows(main[b], more, b) * jnp.concatenate([scale] * (main.shape[2] // LANES), axis=1)

    to_other.wait_send()
    for d in range(2):
        when(has_xl[d], lambda d=d: wait_rims(send_sem, d))
        when(has_ta[d], lambda d=d: wait_halos(send_sem, d))
        for e in range(2):
            when(has_xl[d] & has_ta[e], lambda d=d, e=e: wait_diags(send_sem, d, e))

    for d in range(2):
        for e in range(2):
            when(has_xl[1 - d] & has_ta[1 - e], lambda d=d, e=e: wait_diags(received, d, e))
    for d in range(2):
        first, last = [diag_recv[d, e] + jnp.where(sub == own_row, diag_corner[d, e], 0.0) for e in (1, 0)]
        rim_out[d * n_pairs: (d + 1) * n_pairs] = jnp.where(is_first, first, jnp.where(is_last, last, 0.0))
    for e in range(2):
        when(has_ta[1 - e], lambda e=e: wait_halos(received, e))
        halo_out[e] = halo_recv[e, :n_pairs]
        halo_out[e, own_row] = halo_recv[e, own_row] + halo_recv[e, n_pairs]


def finish(main, factor, halo, rim, t_edge, t_rim, out, staged, out_sem):
    n_pairs, own_cols, width = main.shape
    starts = (0, width - LANES)
    has_before = lax.axis_index("ta") > 0

    def write_tiles(source, start, size, slot):
        return pltpu.make_async_copy(source, out.at[:, :, pl.ds(start, size)], out_sem.at[slot])

    def from_main(start, size, slot):
        return write_tiles(main.at[:, :, pl.ds(start, size)], start, size, slot)

    from_main(LANES, width - 2 * LANES, 2).start()
    pl.when(jnp.logical_not(has_before))(from_main(0, LANES, 0).start)
    ends_row = lax.broadcasted_iota(jnp.int32, (8, 1), 0)
    tops = ((0, 0, 0), (own_cols - 8, 7, n_pairs))

    def add_halo(tiles, table):
        high = rim[...].astype(BF16)
        low = (rim[...] - high.astype(F32)).astype(BF16)
        more = dot(jnp.concatenate([high, low, high], axis=1), t_rim[...])
        for pair in zip(tiles[::2], tiles[1::2]):
            terms = []
            for d, b in pair:
                high = halo[d, b].astype(BF16).astype(F32)
                terms += [high, halo[d, b] - high, high]
            both = dot(jnp.concatenate(terms, axis=0).T[:own_cols].astype(BF16), t_edge[table])
            for i, (d, b) in enumerate(pair):
                ends, lanes = both[:, i * LANES: (i + 1) * LANES], slice(d * LANES, (d + 1) * LANES)
                top, bottom = [ends[at: at + 8] + jnp.where(ends_row == where, more[base + b: base + b + 1, lanes], 0.0)
                               for at, where, base in tops]
                ends = jnp.concatenate([top, ends[8: own_cols - 8], bottom], axis=0)
                staged[d, b] = main[b, :, starts[d]: starts[d] + LANES] + ends * factor[b]
                pltpu.make_async_copy(staged.at[d, b], out.at[b, :, pl.ds(starts[d], LANES)], out_sem.at[d]).start()

    rows = range(n_pairs)
    pl.when(has_before)(lambda: add_halo([(d, b) for b in rows for d in range(2)], 0))
    pl.when(jnp.logical_not(has_before))(lambda: add_halo([(1, b) for b in rows], 1))
    from_main(LANES, width - 2 * LANES, 2).wait()
    for d in range(2):
        write_tiles(staged.at[d], starts[d], LANES, d).wait()


def shards(n_xl, n_ta, traces, bin_steps):
    n_rows, n_cols, span = traces.shape
    n_pairs, own_cols = n_rows // 2, n_cols // 2
    width = span + LANES
    out_span = span * P_SIZE // Q
    if n_pairs % 8 or span % LANES or out_span % LANES or out_span < 3 * LANES:
        raise ValueError("block shape")
    table = lanczos_table(span)
    tables = np.stack(split_table(table[REACH:-REACH]))
    edge_cols = np.concatenate([table[:, :LANES], table[:, -LANES:]], axis=1)
    edge_high, edge_low = split_table(np.stack([edge_cols[:REACH, :LANES], edge_cols[-REACH:, LANES:]]))
    before, after = np.concatenate([edge_high, edge_high, edge_low], axis=1)
    none = np.zeros_like(before)
    t_edge = np.stack([np.block([[first, none], [none, after]]) for first in (before, after)])
    rim_high, rim_low = split_table(np.concatenate(
        [edge_cols[-REACH:], np.zeros((LANES - 2 * REACH, 2 * LANES), np.float32), edge_cols[:REACH]]))
    t_rim = np.concatenate([rim_high, rim_high, rim_low])
    vmem = pl.BlockSpec(memory_space=pltpu.VMEM)
    hbm = pl.BlockSpec(memory_space=pltpu.HBM)
    (start_a, stop_a, _, height_a), (start_b, stop_b, _, height_b) = column_ranges(n_cols)
    main, factor, halo, rim = pl.pallas_call(
        scoped(functools.partial(binning, n_xl, n_ta), pltpu.SemaphoreType.DMA((10,)), pltpu.SemaphoreType.REGULAR((2,)),
               pltpu.SemaphoreType.DMA((9,))),
        out_shape=(pltpu.VMEM((n_pairs, own_cols, out_span), F32), pltpu.VMEM((n_pairs, own_cols, LANES), F32),
                   pltpu.VMEM((2, n_pairs, REACH, LANES), F32), pltpu.VMEM((2 * n_pairs, LANES), F32)),
        in_specs=[hbm] * 3,
        out_specs=[vmem] * 4,
        scratch_shapes=[
            pltpu.VMEM((n_rows, n_cols, LANES), F32),
            pltpu.VMEM((n_rows, n_cols, span - LANES), F32),
            pltpu.VMEM((2, n_rows, 8, span), F32),
            pltpu.VMEM((2, n_rows, n_cols), jnp.int32),
            pltpu.VMEM(tables.shape, BF16),
            pltpu.VMEM((3, n_rows, LANES), jnp.int32),
            pltpu.VMEM((n_pairs, 3 * height_a, 2 * (stop_a - start_a)), BF16),
            pltpu.VMEM((n_pairs, 3 * height_b, 2 * (stop_b - start_b)), BF16),
            pltpu.VMEM((n_pairs + 2, own_cols, width), F32),
            pltpu.VMEM((2, n_pairs, width), F32),
            pltpu.VMEM((2, 1, width), F32),
            pltpu.VMEM((2, n_pairs, width), F32),
            pltpu.VMEM((2, 1, width), F32),
            pltpu.VMEM((own_cols, width), F32),
            pltpu.VMEM((2, n_pairs + 1, REACH, LANES), F32),
            pltpu.VMEM((2, n_pairs + 1, REACH, LANES), F32),
            pltpu.VMEM((n_pairs + 1, 1, width), F32),
            pltpu.VMEM((2, 2, n_pairs, LANES), F32),
            pltpu.VMEM((2, 2, 1, LANES), F32),
        ],
        compiler_params=pltpu.CompilerParams(collective_id=0, has_side_effects=True, vmem_limit_bytes=24 * 2**20),
        name="binning",
    )(*[pltpu.with_memory_space_constraint(a, pltpu.HBM) for a in (traces, bin_steps, jnp.asarray(tables))])
    return pl.pallas_call(
        scoped(finish, pltpu.SemaphoreType.DMA((3,))),
        out_shape=jax.ShapeDtypeStruct((n_pairs, own_cols, out_span), F32),
        in_specs=[vmem] * 6,
        out_specs=hbm,
        scratch_shapes=[pltpu.VMEM((2, n_pairs, own_cols, LANES), F32)],
        compiler_params=pltpu.CompilerParams(vmem_limit_bytes=16 * 2**20),
        name="finish",
    )(main, factor, halo, rim, jnp.asarray(t_edge), jnp.asarray(t_rim))


def solution(mesh):
    if mesh.shape["il"] != 2:
        raise ValueError("il size")
    return jax.shard_map(
        functools.partial(shards, mesh.shape["xl"], mesh.shape["ta"]),
        mesh=mesh,
        in_specs=(P("il", "xl", "ta"), P(None, "il", "xl")),
        out_specs=P("il", "xl", "ta"),
        check_vma=False,
    )
```

```python
import functools

import numpy as np
import jax
import jax.numpy as jnp
from jax import lax
from jax.experimental import pallas as pl
from jax.experimental.pallas import tpu as pltpu
from jax.sharding import PartitionSpec as P

TAPS = 16
P_SIZE = 3
Q = 2
REACH = TAPS // 2
LANES = 128
LOADS = 4
MESH = pl.DeviceIdType.MESH
F32, BF16 = jnp.float32, jnp.bfloat16


def lanczos_table(span):
    rows = np.arange(span + 2 * REACH)[:, None] - REACH
    cols = np.arange(span * P_SIZE // Q)[None, :]
    offset = (cols * Q - rows * P_SIZE).astype(np.float64) / P_SIZE
    weights = np.sinc(offset) * np.sinc(offset / REACH)
    return np.where(np.abs(offset) < REACH, weights, 0.0).astype(np.float32)


def split_table(table):
    high = table.astype(BF16)
    low = (table - high.astype(np.float32)).astype(BF16)
    return high, low


def halves(values):
    high = values.astype(BF16)
    low = (values - high.astype(F32)).astype(BF16)
    return high, low


def dot(a, b):
    return jnp.dot(a, b, preferred_element_type=F32)


def column_ranges(n_cols):
    own_cols, rest = n_cols // 2, n_cols - LANES
    if own_cols % 8 or rest % 16 or not LANES < 2 * rest <= 2 * LANES:
        raise ValueError("column count")
    height = (LANES // 2 + 1 + 7) // 8 * 8
    first = (LANES // 2 - 1) // 8 * 8
    return (0, LANES, 0, height), (LANES, n_cols, first, own_cols - first)


def scoped(kernel, *semaphores):
    def run(*refs):
        pl.run_scoped(lambda *scratch: kernel(*refs, *scratch), *semaphores)
    return run


def binning(n_xl, n_ta, traces, steps_hbm, tables_hbm, main, factor, halo_out, rim_out,
            x_left, x_right, edge_x, steps, tables, keys, hot_a, hot_b, acc,
            rim_send, corner_send, rim_recv, corner_recv, il_recv, halo_send, halo_recv, wide_rows,
            diag_recv, diag_corner, load_sem, late_sem, recv_sem):
    n_rows, n_cols, _ = x_left.shape
    span = LANES + x_right.shape[2]
    n_pairs, own_cols = n_rows // 2, n_cols // 2
    il, xl, ta = lax.axis_index("il"), lax.axis_index("xl"), lax.axis_index("ta")
    other = 1 - il
    has_xl, has_ta = (xl < n_xl - 1, xl > 0), (ta < n_ta - 1, ta > 0)
    xl_at, ta_at = (xl + 1, xl - 1), (ta + 1, ta - 1)
    ranges = column_ranges(n_cols)

    def when(condition, work):
        pl.when(condition)(work)

    barrier = pltpu.get_barrier_semaphore()

    def greet(has, partner):
        def signal():
            pl.semaphore_signal(barrier, inc=1, device_id=partner, device_id_type=MESH)
            pl.semaphore_signal(barrier, inc=1, device_id={"il": other, **partner}, device_id_type=MESH)
        when(has, signal)

    greet(has_ta[1], {"ta": ta - 1})
    greet(has_xl[1], {"xl": xl - 1})
    greet(has_xl[0] & has_ta[1], {"xl": xl + 1, "ta": ta - 1})

    step_load = pltpu.make_async_copy(steps_hbm, steps, load_sem.at[3])
    step_load.start()
    edge_loads = [pltpu.make_async_copy(traces.at[:, pl.ds(start, 8)], edge_x.at[d], load_sem.at[4 + d])
                  for d, start in enumerate((n_cols - 8, 0))]
    for load in edge_loads:
        load.start()

    def load_samples(x, start, rows, slot):
        samples = pl.ds(start, x.shape[2])
        return pltpu.make_async_copy(traces.at[rows, :, samples], x.at[rows], load_sem.at[slot])

    table_load = pltpu.make_async_copy(tables_hbm, tables, load_sem.at[2])

    quarter = n_rows // LOADS
    for p in range(LOADS):
        load_samples(x_left, 0, pl.ds(quarter * p, quarter), 0).start()

    greet(has_xl[0] & has_ta[0], {"xl": xl + 1, "ta": ta + 1})
    greet(has_xl[0], {"xl": xl + 1})
    greet(has_ta[0], {"ta": ta + 1})
    pl.semaphore_signal(barrier, inc=1, device_id={"il": other}, device_id_type=MESH)
    count_xl, count_ta = [sum(jnp.where(has, 1, 0) for has in pair) for pair in (has_xl, has_ta)]
    peers = 1 + 2 * (count_xl + count_ta + jnp.where(has_xl[1], count_ta, 0))

    for e in range(2):
        def no_ta(e=e):
            halo_recv[e] = jnp.zeros_like(halo_recv[e])
        when(jnp.logical_not(has_ta[1 - e]), no_ta)
    for d in range(2):
        def no_xl(d=d):
            rim_recv[d] = jnp.zeros_like(rim_recv[d])
            corner_recv[d] = jnp.zeros_like(corner_recv[d])
        when(jnp.logical_not(has_xl[1 - d]), no_xl)
        for e in range(2):
            def no_diag(d=d, e=e):
                diag_recv[d, e] = jnp.zeros_like(diag_recv[d, e])
                diag_corner[d, e] = jnp.zeros_like(diag_corner[d, e])
            when(jnp.logical_not(has_xl[1 - d] & has_ta[1 - e]), no_diag)

    lane = lax.broadcasted_iota(jnp.int32, (1, LANES), 1)
    is_first, is_last = lane < REACH, lane >= LANES - REACH
    step_load.wait()
    col = lax.broadcasted_iota(jnp.int32, (n_rows, n_cols), 1)
    row = lax.broadcasted_iota(jnp.int32, (n_rows, n_cols), 0)
    bin_col = lax.shift_right_logical(col, 1) + steps[1]
    bin_row = steps[0] + 1
    own = (bin_col >= 0) & (bin_col < own_cols)
    code_a, code_b = [jnp.where(own, bin_row * height + bin_col - first, -1)[:, start:stop]
                      for start, stop, first, height in ranges]
    rest = n_cols - LANES
    keys[0] = code_a
    padded = jnp.concatenate([code_b, jnp.full((n_rows, LANES - rest), -1, jnp.int32)], axis=1)
    keys[1] = padded
    keys[2] = pltpu.roll(padded, rest, 1)

    def one_hot(key, height):
        rows = lax.broadcasted_iota(jnp.int32, (height, key.shape[1]), 0)
        return jnp.where(rows == key, 1.0, 0.0).astype(BF16)

    for p in range(n_pairs):
        key = jnp.concatenate([keys[0, 2 * p: 2 * p + 1], keys[0, 2 * p + 1: 2 * p + 2]], axis=1)
        hot_a[p] = one_hot(key, 3 * ranges[0][3])
        second = keys[2, 2 * p + 1: 2 * p + 2]
        key = jnp.concatenate([jnp.where(lane < rest, keys[1, 2 * p: 2 * p + 1], second),
                               second[:, :2 * rest - LANES]], axis=1)
        hot_b[p] = one_hot(key, 3 * ranges[1][3])
    rim_bin = bin_row - 1 + lax.shift_right_logical(row, 1)
    outside = jnp.where(il == 0, n_pairs, -1)
    rim_code = jnp.where(rim_bin == outside, n_pairs, jnp.where((rim_bin < 0) | (rim_bin >= n_pairs), -1, rim_bin))
    for load in edge_loads:
        load.wait()
    for d, (start, column) in enumerate(((n_cols - 8, own_cols), (0, -1))):
        target = jnp.where(bin_col == column, rim_code, -1)
        key = jnp.concatenate([target[i: i + 1, start: start + 8] for i in range(n_rows)], axis=1)
        chosen = one_hot(key, n_pairs + 8)
        high, low = halves(edge_x[d].reshape(n_rows * 8, span))
        sums = dot(chosen, high) + dot(chosen, low)
        folds = dot(chosen, jnp.ones((n_rows * 8, LANES), BF16))
        ends = jnp.where(is_first, sums[:, :LANES], jnp.where(is_last, sums[:, span - LANES:], folds))
        rim_send[d, :, :span] = sums[:n_pairs]
        rim_send[d, :, span:] = ends[:n_pairs]
        corner_send[d, :, :span] = sums[n_pairs: n_pairs + 1]
        corner_send[d, :, span:] = ends[n_pairs: n_pairs + 1]

    hots = (hot_a, hot_b)
    for p in range(LOADS):
        load_samples(x_right, LANES, pl.ds(quarter * p, quarter), 1).start()
    table_load.start()

    def merge(p, r, parts, lanes):
        (_, _, _, height), (_, _, first, _) = ranges
        a, b = parts
        both = a[first:] + b[: height - first]
        for at, part in ((0, a[:first]), (first, both), (height, b[height - first:])):
            where = (p + r, slice(at, at + part.shape[0]), lanes)
            acc[where] = part if p == 0 or r == 2 else acc[where] + part

    def groups(parts, r):
        return [part[r * height: (r + 1) * height] for part, (_, _, _, height) in zip(parts, ranges)]

    def bin_pair(p, x, lanes):
        parts, wide = [], x.shape[2]
        for hot, (start, stop, _, _) in zip(hots, ranges):
            high, low = halves(jnp.concatenate([x[2 * p, start:stop], x[2 * p + 1, start:stop]], axis=0))
            sums = dot(hot[p], jnp.concatenate([high, low], axis=1))
            parts.append(sums[:, :wide] + sums[:, wide:])
        for r in range(3):
            merge(p, r, groups(parts, r), lanes)

    ends = (0, 0), (n_pairs - 1, 2)

    def count_pair(p):
        parts = [dot(hot[p], jnp.ones((hot.shape[2], LANES), BF16)) for hot in hots]
        for r in range(3):
            if (p, r) not in ends:
                merge(p, r, groups(parts, r), slice(span, span + LANES))

    def send_sem(slot):
        return load_sem.at[(6, 7, 3, 8, 0, 1, 9, 4, 5)[slot]]

    def remote(src, dst, slot, partner):
        return pltpu.make_async_remote_copy(src_ref=src, dst_ref=dst, send_sem=send_sem(slot), recv_sem=recv_sem.at[slot],
                                            device_id=partner, device_id_type=MESH)

    rim_row = jnp.where(il == 0, n_pairs + 1, 0)
    own_row = jnp.where(il == 0, n_pairs - 1, 0)
    to_other = remote(acc.at[rim_row], il_recv, 0, {"il": other})

    rims, halos, diags = [], [], {}
    for d in range(2):
        to, rows = {"xl": xl_at[d]}, pl.ds(0, n_pairs)
        rims.append((remote(rim_send.at[d], rim_recv.at[d], 1 + d, to),
                     remote(corner_send.at[d], corner_recv.at[d], 1 + d, {"il": other, **to})))
        to = {"ta": ta_at[d]}
        halos.append((remote(halo_send.at[d, rows], halo_recv.at[d, rows], 3 + d, to),
                      remote(halo_send.at[d, n_pairs], halo_recv.at[d, n_pairs], 3 + d, {"il": other, **to})))
        for e in range(2):
            to, end, slot = {"xl": xl_at[d], "ta": ta_at[e]}, pl.ds(span, LANES), 5 + 2 * d + e
            diags[d, e] = (remote(rim_send.at[d, :, end], diag_recv.at[d, e], slot, to),
                           remote(corner_send.at[d, :, end], diag_corner.at[d, e], slot, {"il": other, **to}))

    def received(slot):
        return recv_sem.at[slot]

    def wait_all(semaphores, slot, rows):
        pltpu.make_async_copy(rows, rows, semaphores(slot)).wait()

    def wait_rims(semaphores, d):
        wait_all(semaphores, 1 + d, wide_rows)

    def wait_halos(semaphores, e):
        wait_all(semaphores, 3 + e, halo_recv.at[e])

    def wait_diags(semaphores, d, e):
        wait_all(semaphores, 5 + 2 * d + e, wide_rows.at[:, :, pl.ds(0, LANES)])

    def start_all(copies):
        for copy in copies:
            copy.start()

    def pack_halo(e):
        lanes = slice(0, LANES) if e else slice(span - LANES, span)
        rows = slice(0, REACH) if e else slice(LANES - REACH, LANES)
        for b in range(n_pairs):
            halo_send[e, b, :, :own_cols] = acc[b + 1, :, lanes].T[rows]
        halo_send[e, n_pairs, :, :own_cols] = acc[rim_row, :, lanes].T[rows]

    def send_diags(d):
        for e in (1, 0):
            when(has_ta[e], lambda e=e: start_all(diags[d, e]))

    def send_rims(d):
        send_diags(d)
        start_all(rims[d])

    def late(e):
        def go():
            pl.semaphore_wait(late_sem.at[e], 1)
            when(has_xl[0], lambda: start_all(diags[0, e]))
        when(has_ta[e], go)

    every_row = pl.ds(0, n_rows)
    def bin_left():
        load_samples(x_left, 0, every_row, 0).wait()
        for p in range(n_pairs):
            bin_pair(p, x_left, slice(0, LANES))
        pack_halo(1)

    first = (xl == 0) & (ta == 0)
    opens_late = first | (xl >= 2)
    when(opens_late, bin_left)
    pl.semaphore_wait(barrier, peers)
    when(has_xl[1], lambda: send_rims(1))
    for e in range(2):
        when(has_ta[e], lambda e=e: pl.semaphore_signal(late_sem.at[1 - e], inc=1, device_id={"ta": ta_at[e]},
                                                        device_id_type=MESH))
    when(has_xl[0], lambda: start_all(rims[0]))
    when(jnp.logical_not(opens_late), bin_left)
    when(has_ta[1], lambda: start_all(halos[1]))
    late(1)
    load_samples(x_right, LANES, every_row, 1).wait()
    for p in range(n_pairs):
        bin_pair(p, x_right, slice(LANES, span))

    when(jnp.logical_not(opens_late), lambda: late(0))
    pack_halo(0)
    when(has_ta[0], lambda: start_all(halos[0]))
    when(xl >= 2, lambda: late(0))
    for p, r in ends:
        chosen = [hot[p, r * height: (r + 1) * height] for hot, (_, _, _, height) in zip(hots, ranges)]
        merge(p, r, [dot(part, jnp.ones((part.shape[1], LANES), BF16)) for part in chosen], slice(span, span + LANES))
    to_other.start()
    for p in range(n_pairs):
        count_pair(p)
    when(first, lambda: late(0))

    def resample(values):
        high, low = halves(values)
        return dot(high, tables[0]) + (dot(low, tables[0]) + dot(high, tables[1]))

    table_load.wait()
    for i in range(n_pairs):
        b = jnp.where(il == 0, i, n_pairs - 1 - i)
        if i == n_pairs - 1:
            to_other.wait_recv()
            acc[b + 1] = acc[b + 1] + il_recv[...]
        main[b] = resample(acc[b + 1, :, :span])
    for d in range(2):
        when(has_xl[1 - d], lambda d=d: wait_rims(received, d))
    sub = lax.broadcasted_iota(jnp.int32, (n_pairs, 1), 0)
    rim = jnp.concatenate([rim_recv[d] + jnp.where(sub == own_row, corner_recv[d], 0.0) for d in range(2)], axis=0)
    more = resample(rim[:, :span])
    more_fold = jnp.broadcast_to(rim[:, span + LANES // 2: span + LANES // 2 + 1], (2 * n_pairs, LANES))
    ends_row = lax.broadcasted_iota(jnp.int32, (8, 1), 0)
    tops = ((0, 0, 0), (own_cols - 8, 7, n_pairs))

    def add_rows(values, extra, b):
        top, bottom = [values[at: at + 8] + jnp.where(ends_row == where, extra[base + b: base + b + 1], 0.0)
                       for at, where, base in tops]
        return jnp.concatenate([top, values[8: own_cols - 8], bottom], axis=0)

    for b in range(n_pairs):
        scale = 1.0 / jnp.maximum(add_rows(acc[b + 1, :, span:], more_fold, b), 1.0)
        factor[b] = scale
        main[b] = add_rows(main[b], more, b) * jnp.concatenate([scale] * (main.shape[2] // LANES), axis=1)

    to_other.wait_send()
    for d in range(2):
        when(has_xl[d], lambda d=d: wait_rims(send_sem, d))
        when(has_ta[d], lambda d=d: wait_halos(send_sem, d))
        for e in range(2):
            when(has_xl[d] & has_ta[e], lambda d=d, e=e: wait_diags(send_sem, d, e))

    for d in range(2):
        for e in range(2):
            when(has_xl[1 - d] & has_ta[1 - e], lambda d=d, e=e: wait_diags(received, d, e))
    for d in range(2):
        first, last = [diag_recv[d, e] + jnp.where(sub == own_row, diag_corner[d, e], 0.0) for e in (1, 0)]
        rim_out[d * n_pairs: (d + 1) * n_pairs] = jnp.where(is_first, first, jnp.where(is_last, last, 0.0))
    for e in range(2):
        when(has_ta[1 - e], lambda e=e: wait_halos(received, e))
        halo_out[e] = halo_recv[e, :n_pairs]
        halo_out[e, own_row] = halo_recv[e, own_row] + halo_recv[e, n_pairs]


def finish(main, factor, halo, rim, tables, out, staged, out_sem):
    n_pairs, own_cols, width = main.shape
    starts = (0, width - LANES)
    has_before = lax.axis_index("ta") > 0

    def write_tiles(source, start, size, slot):
        return pltpu.make_async_copy(source, out.at[:, :, pl.ds(start, size)], out_sem.at[slot])

    def from_main(start, size, slot):
        return write_tiles(main.at[:, :, pl.ds(start, size)], start, size, slot)

    from_main(LANES, width - 2 * LANES, 2).start()
    pl.when(jnp.logical_not(has_before))(from_main(0, LANES, 0).start)
    ends_row = lax.broadcasted_iota(jnp.int32, (8, 1), 0)
    tops = ((0, 0, 0), (own_cols - 8, 7, n_pairs))

    def add_halo(tiles, table):
        high = rim[...].astype(BF16)
        low = (rim[...] - high.astype(F32)).astype(BF16)
        more = dot(jnp.concatenate([high, low, high], axis=1), tables[12 * REACH:])
        for pair in zip(tiles[::2], tiles[1::2]):
            terms = []
            for d, b in pair:
                high = halo[d, b].astype(BF16).astype(F32)
                terms += [high, halo[d, b] - high, high]
            both = dot(jnp.concatenate(terms, axis=0).T[:own_cols].astype(BF16), tables[table * 6 * REACH: (table + 1) * 6 * REACH])
            for i, (d, b) in enumerate(pair):
                ends, lanes = both[:, i * LANES: (i + 1) * LANES], slice(d * LANES, (d + 1) * LANES)
                top, bottom = [ends[at: at + 8] + jnp.where(ends_row == where, more[base + b: base + b + 1, lanes], 0.0)
                               for at, where, base in tops]
                ends = jnp.concatenate([top, ends[8: own_cols - 8], bottom], axis=0)
                staged[d, b] = main[b, :, starts[d]: starts[d] + LANES] + ends * factor[b]
                pltpu.make_async_copy(staged.at[d, b], out.at[b, :, pl.ds(starts[d], LANES)], out_sem.at[d]).start()

    rows = range(n_pairs)
    pl.when(has_before)(lambda: add_halo([(d, b) for b in rows for d in range(2)], 0))
    pl.when(jnp.logical_not(has_before))(lambda: add_halo([(1, b) for b in rows], 1))
    from_main(LANES, width - 2 * LANES, 2).wait()
    for d in range(2):
        write_tiles(staged.at[d], starts[d], LANES, d).wait()


def shards(n_xl, n_ta, traces, bin_steps):
    n_rows, n_cols, span = traces.shape
    n_pairs, own_cols = n_rows // 2, n_cols // 2
    width = span + LANES
    out_span = span * P_SIZE // Q
    if n_pairs % 8 or span % LANES or out_span % LANES or out_span < 3 * LANES:
        raise ValueError("block shape")
    table = lanczos_table(span)
    tables = np.stack(split_table(table[REACH:-REACH]))
    edge_cols = np.concatenate([table[:, :LANES], table[:, -LANES:]], axis=1)
    edge_high, edge_low = split_table(np.stack([edge_cols[:REACH, :LANES], edge_cols[-REACH:, LANES:]]))
    before, after = np.concatenate([edge_high, edge_high, edge_low], axis=1)
    none = np.zeros_like(before)
    t_edge = np.stack([np.block([[first, none], [none, after]]) for first in (before, after)])
    rim_high, rim_low = split_table(np.concatenate(
        [edge_cols[-REACH:], np.zeros((LANES - 2 * REACH, 2 * LANES), np.float32), edge_cols[:REACH]]))
    t_rim = np.concatenate([rim_high, rim_high, rim_low])
    vmem = pl.BlockSpec(memory_space=pltpu.VMEM)
    hbm = pl.BlockSpec(memory_space=pltpu.HBM)
    (start_a, stop_a, _, height_a), (start_b, stop_b, _, height_b) = column_ranges(n_cols)
    main, factor, halo, rim = pl.pallas_call(
        scoped(functools.partial(binning, n_xl, n_ta), pltpu.SemaphoreType.DMA((10,)), pltpu.SemaphoreType.REGULAR((2,)),
               pltpu.SemaphoreType.DMA((9,))),
        out_shape=(pltpu.VMEM((n_pairs, own_cols, out_span), F32), pltpu.VMEM((n_pairs, own_cols, LANES), F32),
                   pltpu.VMEM((2, n_pairs, REACH, LANES), F32), pltpu.VMEM((2 * n_pairs, LANES), F32)),
        in_specs=[hbm] * 3,
        out_specs=[vmem] * 4,
        scratch_shapes=[
            pltpu.VMEM((n_rows, n_cols, LANES), F32),
            pltpu.VMEM((n_rows, n_cols, span - LANES), F32),
            pltpu.VMEM((2, n_rows, 8, span), F32),
            pltpu.VMEM((2, n_rows, n_cols), jnp.int32),
            pltpu.VMEM(tables.shape, BF16),
            pltpu.VMEM((3, n_rows, LANES), jnp.int32),
            pltpu.VMEM((n_pairs, 3 * height_a, 2 * (stop_a - start_a)), BF16),
            pltpu.VMEM((n_pairs, 3 * height_b, 2 * (stop_b - start_b)), BF16),
            pltpu.VMEM((n_pairs + 2, own_cols, width), F32),
            pltpu.VMEM((2, n_pairs, width), F32),
            pltpu.VMEM((2, 1, width), F32),
            pltpu.VMEM((2, n_pairs, width), F32),
            pltpu.VMEM((2, 1, width), F32),
            pltpu.VMEM((own_cols, width), F32),
            pltpu.VMEM((2, n_pairs + 1, REACH, LANES), F32),
            pltpu.VMEM((2, n_pairs + 1, REACH, LANES), F32),
            pltpu.VMEM((n_pairs + 1, 1, width), F32),
            pltpu.VMEM((2, 2, n_pairs, LANES), F32),
            pltpu.VMEM((2, 2, 1, LANES), F32),
        ],
        compiler_params=pltpu.CompilerParams(collective_id=0, has_side_effects=True, vmem_limit_bytes=24 * 2**20),
        name="binning",
    )(*[pltpu.with_memory_space_constraint(a, pltpu.HBM) for a in (traces, bin_steps, jnp.asarray(tables))])
    return pl.pallas_call(
        scoped(finish, pltpu.SemaphoreType.DMA((3,))),
        out_shape=jax.ShapeDtypeStruct((n_pairs, own_cols, out_span), F32),
        in_specs=[vmem] * 5,
        out_specs=hbm,
        scratch_shapes=[pltpu.VMEM((2, n_pairs, own_cols, LANES), F32)],
        compiler_params=pltpu.CompilerParams(vmem_limit_bytes=16 * 2**20),
        name="finish",
    )(main, factor, halo, rim, jnp.asarray(np.concatenate([*t_edge, t_rim])))


def solution(mesh):
    if mesh.shape["il"] != 2:
        raise ValueError("il size")
    return jax.shard_map(
        functools.partial(shards, mesh.shape["xl"], mesh.shape["ta"]),
        mesh=mesh,
        in_specs=(P("il", "xl", "ta"), P(None, "il", "xl")),
        out_specs=P("il", "xl", "ta"),
        check_vma=False,
    )
```

```python
import functools

import numpy as np
import jax
import jax.numpy as jnp
from jax import lax
from jax.experimental import pallas as pl
from jax.experimental.pallas import tpu as pltpu
from jax.sharding import PartitionSpec as P

TAPS = 16
P_SIZE = 3
Q = 2
REACH = TAPS // 2
LANES = 128
LOADS = 4
MESH = pl.DeviceIdType.MESH
F32, BF16 = jnp.float32, jnp.bfloat16


def lanczos_table(span):
    rows = np.arange(span + 2 * REACH)[:, None] - REACH
    cols = np.arange(span * P_SIZE // Q)[None, :]
    offset = (cols * Q - rows * P_SIZE).astype(np.float64) / P_SIZE
    weights = np.sinc(offset) * np.sinc(offset / REACH)
    return np.where(np.abs(offset) < REACH, weights, 0.0).astype(np.float32)


def split_table(table):
    high = table.astype(BF16)
    low = (table - high.astype(np.float32)).astype(BF16)
    return high, low


def halves(values):
    high = values.astype(BF16)
    low = (values - high.astype(F32)).astype(BF16)
    return high, low


def dot(a, b):
    return jnp.dot(a, b, preferred_element_type=F32)


def column_ranges(n_cols):
    own_cols, rest = n_cols // 2, n_cols - LANES
    if own_cols % 8 or rest % 16 or not LANES < 2 * rest <= 2 * LANES:
        raise ValueError("column count")
    height = (LANES // 2 + 1 + 7) // 8 * 8
    first = (LANES // 2 - 1) // 8 * 8
    return (0, LANES, 0, height), (LANES, n_cols, first, own_cols - first)


def scoped(kernel, *semaphores):
    def run(*refs):
        pl.run_scoped(lambda *scratch: kernel(*refs, *scratch), *semaphores)
    return run


def binning(n_xl, n_ta, traces, steps_hbm, tables_hbm, main, factor, halo_out, rim_out,
            x_left, x_right, edge_x, steps, tables, keys, hot_a, hot_b, acc,
            rim_send, corner_send, rim_recv, corner_recv, il_recv, halo_send, halo_recv, wide_rows,
            diag_recv, diag_corner, load_sem, late_sem, recv_sem):
    n_rows, n_cols, _ = x_left.shape
    span = LANES + x_right.shape[2]
    n_pairs, own_cols = n_rows // 2, n_cols // 2
    il, xl, ta = lax.axis_index("il"), lax.axis_index("xl"), lax.axis_index("ta")
    other = 1 - il
    has_xl, has_ta = (xl < n_xl - 1, xl > 0), (ta < n_ta - 1, ta > 0)
    xl_at, ta_at = (xl + 1, xl - 1), (ta + 1, ta - 1)
    ranges = column_ranges(n_cols)

    def when(condition, work):
        pl.when(condition)(work)

    barrier = pltpu.get_barrier_semaphore()

    def greet(has, partner):
        def signal():
            pl.semaphore_signal(barrier, inc=1, device_id=partner, device_id_type=MESH)
            pl.semaphore_signal(barrier, inc=1, device_id={"il": other, **partner}, device_id_type=MESH)
        when(has, signal)

    greet(has_ta[1], {"ta": ta - 1})
    greet(has_xl[1], {"xl": xl - 1})
    greet(has_xl[0] & has_ta[1], {"xl": xl + 1, "ta": ta - 1})

    step_load = pltpu.make_async_copy(steps_hbm, steps, load_sem.at[3])
    step_load.start()
    edge_loads = [pltpu.make_async_copy(traces.at[:, pl.ds(start, 8)], edge_x.at[d], load_sem.at[4 + d])
                  for d, start in enumerate((n_cols - 8, 0))]
    for load in edge_loads:
        load.start()

    def load_samples(x, start, rows, slot):
        samples = pl.ds(start, x.shape[2])
        return pltpu.make_async_copy(traces.at[rows, :, samples], x.at[rows], load_sem.at[slot])

    table_load = pltpu.make_async_copy(tables_hbm, tables, load_sem.at[2])

    quarter = n_rows // LOADS
    for p in range(LOADS):
        load_samples(x_left, 0, pl.ds(quarter * p, quarter), 0).start()

    greet(has_xl[0] & has_ta[0], {"xl": xl + 1, "ta": ta + 1})
    greet(has_xl[0], {"xl": xl + 1})
    greet(has_ta[0], {"ta": ta + 1})
    pl.semaphore_signal(barrier, inc=1, device_id={"il": other}, device_id_type=MESH)
    count_xl, count_ta = [sum(jnp.where(has, 1, 0) for has in pair) for pair in (has_xl, has_ta)]
    peers = 1 + 2 * (count_xl + count_ta + jnp.where(has_xl[1], count_ta, 0))

    for e in range(2):
        def no_ta(e=e):
            halo_recv[e] = jnp.zeros_like(halo_recv[e])
        when(jnp.logical_not(has_ta[1 - e]), no_ta)
    for d in range(2):
        def no_xl(d=d):
            rim_recv[d] = jnp.zeros_like(rim_recv[d])
            corner_recv[d] = jnp.zeros_like(corner_recv[d])
        when(jnp.logical_not(has_xl[1 - d]), no_xl)
        for e in range(2):
            def no_diag(d=d, e=e):
                diag_recv[d, e] = jnp.zeros_like(diag_recv[d, e])
                diag_corner[d, e] = jnp.zeros_like(diag_corner[d, e])
            when(jnp.logical_not(has_xl[1 - d] & has_ta[1 - e]), no_diag)

    lane = lax.broadcasted_iota(jnp.int32, (1, LANES), 1)
    is_first, is_last = lane < REACH, lane >= LANES - REACH
    step_load.wait()
    col = lax.broadcasted_iota(jnp.int32, (n_rows, n_cols), 1)
    row = lax.broadcasted_iota(jnp.int32, (n_rows, n_cols), 0)
    bin_col = lax.shift_right_logical(col, 1) + steps[1]
    bin_row = steps[0] + 1
    own = (bin_col >= 0) & (bin_col < own_cols)
    code_a, code_b = [jnp.where(own, bin_row * height + bin_col - first, -1)[:, start:stop]
                      for start, stop, first, height in ranges]
    rest = n_cols - LANES
    keys[0] = code_a
    padded = jnp.concatenate([code_b, jnp.full((n_rows, LANES - rest), -1, jnp.int32)], axis=1)
    keys[1] = padded
    keys[2] = pltpu.roll(padded, rest, 1)

    def one_hot(key, height):
        rows = lax.broadcasted_iota(jnp.int32, (height, key.shape[1]), 0)
        return jnp.where(rows == key, 1.0, 0.0).astype(BF16)

    for p in range(n_pairs):
        key = jnp.concatenate([keys[0, 2 * p: 2 * p + 1], keys[0, 2 * p + 1: 2 * p + 2]], axis=1)
        hot_a[p] = one_hot(key, 3 * ranges[0][3])
        second = keys[2, 2 * p + 1: 2 * p + 2]
        key = jnp.concatenate([jnp.where(lane < rest, keys[1, 2 * p: 2 * p + 1], second),
                               second[:, :2 * rest - LANES]], axis=1)
        hot_b[p] = one_hot(key, 3 * ranges[1][3])
    rim_bin = bin_row - 1 + lax.shift_right_logical(row, 1)
    outside = jnp.where(il == 0, n_pairs, -1)
    rim_code = jnp.where(rim_bin == outside, n_pairs, jnp.where((rim_bin < 0) | (rim_bin >= n_pairs), -1, rim_bin))
    for load in edge_loads:
        load.wait()
    for d, (start, column) in enumerate(((n_cols - 8, own_cols), (0, -1))):
        target = jnp.where(bin_col == column, rim_code, -1)
        key = jnp.concatenate([target[i: i + 1, start: start + 8] for i in range(n_rows)], axis=1)
        chosen = one_hot(key, n_pairs + 8)
        high, low = halves(edge_x[d].reshape(n_rows * 8, span))
        sums = dot(chosen, high) + dot(chosen, low)
        folds = dot(chosen, jnp.ones((n_rows * 8, LANES), BF16))
        ends = jnp.where(is_first, sums[:, :LANES], jnp.where(is_last, sums[:, span - LANES:], folds))
        rim_send[d, :, :span] = sums[:n_pairs]
        rim_send[d, :, span:] = ends[:n_pairs]
        corner_send[d, :, :span] = sums[n_pairs: n_pairs + 1]
        corner_send[d, :, span:] = ends[n_pairs: n_pairs + 1]

    hots = (hot_a, hot_b)
    for p in range(LOADS):
        load_samples(x_right, LANES, pl.ds(quarter * p, quarter), 1).start()

    def merge(p, r, parts, lanes):
        (_, _, _, height), (_, _, first, _) = ranges
        a, b = parts
        both = a[first:] + b[: height - first]
        for at, part in ((0, a[:first]), (first, both), (height, b[height - first:])):
            where = (p + r, slice(at, at + part.shape[0]), lanes)
            acc[where] = part if p == 0 or r == 2 else acc[where] + part

    def groups(parts, r):
        return [part[r * height: (r + 1) * height] for part, (_, _, _, height) in zip(parts, ranges)]

    def bin_pair(p, x, lanes):
        parts, wide = [], x.shape[2]
        for hot, (start, stop, _, _) in zip(hots, ranges):
            high, low = halves(jnp.concatenate([x[2 * p, start:stop], x[2 * p + 1, start:stop]], axis=0))
            sums = dot(hot[p], jnp.concatenate([high, low], axis=1))
            parts.append(sums[:, :wide] + sums[:, wide:])
        for r in range(3):
            merge(p, r, groups(parts, r), lanes)

    ends = (0, 0), (n_pairs - 1, 2)

    def count_pair(p):
        parts = [dot(hot[p], jnp.ones((hot.shape[2], LANES), BF16)) for hot in hots]
        for r in range(3):
            if (p, r) not in ends:
                merge(p, r, groups(parts, r), slice(span, span + LANES))

    def send_sem(slot):
        return load_sem.at[(6, 7, 3, 8, 0, 1, 9, 4, 5)[slot]]

    def remote(src, dst, slot, partner):
        return pltpu.make_async_remote_copy(src_ref=src, dst_ref=dst, send_sem=send_sem(slot), recv_sem=recv_sem.at[slot],
                                            device_id=partner, device_id_type=MESH)

    rim_row = jnp.where(il == 0, n_pairs + 1, 0)
    own_row = jnp.where(il == 0, n_pairs - 1, 0)
    to_other = remote(acc.at[rim_row], il_recv, 0, {"il": other})

    rims, halos, diags = [], [], {}
    for d in range(2):
        to, rows = {"xl": xl_at[d]}, pl.ds(0, n_pairs)
        rims.append((remote(rim_send.at[d], rim_recv.at[d], 1 + d, to),
                     remote(corner_send.at[d], corner_recv.at[d], 1 + d, {"il": other, **to})))
        to = {"ta": ta_at[d]}
        halos.append((remote(halo_send.at[d, rows], halo_recv.at[d, rows], 3 + d, to),
                      remote(halo_send.at[d, n_pairs], halo_recv.at[d, n_pairs], 3 + d, {"il": other, **to})))
        for e in range(2):
            to, end, slot = {"xl": xl_at[d], "ta": ta_at[e]}, pl.ds(span, LANES), 5 + 2 * d + e
            diags[d, e] = (remote(rim_send.at[d, :, end], diag_recv.at[d, e], slot, to),
                           remote(corner_send.at[d, :, end], diag_corner.at[d, e], slot, {"il": other, **to}))

    def received(slot):
        return recv_sem.at[slot]

    def wait_all(semaphores, slot, rows):
        pltpu.make_async_copy(rows, rows, semaphores(slot)).wait()

    def wait_rims(semaphores, d):
        wait_all(semaphores, 1 + d, wide_rows)

    def wait_halos(semaphores, e):
        wait_all(semaphores, 3 + e, halo_recv.at[e])

    def wait_diags(semaphores, d, e):
        wait_all(semaphores, 5 + 2 * d + e, wide_rows.at[:, :, pl.ds(0, LANES)])

    def start_all(copies):
        for copy in copies:
            copy.start()

    def pack_halo(e):
        lanes = slice(0, LANES) if e else slice(span - LANES, span)
        rows = slice(0, REACH) if e else slice(LANES - REACH, LANES)
        for b in range(n_pairs):
            halo_send[e, b, :, :own_cols] = acc[b + 1, :, lanes].T[rows]
        halo_send[e, n_pairs, :, :own_cols] = acc[rim_row, :, lanes].T[rows]

    def send_diags(d):
        for e in (1, 0):
            when(has_ta[e], lambda e=e: start_all(diags[d, e]))

    def send_rims(d):
        send_diags(d)
        start_all(rims[d])

    def late(e):
        def go():
            pl.semaphore_wait(late_sem.at[e], 1)
            when(has_xl[0], lambda: start_all(diags[0, e]))
        when(has_ta[e], go)

    every_row = pl.ds(0, n_rows)
    def bin_left():
        load_samples(x_left, 0, every_row, 0).wait()
        for p in range(n_pairs):
            bin_pair(p, x_left, slice(0, LANES))
        pack_halo(1)

    first = (xl == 0) & (ta == 0)
    opens_late = first | (xl >= 2)
    when(opens_late, bin_left)
    pl.semaphore_wait(barrier, peers)
    when(has_xl[1], lambda: send_rims(1))
    for e in range(2):
        when(has_ta[e], lambda e=e: pl.semaphore_signal(late_sem.at[1 - e], inc=1, device_id={"ta": ta_at[e]},
                                                        device_id_type=MESH))
    when(has_xl[0], lambda: start_all(rims[0]))
    when(jnp.logical_not(opens_late), bin_left)
    when(has_ta[1], lambda: start_all(halos[1]))
    late(1)
    load_samples(x_right, LANES, every_row, 1).wait()
    table_load.start()
    for p in range(n_pairs):
        bin_pair(p, x_right, slice(LANES, span))

    when(jnp.logical_not(opens_late), lambda: late(0))
    pack_halo(0)
    when(has_ta[0], lambda: start_all(halos[0]))
    when(xl >= 2, lambda: late(0))
    for p, r in ends:
        chosen = [hot[p, r * height: (r + 1) * height] for hot, (_, _, _, height) in zip(hots, ranges)]
        merge(p, r, [dot(part, jnp.ones((part.shape[1], LANES), BF16)) for part in chosen], slice(span, span + LANES))
    to_other.start()
    for p in range(n_pairs):
        count_pair(p)
    when(first, lambda: late(0))

    def resample(values):
        high, low = halves(values)
        return dot(high, tables[0]) + (dot(low, tables[0]) + dot(high, tables[1]))

    table_load.wait()
    for i in range(n_pairs):
        b = jnp.where(il == 0, i, n_pairs - 1 - i)
        if i == n_pairs - 1:
            to_other.wait_recv()
            acc[b + 1] = acc[b + 1] + il_recv[...]
        main[b] = resample(acc[b + 1, :, :span])
    for d in range(2):
        when(has_xl[1 - d], lambda d=d: wait_rims(received, d))
    sub = lax.broadcasted_iota(jnp.int32, (n_pairs, 1), 0)
    rim = jnp.concatenate([rim_recv[d] + jnp.where(sub == own_row, corner_recv[d], 0.0) for d in range(2)], axis=0)
    more = resample(rim[:, :span])
    more_fold = jnp.broadcast_to(rim[:, span + LANES // 2: span + LANES // 2 + 1], (2 * n_pairs, LANES))
    ends_row = lax.broadcasted_iota(jnp.int32, (8, 1), 0)
    tops = ((0, 0, 0), (own_cols - 8, 7, n_pairs))

    def add_rows(values, extra, b):
        top, bottom = [values[at: at + 8] + jnp.where(ends_row == where, extra[base + b: base + b + 1], 0.0)
                       for at, where, base in tops]
        return jnp.concatenate([top, values[8: own_cols - 8], bottom], axis=0)

    for b in range(n_pairs):
        scale = 1.0 / jnp.maximum(add_rows(acc[b + 1, :, span:], more_fold, b), 1.0)
        factor[b] = scale
        main[b] = add_rows(main[b], more, b) * jnp.concatenate([scale] * (main.shape[2] // LANES), axis=1)

    to_other.wait_send()
    for d in range(2):
        when(has_xl[d], lambda d=d: wait_rims(send_sem, d))
        when(has_ta[d], lambda d=d: wait_halos(send_sem, d))
        for e in range(2):
            when(has_xl[d] & has_ta[e], lambda d=d, e=e: wait_diags(send_sem, d, e))

    for d in range(2):
        for e in range(2):
            when(has_xl[1 - d] & has_ta[1 - e], lambda d=d, e=e: wait_diags(received, d, e))
    for d in range(2):
        first, last = [diag_recv[d, e] + jnp.where(sub == own_row, diag_corner[d, e], 0.0) for e in (1, 0)]
        rim_out[d * n_pairs: (d + 1) * n_pairs] = jnp.where(is_first, first, jnp.where(is_last, last, 0.0))
    for e in range(2):
        when(has_ta[1 - e], lambda e=e: wait_halos(received, e))
        halo_out[e] = halo_recv[e, :n_pairs]
        halo_out[e, own_row] = halo_recv[e, own_row] + halo_recv[e, n_pairs]


def finish(main, factor, halo, rim, tables, out, staged, out_sem):
    n_pairs, own_cols, width = main.shape
    starts = (0, width - LANES)
    has_before = lax.axis_index("ta") > 0

    def write_tiles(source, start, size, slot):
        return pltpu.make_async_copy(source, out.at[:, :, pl.ds(start, size)], out_sem.at[slot])

    def from_main(start, size, slot):
        return write_tiles(main.at[:, :, pl.ds(start, size)], start, size, slot)

    from_main(LANES, width - 2 * LANES, 2).start()
    pl.when(jnp.logical_not(has_before))(from_main(0, LANES, 0).start)
    ends_row = lax.broadcasted_iota(jnp.int32, (8, 1), 0)
    tops = ((0, 0, 0), (own_cols - 8, 7, n_pairs))

    def add_halo(tiles, table):
        high = rim[...].astype(BF16)
        low = (rim[...] - high.astype(F32)).astype(BF16)
        more = dot(jnp.concatenate([high, low, high], axis=1), tables[12 * REACH:])
        for pair in zip(tiles[::2], tiles[1::2]):
            terms = []
            for d, b in pair:
                high = halo[d, b].astype(BF16).astype(F32)
                terms += [high, halo[d, b] - high, high]
            both = dot(jnp.concatenate(terms, axis=0).T[:own_cols].astype(BF16), tables[table * 6 * REACH: (table + 1) * 6 * REACH])
            for i, (d, b) in enumerate(pair):
                ends, lanes = both[:, i * LANES: (i + 1) * LANES], slice(d * LANES, (d + 1) * LANES)
                top, bottom = [ends[at: at + 8] + jnp.where(ends_row == where, more[base + b: base + b + 1, lanes], 0.0)
                               for at, where, base in tops]
                ends = jnp.concatenate([top, ends[8: own_cols - 8], bottom], axis=0)
                staged[d, b] = main[b, :, starts[d]: starts[d] + LANES] + ends * factor[b]
                pltpu.make_async_copy(staged.at[d, b], out.at[b, :, pl.ds(starts[d], LANES)], out_sem.at[d]).start()

    rows = range(n_pairs)
    pl.when(has_before)(lambda: add_halo([(d, b) for b in rows for d in range(2)], 0))
    pl.when(jnp.logical_not(has_before))(lambda: add_halo([(1, b) for b in rows], 1))
    from_main(LANES, width - 2 * LANES, 2).wait()
    for d in range(2):
        write_tiles(staged.at[d], starts[d], LANES, d).wait()


def shards(n_xl, n_ta, traces, bin_steps):
    n_rows, n_cols, span = traces.shape
    n_pairs, own_cols = n_rows // 2, n_cols // 2
    width = span + LANES
    out_span = span * P_SIZE // Q
    if n_pairs % 8 or span % LANES or out_span % LANES or out_span < 3 * LANES:
        raise ValueError("block shape")
    table = lanczos_table(span)
    tables = np.stack(split_table(table[REACH:-REACH]))
    edge_cols = np.concatenate([table[:, :LANES], table[:, -LANES:]], axis=1)
    edge_high, edge_low = split_table(np.stack([edge_cols[:REACH, :LANES], edge_cols[-REACH:, LANES:]]))
    before, after = np.concatenate([edge_high, edge_high, edge_low], axis=1)
    none = np.zeros_like(before)
    t_edge = np.stack([np.block([[first, none], [none, after]]) for first in (before, after)])
    rim_high, rim_low = split_table(np.concatenate(
        [edge_cols[-REACH:], np.zeros((LANES - 2 * REACH, 2 * LANES), np.float32), edge_cols[:REACH]]))
    t_rim = np.concatenate([rim_high, rim_high, rim_low])
    vmem = pl.BlockSpec(memory_space=pltpu.VMEM)
    hbm = pl.BlockSpec(memory_space=pltpu.HBM)
    (start_a, stop_a, _, height_a), (start_b, stop_b, _, height_b) = column_ranges(n_cols)
    main, factor, halo, rim = pl.pallas_call(
        scoped(functools.partial(binning, n_xl, n_ta), pltpu.SemaphoreType.DMA((10,)), pltpu.SemaphoreType.REGULAR((2,)),
               pltpu.SemaphoreType.DMA((9,))),
        out_shape=(pltpu.VMEM((n_pairs, own_cols, out_span), F32), pltpu.VMEM((n_pairs, own_cols, LANES), F32),
                   pltpu.VMEM((2, n_pairs, REACH, LANES), F32), pltpu.VMEM((2 * n_pairs, LANES), F32)),
        in_specs=[hbm] * 3,
        out_specs=[vmem] * 4,
        scratch_shapes=[
            pltpu.VMEM((n_rows, n_cols, LANES), F32),
            pltpu.VMEM((n_rows, n_cols, span - LANES), F32),
            pltpu.VMEM((2, n_rows, 8, span), F32),
            pltpu.VMEM((2, n_rows, n_cols), jnp.int32),
            pltpu.VMEM(tables.shape, BF16),
            pltpu.VMEM((3, n_rows, LANES), jnp.int32),
            pltpu.VMEM((n_pairs, 3 * height_a, 2 * (stop_a - start_a)), BF16),
            pltpu.VMEM((n_pairs, 3 * height_b, 2 * (stop_b - start_b)), BF16),
            pltpu.VMEM((n_pairs + 2, own_cols, width), F32),
            pltpu.VMEM((2, n_pairs, width), F32),
            pltpu.VMEM((2, 1, width), F32),
            pltpu.VMEM((2, n_pairs, width), F32),
            pltpu.VMEM((2, 1, width), F32),
            pltpu.VMEM((own_cols, width), F32),
            pltpu.VMEM((2, n_pairs + 1, REACH, LANES), F32),
            pltpu.VMEM((2, n_pairs + 1, REACH, LANES), F32),
            pltpu.VMEM((n_pairs + 1, 1, width), F32),
            pltpu.VMEM((2, 2, n_pairs, LANES), F32),
            pltpu.VMEM((2, 2, 1, LANES), F32),
        ],
        compiler_params=pltpu.CompilerParams(collective_id=0, has_side_effects=True, vmem_limit_bytes=24 * 2**20),
        name="binning",
    )(*[pltpu.with_memory_space_constraint(a, pltpu.HBM) for a in (traces, bin_steps, jnp.asarray(tables))])
    return pl.pallas_call(
        scoped(finish, pltpu.SemaphoreType.DMA((3,))),
        out_shape=jax.ShapeDtypeStruct((n_pairs, own_cols, out_span), F32),
        in_specs=[vmem] * 5,
        out_specs=hbm,
        scratch_shapes=[pltpu.VMEM((2, n_pairs, own_cols, LANES), F32)],
        compiler_params=pltpu.CompilerParams(vmem_limit_bytes=16 * 2**20),
        name="finish",
    )(main, factor, halo, rim, jnp.asarray(np.concatenate([*t_edge, t_rim])))


def solution(mesh):
    if mesh.shape["il"] != 2:
        raise ValueError("il size")
    return jax.shard_map(
        functools.partial(shards, mesh.shape["xl"], mesh.shape["ta"]),
        mesh=mesh,
        in_specs=(P("il", "xl", "ta"), P(None, "il", "xl")),
        out_specs=P("il", "xl", "ta"),
        check_vma=False,
    )
```
